32 devices in a mesh: dp: 8 (over z, y), seq: 4 (over x, core).
Axes of the slice: x: 2, y: 2, z: 4, core: 2. Of those that a mesh axis runs over, the one named last changes fastest.
Arguments:
- tokens: bfloat16 [16, 256, 1152], P('dp', 'seq'), may hold values from -6 to 6
- cotangent: bfloat16 [16, 256, 1152], P('dp', 'seq'), may hold values from -6 to 6
- ln1_gain: bfloat16 [1152], P('dp'), may hold values from 0.5 to 1.5
- ln1_shift: bfloat16 [1152], P('dp'), may hold values from -1.5 to 1.5
- q_weight: bfloat16 [1152, 1152], P('dp'), may hold values from -0.1875 to 0.1875
- q_bias: bfloat16 [1152], P('dp'), may hold values from -1.5 to 1.5
- k_weight: bfloat16 [1152, 1152], P('dp'), may hold values from -0.1875 to 0.1875
- v_weight: bfloat16 [1152, 1152], P('dp'), may hold values from -0.1875 to 0.1875
- v_bias: bfloat16 [1152], P('dp'), may hold values from -0.25 to 0.25
- o_weight: bfloat16 [1152, 1152], P('dp'), may hold values from -1.5 to 1.5
- o_bias: bfloat16 [1152], P('dp'), may hold values from -1.5 to 1.5
- ln2_gain: bfloat16 [1152], P('dp'), may hold values from 0.5 to 1.5
- ln2_shift: bfloat16 [1152], P('dp'), may hold values from -1.5 to 1.5
- in_weight: bfloat16 [1152, 4304], P('dp'), may hold values from -0.1875 to 0.1875
- in_bias: bfloat16 [4304], replicated, may hold values from -2.5 to 2.5
- out_weight: bfloat16 [4304, 1152], P(None, 'dp'), may hold values from -0.09375 to 0.09375
- out_bias: bfloat16 [1152], P('dp'), may hold values from -1.5 to 1.5
Outputs:
- output: bfloat16 [16, 256, 1152], P('dp', 'seq')
- grad_tokens: bfloat16 [16, 256, 1152], P('dp', 'seq')
- grad_ln1_gain: float32 [1152], P('dp')
- grad_ln1_shift: float32 [1152], P('dp')
- grad_q_weight: float32 [1152, 1152], P('dp')
- grad_q_bias: float32 [1152], P('dp')
- grad_k_weight: float32 [1152, 1152], P('dp')
- grad_v_weight: float32 [1152, 1152], P('dp')
- grad_v_bias: float32 [1152], P('dp')
- grad_o_weight: float32 [1152, 1152], P('dp')
- grad_o_bias: float32 [1152], P('dp')
- grad_ln2_gain: float32 [1152], P('dp')
- grad_ln2_shift: float32 [1152], P('dp')
- grad_in_weight: float32 [1152, 4304], P('dp')
- grad_in_bias: float32 [4304], replicated
- grad_out_weight: float32 [4304, 1152], P(None, 'dp')
- grad_out_bias: float32 [1152], P('dp')
The draws below stay inside these ranges and needn't reach their ends.
All inputs are finite; a program needn't handle non-finite values.
Results may differ from the reference program's by a relative error of at most 0.019.
Values may be sent and summed in bfloat16 or wider, within the bound.
A program may use at most 256 MiB of HBM per device.

```python
import math
import jax
import jax.numpy as jnp
from jax import lax

D = 1152
HEADS = 16
HEAD_DIM = 72
FF = 4304
LENGTH = 256
IMAGES = 16


def block_levels(own_key, shape, split, least, largest):
    factor_of = 1.0
    for axis_at, parts in split:
        heights = jax.random.uniform(jax.random.fold_in(jax.random.fold_in(own_key, 6), axis_at), (parts,), jnp.float32, least / len(split), largest / len(split))
        factor_of = factor_of * jnp.repeat(jnp.exp(heights), shape[axis_at] // parts).reshape((-1,) + (1,) * (len(shape) - 1 - axis_at))
    return factor_of


def normal_values(own_key, extent, width, most, pieces=(), held_as=jnp.bfloat16):
    entries = jax.random.normal(own_key, extent, jnp.float32) * width
    if len(pieces) > 0:
        entries = block_levels(own_key, extent, pieces, -0.22, 0.18) * entries
    return jnp.clip(entries, min=-most, max=most).astype(held_as)


def setup_inputs(seed: int = 0) -> dict:
    key_list = jax.random.split(jax.random.key(seed), 18)
    tokens = normal_values(key_list[0], (IMAGES, LENGTH, D), 1.0, 6.0, ((0, 8), (1, 4)))
    cotangent = normal_values(key_list[1], (IMAGES, LENGTH, D), 1.0, 6.0, ((0, 8), (1, 4)))
    ln1_gain = jnp.clip(1.0 + 0.1 * jax.random.normal(key_list[2], (D,), jnp.float32), 0.5, 1.5).astype(jnp.bfloat16)
    ln1_shift = normal_values(key_list[3], (D,), 0.3, 1.5, ((0, 8),))
    q_weight = normal_values(key_list[4], (D, D), D ** -0.5, 0.1875, ((0, 8),))
    q_bias = normal_values(key_list[5], (D,), 0.3, 1.5, ((0, 8),))
    k_weight = normal_values(key_list[6], (D, D), D ** -0.5, 0.1875, ((0, 8),))
    v_weight = normal_values(key_list[7], (D, D), D ** -0.5, 0.1875, ((0, 8),))
    v_bias = normal_values(key_list[8], (D,), 0.05, 0.25, ((0, 8),))
    o_weight = normal_values(key_list[9], (D, D), (D // 64) ** -0.5, 1.5, ((0, 8),))
    o_bias = normal_values(key_list[10], (D,), 0.3, 1.5, ((0, 8),))
    ln2_gain = jnp.clip(1.0 + 0.1 * jax.random.normal(key_list[11], (D,), jnp.float32), 0.5, 1.5).astype(jnp.bfloat16)
    ln2_shift = normal_values(key_list[12], (D,), 0.3, 1.5, ((0, 8),))
    in_weight = normal_values(key_list[13], (D, FF), D ** -0.5, 0.1875, ((0, 8),))
    in_bias = normal_values(key_list[14], (FF,), 0.5, 2.5)
    out_weight = normal_values(key_list[15], (FF, D), FF ** -0.5, 0.09375, ((1, 8),))
    out_bias = normal_values(key_list[16], (D,), 0.3, 1.5, ((0, 8),))
    return {"tokens": tokens, "cotangent": cotangent, "ln1_gain": ln1_gain, "ln1_shift": ln1_shift, "q_weight": q_weight, "q_bias": q_bias, "k_weight": k_weight, "v_weight": v_weight, "v_bias": v_bias, "o_weight": o_weight, "o_bias": o_bias, "ln2_gain": ln2_gain, "ln2_shift": ln2_shift, "in_weight": in_weight, "in_bias": in_bias, "out_weight": out_weight, "out_bias": out_bias}


@jax.custom_vjp
def low(v):
    return lax.optimization_barrier(v.astype(jnp.bfloat16)).astype(jnp.float32)

@jax.custom_vjp
def low_back(v):
    return v

def low_keep(v):
    return (low(v), None)

def low_pass(kept, grad):
    return (grad,)

def back_keep(v):
    return (v, None)

def back_low(kept, grad):
    return (low(grad),)
low.defvjp(low_keep, low_pass)
low_back.defvjp(back_keep, back_low)
eps_norm = 1e-06
gelu_coef = 0.7978845608028654
gelu_cube = 0.044715

def layer_norm(values, gain_vec, shift_vec):
    row_mean = lax.optimization_barrier(jnp.mean(values, axis=-1, keepdims=True))
    centred = values - row_mean
    variance = lax.optimization_barrier(jnp.mean(centred * centred, axis=-1, keepdims=True))
    return centred * lax.rsqrt(variance + eps_norm) * gain_vec + shift_vec

def matmul(left_mat, right_mat):
    return jnp.dot(left_mat, right_mat, precision=lax.Precision.HIGHEST, preferred_element_type=jnp.float32)

def gelu_tanh(pre_act):
    return 0.5 * pre_act * (1.0 + jnp.tanh(gelu_coef * (pre_act + gelu_cube * pre_act * pre_act * pre_act)))

def image_forward(start_rows, params):
    ln1_gain, ln1_shift, q_weight, q_bias, k_weight, v_weight, v_bias, o_weight, o_bias, ln2_gain, ln2_shift, in_weight, in_bias, out_weight, out_bias = params
    length = start_rows.shape[0]
    normed1 = low(layer_norm(start_rows, ln1_gain, ln1_shift))
    queries = low(low_back(matmul(normed1, q_weight) + q_bias))
    key_rows = low(low_back(matmul(normed1, k_weight)))
    value_rows = low(low_back(matmul(normed1, v_weight) + v_bias))
    query_heads = queries.reshape(length, HEADS, HEAD_DIM)
    key_heads = key_rows.reshape(length, HEADS, HEAD_DIM)
    value_heads = value_rows.reshape(length, HEADS, HEAD_DIM)
    scores = low_back(jnp.einsum('qhd,khd->hqk', query_heads, key_heads, precision=lax.Precision.HIGHEST) * (1.0 / math.sqrt(HEAD_DIM)))
    attn_probs = jax.nn.softmax(scores, axis=-1)
    mixed_rows = jnp.einsum('hqk,khd->qhd', low(attn_probs), value_heads, precision=lax.Precision.HIGHEST)
    mixed_rows = low(low_back(mixed_rows.reshape(length, HEADS * HEAD_DIM)))
    hidden = start_rows + low_back(matmul(mixed_rows, o_weight) + o_bias)
    normed2 = low(layer_norm(hidden, ln2_gain, ln2_shift))
    pre_act = low_back(matmul(normed2, in_weight) + in_bias)
    active = low(gelu_tanh(pre_act))
    return hidden + low_back(matmul(active, out_weight) + out_bias)

def reference(tokens, cotangent, ln1_gain, ln1_shift, q_weight, q_bias, k_weight, v_weight, v_bias, o_weight, o_bias, ln2_gain, ln2_shift, in_weight, in_bias, out_weight, out_bias):
    params = tuple((weight_arr.astype(jnp.float32) for weight_arr in (ln1_gain, ln1_shift, q_weight, q_bias, k_weight, v_weight, v_bias, o_weight, o_bias, ln2_gain, ln2_shift, in_weight, in_bias, out_weight, out_bias)))

    def step_image(running, slices):
        image_rows, image_cot = slices
        result, pullback = jax.vjp(image_forward, image_rows.astype(jnp.float32), params)
        grad_rows, grad_params = pullback(image_cot.astype(jnp.float32))
        running = tuple((old_sum + new_term for old_sum, new_term in zip(running, grad_params)))
        return (running, (result.astype(jnp.bfloat16), grad_rows.astype(jnp.bfloat16)))
    zero_sums = tuple((jnp.zeros(weight_arr.shape, jnp.float32) for weight_arr in params))
    grad_sums, (outputs, grad_tokens) = lax.scan(step_image, zero_sums, (tokens, cotangent))
    return (outputs, grad_tokens) + grad_sums
```

```python
import math

import jax
import jax.numpy as jnp
from jax import lax
from jax.sharding import PartitionSpec as P

HEADS = 16
HEAD_DIM = 72

eps_norm = 1e-06
gelu_coef = 0.7978845608028654
gelu_cube = 0.044715
F32 = jnp.float32
BF16 = jnp.bfloat16


def mm(a, b, ca, cb):
    return lax.dot_general(a, b, (((ca,), (cb,)), ((), ())), preferred_element_type=F32)


def normalize(values):
    row_mean = jnp.mean(values, axis=-1, keepdims=True)
    centred = values - row_mean
    inverse = lax.rsqrt(jnp.mean(centred * centred, axis=-1, keepdims=True) + eps_norm)
    return centred * inverse, inverse


def norm_back(grad_normed, gain_vec, scaled, inverse):
    grad_scaled = grad_normed * gain_vec
    centred_grad = grad_scaled - jnp.mean(grad_scaled, axis=-1, keepdims=True)
    return inverse * (
        centred_grad - scaled * jnp.mean(grad_scaled * scaled, axis=-1, keepdims=True)
    )


def gelu_parts(pre_act):
    tanh_val = jnp.tanh(gelu_coef * (pre_act + gelu_cube * pre_act * pre_act * pre_act))
    value_part = 0.5 * pre_act * (1.0 + tanh_val)
    slope_part = 0.5 * (1.0 + tanh_val) + 0.5 * pre_act * (
        1.0 - tanh_val * tanh_val
    ) * gelu_coef * (1.0 + 3.0 * gelu_cube * pre_act * pre_act)
    return value_part, slope_part


def on_device(
    tokens, cotangent, ln1_gain, ln1_shift, q_weight, q_bias, k_weight, v_weight, v_bias,
    o_weight, o_bias, ln2_gain, ln2_shift, in_weight, in_bias, out_weight, out_bias,
):
    part = lax.axis_index("seq")
    parts = lax.axis_size("seq")
    groups = lax.axis_size("dp")
    images, own_len, width = tokens.shape
    ff = in_weight.shape[1]
    hid = width // parts
    ffp = ff // parts
    heads = HEADS // parts
    length = own_len * parts
    rows = images * length

    def cols(w, n):
        return lax.dynamic_slice_in_dim(w, part * n, n, axis=1)

    vecs = jnp.stack(
        [ln1_gain, ln1_shift, q_bias, v_bias, o_bias, ln2_gain, ln2_shift, out_bias]
    )
    vecs = lax.all_gather(vecs, "dp", axis=1, tiled=True).astype(F32)
    g1, s1, qb, vb, ob, g2, s2, outb = [vecs[i] for i in range(8)]
    x = lax.all_gather(tokens, "seq", axis=1, tiled=True).reshape(rows, width)
    cot = lax.all_gather(cotangent, "seq", axis=1, tiled=True).reshape(rows, width)
    qkv = jnp.concatenate([cols(q_weight, hid), cols(k_weight, hid), cols(v_weight, hid)], axis=1)
    qkv = lax.all_gather(qkv, "dp", axis=0, tiled=True)
    o_w = lax.all_gather(o_weight, "dp", axis=0, tiled=True)
    o_w = lax.dynamic_slice_in_dim(o_w, part * hid, hid, axis=0)
    in_w = lax.all_gather(cols(in_weight, ffp), "dp", axis=0, tiled=True)
    out_w = lax.dynamic_slice_in_dim(out_weight, part * ffp, ffp, axis=0)
    out_w = lax.all_gather(out_w.T, "dp", axis=0, tiled=True)
    qb_own = lax.dynamic_slice_in_dim(qb, part * hid, hid)
    vb_own = lax.dynamic_slice_in_dim(vb, part * hid, hid)
    inb_own = lax.dynamic_slice_in_dim(in_bias, part * ffp, ffp).astype(F32)

    def scatter_tokens(partial):
        return lax.psum_scatter(
            partial.astype(BF16).reshape(images, length, width),
            "seq", scatter_dimension=1, tiled=True,
        ).astype(F32)

    hat1, _ = normalize(x.astype(F32))
    normed1 = (hat1 * g1 + s1).astype(BF16)
    proj = mm(normed1, qkv, 1, 0)
    queries = (proj[:, :hid] + qb_own).astype(BF16).reshape(images, length, heads, HEAD_DIM)
    keys = proj[:, hid : 2 * hid].astype(BF16).reshape(images, length, heads, HEAD_DIM)
    values = (proj[:, 2 * hid :] + vb_own).astype(BF16).reshape(images, length, heads, HEAD_DIM)
    factor = 1.0 / math.sqrt(HEAD_DIM)
    ein = lambda s, a, b: jnp.einsum(s, a, b, preferred_element_type=F32)
    scores = ein("iqhd,ikhd->ihqk", queries, keys) * factor
    top = jnp.max(scores, axis=-1, keepdims=True)
    expo = jnp.exp(scores - top)
    probs = expo / jnp.sum(expo, axis=-1, keepdims=True)
    probs_low = probs.astype(BF16)
    mixed = ein("ihqk,ikhd->iqhd", probs_low, values).astype(BF16).reshape(rows, hid)
    start = tokens.astype(F32)
    hidden = start + scatter_tokens(mm(mixed, o_w, 1, 0)) + ob
    hat2, r2 = normalize(hidden)
    normed2 = (hat2 * g2 + s2).astype(BF16)
    normed2 = lax.all_gather(normed2, "seq", axis=1, tiled=True).reshape(rows, width)
    pre = mm(normed2, in_w, 1, 0) + inb_own
    act, slope = gelu_parts(pre)
    act = act.astype(BF16)
    out = hidden + scatter_tokens(mm(act, out_w, 1, 1)) + outb
    d_out_w = mm(cot, act, 0, 0)
    cot_own = cotangent.astype(F32)
    grad_pre = (mm(cot, out_w, 1, 0) * slope).astype(BF16)
    d_in_w = mm(normed2, grad_pre, 0, 0)
    d_in_b = jnp.sum(grad_pre.astype(F32), axis=0)
    grad_n2 = scatter_tokens(mm(grad_pre, in_w, 1, 1))
    grad_hidden = cot_own + norm_back(grad_n2, g2, hat2, r2)
    branch_own = grad_hidden.astype(BF16)
    branch = lax.all_gather(branch_own, "seq", axis=1, tiled=True).reshape(rows, width)
    d_o_w = mm(mixed, branch, 0, 0)
    grad_mixed = mm(branch, o_w, 1, 1).astype(BF16).reshape(images, length, heads, HEAD_DIM)
    grad_probs = ein("iqhd,ikhd->ihqk", grad_mixed, values)
    row_dot = jnp.sum(probs * grad_probs, axis=-1, keepdims=True)
    grad_scores = (probs * (grad_probs - row_dot)).astype(BF16)
    grad_q = (ein("ihqk,ikhd->iqhd", grad_scores, keys) * factor).astype(BF16).reshape(rows, hid)
    grad_k = (ein("ihqk,iqhd->ikhd", grad_scores, queries) * factor).astype(BF16).reshape(rows, hid)
    grad_v = ein("ihqk,iqhd->ikhd", probs_low, grad_mixed).astype(BF16).reshape(rows, hid)
    grad_qkv = jnp.concatenate([grad_q, grad_k, grad_v], axis=1)
    d_qkv = mm(normed1, grad_qkv, 0, 0)
    d_qb = jnp.sum(grad_q.astype(F32), axis=0)
    d_vb = jnp.sum(grad_v.astype(F32), axis=0)
    grad_n1 = scatter_tokens(mm(grad_qkv, qkv, 1, 1))
    hat1o, r1o = normalize(start)
    grad_tokens = grad_hidden + norm_back(grad_n1, g1, hat1o, r1o)
    wide = jnp.concatenate([d_qkv, d_in_w, d_out_w], axis=1).astype(BF16)
    wide = lax.psum_scatter(wide, "dp", scatter_dimension=0, tiled=True)
    wide = lax.all_gather(wide, "seq", axis=0, tiled=False).astype(F32)

    def spread(lo, n):
        return wide[:, :, lo : lo + n].transpose(1, 0, 2).reshape(width // groups, n * parts)

    gq, gk, gv = [spread(i * hid, hid) for i in range(3)]
    gin = spread(3 * hid, ffp)
    gout = wide[:, :, 3 * hid + ffp :].transpose(0, 2, 1).reshape(ff, width // groups)
    o_full = lax.all_gather(
        lax.psum_scatter(d_o_w.astype(BF16), "dp", scatter_dimension=1, tiled=True),
        "seq", axis=0, tiled=True,
    )
    go = lax.all_to_all(o_full, "dp", split_axis=0, concat_axis=1, tiled=True).astype(F32)
    own_sums = jnp.stack([
        jnp.sum(grad_n1 * hat1o, axis=(0, 1)), jnp.sum(grad_n1, axis=(0, 1)),
        jnp.sum(grad_n2 * hat2, axis=(0, 1)), jnp.sum(grad_n2, axis=(0, 1)),
        jnp.sum(branch_own.astype(F32), axis=(0, 1)), jnp.sum(cot_own, axis=(0, 1)),
        lax.dynamic_update_slice_in_dim(jnp.zeros(width, F32), d_qb, part * hid, 0),
        lax.dynamic_update_slice_in_dim(jnp.zeros(width, F32), d_vb, part * hid, 0),
    ])
    bias_in = lax.dynamic_update_slice_in_dim(jnp.zeros(ff, F32), d_in_b, part * ffp, 0)
    total = lax.psum(jnp.concatenate([own_sums.reshape(-1), bias_in]), ("dp", "seq"))
    vec_part = total[: 8 * width].reshape(8, groups, width // groups)
    vec_part = lax.dynamic_index_in_dim(vec_part, lax.axis_index("dp"), axis=1, keepdims=False)
    bias_total = total[8 * width :]
    return (
        out.astype(BF16), grad_tokens.astype(BF16), vec_part[0], vec_part[1], gq, vec_part[6],
        gk, gv, vec_part[7], go, vec_part[4], vec_part[2], vec_part[3], gin, bias_total, gout,
        vec_part[5],
    )


def solution(mesh):
    rows, vec = P("dp", None), P("dp")
    tok = P("dp", "seq", None)
    return jax.shard_map(
        on_device,
        mesh=mesh,
        in_specs=(tok, tok, vec, vec, rows, vec, rows, rows, vec, rows, vec, vec, vec, rows,
                  P(), P(None, "dp"), vec),
        out_specs=(tok, tok, vec, vec, rows, vec, rows, rows, vec, rows, vec, vec, vec, rows,
                   P(), P(None, "dp"), vec),
        check_vma=False,
    )
```

```python
import functools
import math

import jax
import jax.numpy as jnp
from jax import lax
from jax.experimental import pallas as pl
from jax.experimental.pallas import tpu as pltpu
from jax.sharding import PartitionSpec as P

BF16, F32 = jnp.bfloat16, jnp.float32
HEADS, HEAD_DIM = 16, 72
eps_norm = 1e-06
gelu_coef = 0.7978845608028654
gelu_cube = 0.044715
MESH = pl.DeviceIdType.MESH
VEC = 8


def normalize(values):
    row_mean = jnp.mean(values, axis=-1, keepdims=True)
    centred = values - row_mean
    inverse = lax.rsqrt(jnp.mean(centred * centred, axis=-1, keepdims=True) + eps_norm)
    return centred * inverse, inverse


def norm_back(grad_normed, gain_vec, scaled, inverse):
    grad_scaled = grad_normed * gain_vec
    centred_grad = grad_scaled - jnp.mean(grad_scaled, axis=-1, keepdims=True)
    return inverse * (
        centred_grad - scaled * jnp.mean(grad_scaled * scaled, axis=-1, keepdims=True)
    )


def gelu_parts(pre_act):
    tanh_val = jnp.tanh(gelu_coef * (pre_act + gelu_cube * pre_act * pre_act * pre_act))
    value_part = 0.5 * pre_act * (1.0 + tanh_val)
    slope_part = 0.5 * (1.0 + tanh_val) + 0.5 * pre_act * (
        1.0 - tanh_val * tanh_val
    ) * gelu_coef * (1.0 + 3.0 * gelu_cube * pre_act * pre_act)
    return value_part, slope_part


def dot(a, b, ca, cb):
    return lax.dot_general(a, b, (((ca,), (cb,)), ((), ())), preferred_element_type=F32)


def layer_kernel(
    nz, hid, ffp,
    wp, ow_own, tok, cot_in, inb,
    out_ref, gtok_ref, fgrad, ograd, ibgrad,
    w, ow, xall, call, n1, n2, gb, qkv, probs, mix, act, slope, gp, part, part2, r1, r1b,
    dx, dy, rx, ry, dxb, dyb, rxb, ryb, hid_s, hat2_s, inv2_s, gh_s, n2own, gbown, vecs, g, rb, rbo, gin_tail,
    gout_tail, dqkv, vsum, ibx, isb, og,
    gy_s, gzr_s, gzl_s, g_r, o_s, o_r, ag_s, ag_r, rs_s, rs_r, z_s, z_r, zo_s, zo_r, f_s, f_r,
    ib_s, ib_r,
):
    d, s = lax.axis_index("dp"), lax.axis_index("seq")
    z, y = d // 2, d % 2
    x, c = s // 2, s % 2
    rank = 2 * s + y
    own_len = tok.shape[1]
    nimg, length, width = xall.shape
    rows8 = wp.shape[1]
    plane = 2 * rows8
    cols = 512
    qw = hid
    in_at = VEC + 3 * qw
    in_win = in_at // 128 * 128
    out_at = in_at + ffp
    out_win = out_at // 128 * 128
    win = (ffp + 127) // 128 * 128
    off_in, off_out = in_at - in_win, out_at - out_win
    shift = off_out - off_in
    core_n, x_n, y_n = (d, s + 1 - 2 * c), (d, (s + 2) % 4), (d + 1 - 2 * y, s)
    right, left = (d + 2, s), (d - 2, s)
    has_r, has_l = z < nz - 1, z > 0
    factor = 1.0 / math.sqrt(HEAD_DIM)

    def rc(src, dst, ss, rs, dev):
        return pltpu.make_async_remote_copy(
            src_ref=src, dst_ref=dst, send_sem=ss, recv_sem=rs, device_id=dev, device_id_type=MESH
        )

    barrier = pltpu.get_barrier_semaphore()
    for dev in (core_n, x_n, y_n):
        pl.semaphore_signal(barrier, inc=1, device_id=dev, device_id_type=MESH)
    pl.when(has_r)(lambda: pl.semaphore_signal(barrier, inc=1, device_id=right, device_id_type=MESH))
    pl.when(has_l)(lambda: pl.semaphore_signal(barrier, inc=1, device_id=left, device_id_type=MESH))
    beside = (z + nz - 2) // (nz - 1) + (2 * nz - 3 - z) // (nz - 1)
    pl.semaphore_wait(barrier, 3 + beside)

    def wrows(origin, sub):
        return pl.ds(pl.multiple_of(origin * plane + sub * rows8, 16), rows8)

    def wslab(ch, origin, sub):
        return w.at[wrows(origin, sub), pl.ds(ch * cols, cols)]

    def wsend(ch, origin, sub, src, to_right):
        sems = gzr_s if to_right else gzl_s
        return rc(src, wslab(ch, origin, sub), sems.at[ch, origin, sub], g_r.at[ch, origin, sub],
                  right if to_right else left)

    def wrecv(ch, origin, sub):
        slab = wslab(ch, origin, sub)
        rc(slab, slab, g_r.at[ch, origin, sub], g_r.at[ch, origin, sub], core_n).wait_recv()

    def gather_own(ch):
        src = wp.at[y, :, pl.ds(ch * cols, cols)]
        pl.when(has_r)(lambda: wsend(ch, z, y, src, True).start())
        pl.when(has_l)(lambda: wsend(ch, z, y, src, False).start())
        w[wrows(z, y), ch * cols : (ch + 1) * cols] = wp[y, :, ch * cols : (ch + 1) * cols]

    def gather_swap(ch):
        rc(wp.at[1 - y, :, pl.ds(ch * cols, cols)], wslab(ch, z, y), gy_s.at[ch], g_r.at[ch, z, y],
           y_n).start()

    def gather_other(ch):
        wrecv(ch, z, 1 - y)
        src = wslab(ch, z, 1 - y)
        pl.when(has_r)(lambda: wsend(ch, z, 1 - y, src, True).start())
        pl.when(has_l)(lambda: wsend(ch, z, 1 - y, src, False).start())

    def gather_hop(ch, k):
        def from_left():
            for sub in range(2):
                wrecv(ch, z - k, sub)
                pl.when(has_r)(lambda: wsend(ch, z - k, sub, wslab(ch, z - k, sub), True).start())

        def from_right():
            for sub in range(2):
                wrecv(ch, z + k, sub)
                pl.when(has_l)(lambda: wsend(ch, z + k, sub, wslab(ch, z + k, sub), False).start())

        pl.when(z - k >= 0)(from_left)
        pl.when(z + k < nz)(from_right)

    def gather_drain(ch):
        for k in range(nz):
            for sub in range(2):
                pl.when((z - k >= 0) & has_r)(
                    lambda: wsend(ch, z - k, sub, wslab(ch, z - k, sub), True).wait_send())
                pl.when((z + k < nz) & has_l)(
                    lambda: wsend(ch, z + k, sub, wslab(ch, z + k, sub), False).wait_send())
        rc(wp.at[1 - y, :, pl.ds(ch * cols, cols)], wslab(ch, z, y), gy_s.at[ch], g_r.at[ch, z, y],
           y_n).wait_send()

    def osend(to_right):
        return rc(ow, ow, o_s.at[0 if to_right else 1], o_r.at[0], right if to_right else left)

    def o_own():
        def go():
            ow[...] = ow_own[...]
            pl.when(has_r)(lambda: rc(ow_own, ow, o_s.at[0], o_r.at[0], right).start())
            pl.when(has_l)(lambda: rc(ow_own, ow, o_s.at[1], o_r.at[0], left).start())
        pl.when(z == s)(go)

    def o_pass():
        def go():
            rc(ow, ow, o_r.at[0], o_r.at[0], core_n).wait_recv()
            pl.when((z > s) & has_r)(lambda: osend(True).start())
            pl.when((z < s) & has_l)(lambda: osend(False).start())
        pl.when(z != s)(go)

    def o_drain():
        pl.when((z >= s) & has_r)(lambda: osend(True).wait_send())
        pl.when((z <= s) & has_l)(lambda: osend(False).wait_send())

    def agather(inst, dst):
        ss, rr = ag_s.at[inst], ag_r.at[inst]

        def blk(yy, sq, i):
            return dst.at[2 * yy + i, pl.ds(pl.multiple_of(sq * own_len, 16), own_len)]

        sx, sp = (s + 2) % 4, s + 1 - 2 * c
        spx = (sp + 2) % 4

        def msg(n, block, dev):
            return rc(block, block, ss.at[n], rr.at[n], dev)

        mine = [blk(y, s, i) for i in range(2)]
        xs = [blk(y, sx, i) for i in range(2)]
        ys = [blk(1 - y, s, i) for i in range(2)]
        dg = [blk(1 - y, sx, i) for i in range(2)]
        sends = [msg(0, mine[0], x_n), msg(1, mine[1], x_n), msg(2, ys[1], x_n),
                 msg(3, mine[0], y_n), msg(4, mine[1], y_n), msg(5, xs[0], y_n)]
        sends += [msg(6 + i, mine[i], core_n) for i in range(2)]
        sends += [msg(8 + i, xs[i], core_n) for i in range(2)]
        sends += [msg(10 + i, ys[i], core_n) for i in range(2)]
        sends += [msg(12 + i, dg[i], core_n) for i in range(2)]
        recvs = [msg(0, xs[0], x_n), msg(1, xs[1], x_n), msg(2, dg[1], x_n),
                 msg(3, ys[0], y_n), msg(4, ys[1], y_n), msg(5, dg[0], y_n)]
        recvs += [msg(6 + i, blk(y, sp, i), core_n) for i in range(2)]
        recvs += [msg(8 + i, blk(y, spx, i), core_n) for i in range(2)]
        recvs += [msg(10 + i, blk(1 - y, sp, i), core_n) for i in range(2)]
        recvs += [msg(12 + i, blk(1 - y, spx, i), core_n) for i in range(2)]

        def begin():
            for n in (0, 4, 1, 3, 6, 7):
                sends[n].start()

        def relay():
            recvs[0].wait_recv()
            sends[5].start()
            recvs[4].wait_recv()
            sends[2].start()
            sends[8].start()
            sends[11].start()
            recvs[1].wait_recv()
            sends[9].start()
            recvs[3].wait_recv()
            sends[10].start()

        def finish():
            recvs[2].wait_recv()
            sends[13].start()
            recvs[5].wait_recv()
            sends[12].start()
            for n in range(6, 14):
                recvs[n].wait_recv()

        def drain():
            for m in sends:
                m.wait_send()

        return begin, relay, finish, drain

    def rscatter(inst, pt, ra, bufs, produce):
        bdx, bdy, brx, bry = bufs
        ss, rr = rs_s.at[inst], rs_r.at[inst]
        xo = 1 - x

        def image(it):
            return (2 * (1 - y) + it) % 4

        def rows(xx, cc):
            return pl.ds(pl.multiple_of((2 * xx + cc) * own_len, 16), own_len)

        def swap(it, xx):
            img = image(it)
            return rc(pt.at[img, rows(xx, 1 - c)], ra.at[img, xx], ss.at[2 * it + xx],
                      rr.at[2 * it + xx], core_n)

        def run():
            def step(it, carry):
                produce(image(it))
                swap(it, xo).start()
                swap(it, x).start()
                return carry
            lax.fori_loop(0, nimg, step, 0)

            def add(it, xx):
                swap(it, xx).wait_recv()
                img = image(it)
                ra[img, xx] = (ra[img, xx].astype(F32) + pt[img, rows(xx, c)].astype(F32)).astype(BF16)
                return ra.at[img, xx]

            msgs = [
                (8, lambda: rc(ra.at[image(0), xo], bdx, ss.at[8], rr.at[8], x_n)),
                (9, lambda: rc(ra.at[image(1), xo], bdy, ss.at[9], rr.at[9], y_n)),
                (10, lambda: rc(ra.at[image(1), x], bry.at[1], ss.at[10], rr.at[10], y_n)),
                (11, lambda: rc(ra.at[image(2), xo], brx.at[0], ss.at[11], rr.at[11], x_n)),
                (12, lambda: rc(ra.at[image(0), x], bry.at[0], ss.at[12], rr.at[12], y_n)),
                (13, lambda: rc(ra.at[image(3), xo], brx.at[1], ss.at[13], rr.at[13], x_n)),
            ]
            m = [f() for _, f in msgs]
            add(0, xo)
            m[0].start()
            add(1, xo)
            m[1].start()
            add(1, x)
            m[2].start()
            add(2, xo)
            m[3].start()
            add(0, x)
            add(3, xo)
            m[0].wait_recv()
            ra[image(0), x] = (ra[image(0), x].astype(F32) + bdx[...].astype(F32)).astype(BF16)
            m[4].start()
            m[1].wait_recv()
            ra[image(3), xo] = (ra[image(3), xo].astype(F32) + bdy[...].astype(F32)).astype(BF16)
            m[5].start()
            add(2, x)
            add(3, x)

        def result(i):
            rc(brx.at[i], brx.at[i], ss.at[11 + 2 * i], rr.at[11 + 2 * i], x_n).wait_recv()
            rc(bry.at[i], bry.at[i], ss.at[12 - 2 * i], rr.at[12 - 2 * i], y_n).wait_recv()
            return (ra[image(2 + i), x].astype(F32) + brx[i].astype(F32)) + bry[i].astype(F32)

        def drain():
            for it in range(nimg):
                swap(it, 0).wait_send()
                swap(it, 1).wait_send()
            for n in range(8, 14):
                rc(bdx, bdx, ss.at[n], rr.at[n], x_n).wait_send()

        return run, result, drain

    gather_swap(0)
    gather_own(0)
    o_own()
    ag_x = agather(0, xall)
    ag_c = agather(1, call)
    for i in range(2):
        xall[2 * y + i, pl.ds(pl.multiple_of(s * own_len, 16), own_len)] = tok[i]
        call[2 * y + i, pl.ds(pl.multiple_of(s * own_len, 16), own_len)] = cot_in[i]
    ag_x[0]()
    gather_other(0)
    ag_x[1]()
    gather_hop(0, 1)
    gather_swap(1)
    gather_swap(2)
    ag_c[0]()
    ag_x[2]()
    gather_hop(0, 2)
    o_pass()
    gather_own(1)
    gather_other(1)
    ag_c[1]()
    ag_c[2]()
    gather_hop(0, 3)

    lane = lax.broadcasted_iota(jnp.int32, (1, cols), 1)
    vt = jnp.transpose(w[:, 0:128].astype(F32), (1, 0))
    vecs[...] = vt[0:8]
    qb = pltpu.roll(vecs[...], (VEC - rank * qw + width) % width, 1)[2:3, :cols]
    vb = pltpu.roll(vecs[...], (VEC + 2 * qw - rank * qw + width) % width, 1)[3:4, :cols]
    qkv_bias = jnp.where((lane >= VEC) & (lane < VEC + qw), qb, 0.0) + jnp.where(
        (lane >= VEC + 2 * qw) & (lane < VEC + 3 * qw), vb, 0.0)
    g1, s1 = vecs[0:1], vecs[1:2]
    o_b, g2, s2, out_b = vecs[4:5], vecs[5:6], vecs[6:7], vecs[7:8]

    def ln1_step(b, carry):
        img, r = b // 4, pl.ds(pl.multiple_of((b % 4) * 64, 64), 64)
        hat, _ = normalize(xall[img, r].astype(F32))
        n1[img, r] = (hat * g1 + s1).astype(BF16)
        return carry
    lax.fori_loop(0, 4 * nimg, ln1_step, 0)

    def att_step(img, carry):
        proj = dot(n1[img], w[:, 0:cols], 1, 0) + qkv_bias
        proj = proj.astype(BF16)
        qkv[img] = proj
        outs = []
        for h in range(2):
            at = VEC + h * HEAD_DIM
            q = proj[:, at : at + HEAD_DIM]
            k = proj[:, qw + at : qw + at + HEAD_DIM]
            v = proj[:, 2 * qw + at : 2 * qw + at + HEAD_DIM]
            sc = dot(q, k, 1, 1) * factor
            e = jnp.exp(sc - jnp.max(sc, axis=-1, keepdims=True))
            p = e / jnp.sum(e, axis=-1, keepdims=True)
            probs[img, h] = p
            outs.append(dot(p.astype(BF16), v, 1, 0).astype(BF16))
        mix[img] = jnp.concatenate(outs, axis=1)
        return carry
    lax.fori_loop(0, nimg, att_step, 0)

    gather_hop(1, 1)
    gather_own(2)
    gather_other(2)
    gather_hop(1, 2)

    def o_part(img):
        part[img] = dot(mix[img], ow[...], 1, 0).astype(BF16)

    rs_h = rscatter(0, part, r1, (dx, dy, rx, ry), o_part)
    rs_h[0]()
    rs_h[2]()
    ag_n = agather(2, n2)
    for i in range(2):
        hidden = tok[i].astype(F32) + rs_h[1](i) + o_b
        hid_s[i] = hidden
        hat, inv = normalize(hidden)
        hat2_s[i] = hat
        inv2_s[i] = jnp.broadcast_to(inv, (own_len, 128))
        n2[2 * y + i, pl.ds(pl.multiple_of(s * own_len, 16), own_len)] = (hat * g2 + s2).astype(BF16)
    ag_n[0]()
    gather_hop(1, 3)
    gather_hop(2, 1)
    ag_n[1]()
    ag_n[2]()
    gather_hop(2, 2)

    wlane = lax.broadcasted_iota(jnp.int32, (1, win), 1)
    valid = (wlane >= off_out) & (wlane < off_out + ffp)

    def in_step(img, carry):
        pre = dot(n2[img], w[:, in_win : in_win + win], 1, 0) + inb[0:1]
        a, sl = gelu_parts(pre)
        act[img] = jnp.where(valid, pltpu.roll(a, shift, 1), 0.0).astype(BF16)
        slope[img] = jnp.where(valid, pltpu.roll(sl, shift, 1), 0.0)
        return carry
    lax.fori_loop(0, nimg, in_step, 0)

    def rb_at(ch, slot, sub):
        return rb.at[ch, slot, sub]

    def gslab(ch, dest, sub):
        return g.at[wrows(dest, sub), pl.ds(ch * cols, cols)]

    def zsend(ch, k, sub, to_right):
        dest = z + k if to_right else z - k
        slot = nz if k == 1 and not to_right else dest
        return rc(gslab(ch, dest, sub), rb_at(ch, slot, sub), z_s.at[ch, dest, sub], z_r.at[ch, slot, sub],
                  right if to_right else left)

    def zadd(ch, dest, slot, sub):
        rc(rb_at(ch, slot, sub), rb_at(ch, slot, sub), z_r.at[ch, slot, sub], z_r.at[ch, slot, sub],
           core_n).wait_recv()
        r, cs = wrows(dest, sub), slice(ch * cols, (ch + 1) * cols)
        g[r, cs] = (g[r, cs].astype(F32) + rb[ch, slot, sub].astype(F32)).astype(BF16)

    def zreduce_hop(ch, k):
        def to_right():
            for sub in range(2):
                pl.when(has_l)(lambda: zadd(ch, z + k, z + k, sub))
                zsend(ch, k, sub, True).start()

        def to_left():
            for sub in range(2):
                pl.when(has_r)(lambda: zadd(ch, z - k, z - k, sub))
                zsend(ch, k, sub, False).start()

        pl.when(z + k < nz)(to_right)
        pl.when(z - k >= 0)(to_left)

    def zreduce_own(ch):
        for sub in range(2):
            pl.when(has_l)(lambda: zadd(ch, z, z, sub))
            pl.when(has_r)(lambda: zadd(ch, z, nz, sub))

    def zdrain(ch):
        for k in range(1, nz):
            for sub in range(2):
                pl.when(z + k < nz)(lambda: zsend(ch, k, sub, True).wait_send())
                pl.when(z - k >= 0)(lambda: zsend(ch, k, sub, False).wait_send())

    def fslot(ch, first, n):
        return fgrad.at[pl.ds(first, n), :, pl.ds(ch * cols, cols)]

    def f_swap(ch):
        src = g.at[wrows(z, 1 - y), pl.ds(ch * cols, cols)]
        return rc(src, fgrad.at[rank, :, pl.ds(ch * cols, cols)], f_s.at[ch, 0], f_r.at[ch, 0], y_n)

    def f_msg(ch, n, first, dev):
        return rc(fslot(ch, first, 2), fslot(ch, first, 2), f_s.at[ch, n], f_r.at[ch, n], dev)

    def f_begin(ch):
        f_swap(ch).start()
        fgrad[rank, :, ch * cols : (ch + 1) * cols] = g[wrows(z, y), ch * cols : (ch + 1) * cols]

    def f_spread(ch):
        other = fgrad.at[2 * s + 1 - y, :, pl.ds(ch * cols, cols)]
        rc(other, other, f_s.at[ch, 0], f_r.at[ch, 0], y_n).wait_recv()
        f_msg(ch, 1, 2 * s, x_n).start()
        f_msg(ch, 2, 2 * s, core_n).start()

    def f_relay(ch):
        sx = (s + 2) % 4
        f_msg(ch, 1, 2 * sx, x_n).wait_recv()
        f_msg(ch, 3, 2 * sx, core_n).start()

    def f_end(ch):
        sp = s + 1 - 2 * c
        f_msg(ch, 2, 2 * sp, core_n).wait_recv()
        f_msg(ch, 3, 2 * ((sp + 2) % 4), core_n).wait_recv()
        f_swap(ch).wait_send()
        for n in (1, 2, 3):
            f_msg(ch, n, 0, core_n).wait_send()

    rtile = width // 3

    def gout_step(t, carry):
        r = pl.ds(pl.multiple_of(t * rtile, rtile), rtile)
        acc = jnp.zeros((rtile, win), F32)
        for img in range(nimg):
            acc = acc + dot(call[img, :, r], act[img], 0, 0)
        gout_tail[r] = acc[:, 0 : 2 * cols - out_win].astype(BF16)
        g[r, 2 * cols : 3 * cols] = acc[:, 2 * cols - out_win :].astype(BF16)
        return carry
    lax.fori_loop(0, 3, gout_step, 0)
    for k in range(nz - 1, 0, -1):
        pl.when(z == 0)(lambda: zreduce_hop(2, k))
        pl.when(z == nz - 1)(lambda: zreduce_hop(2, k))
    gather_hop(2, 3)

    def out_part(img):
        part2[img] = dot(act[img], w[:, out_win : out_win + win], 1, 1).astype(BF16)

    rs_o = rscatter(1, part2, r1b, (dxb, dyb, rxb, ryb), out_part)

    def gp_step(img, carry):
        ga = dot(call[img], w[:, out_win : out_win + win], 1, 0) * slope[img]
        ga = pltpu.roll(ga, win - shift, 1)
        gp[img] = ga.astype(BF16)
        return carry
    lax.fori_loop(0, nimg, gp_step, 0)

    ib = jnp.zeros((1, win), F32)
    for img in range(nimg):
        ib = ib + jnp.sum(gp[img].astype(F32), axis=0, keepdims=True)
    isb[0] = jnp.broadcast_to(ib, (8, win))

    def gn2_part(img):
        part[img] = dot(gp[img], w[:, in_win : in_win + win], 1, 1).astype(BF16)

    rs_g2 = rscatter(2, part, r1, (dx, dy, rx, ry), gn2_part)
    rs_g2[0]()

    def gin_step(t, carry):
        r = pl.ds(pl.multiple_of(t * rtile, rtile), rtile)
        acc = jnp.zeros((rtile, win), F32)
        for img in range(nimg):
            acc = acc + dot(n2[img, :, r], gp[img], 0, 0)
        lo = cols - in_win
        gin_tail[r] = acc[:, 0:lo].astype(BF16)
        g[r, cols : 2 * cols - 128] = acc[:, lo : win - 128].astype(BF16)
        g[r, 2 * cols - 128 : 2 * cols] = (acc[:, win - 128 :] + gout_tail[r].astype(F32)).astype(BF16)
        return carry
    lax.fori_loop(0, 3, gin_step, 0)

    def z_middle(ch, k):
        pl.when((z > 0) & (z < nz - 1))(lambda: zreduce_hop(ch, k))

    def z_ends(ch):
        for k in range(nz - 1, 0, -1):
            pl.when((z == 0) | (z == nz - 1))(lambda: zreduce_hop(ch, k))

    z_ends(1)
    sums = [jnp.zeros((1, width), F32) for _ in range(6)]
    ag_g = agather(3, gb)
    for i in range(2):
        gn2 = rs_g2[1](i)
        hat = hat2_s[i]
        sums[2] = sums[2] + jnp.sum(gn2 * hat, axis=0, keepdims=True)
        sums[3] = sums[3] + jnp.sum(gn2, axis=0, keepdims=True)
        up = cot_in[i].astype(F32)
        gh = up + norm_back(gn2, g2, hat, inv2_s[i][:, 0:1])
        gh_s[i] = gh
        low = gh.astype(BF16)
        gb[2 * y + i, pl.ds(pl.multiple_of(s * own_len, 16), own_len)] = low
        sums[4] = sums[4] + jnp.sum(low.astype(F32), axis=0, keepdims=True)
        sums[5] = sums[5] + jnp.sum(up, axis=0, keepdims=True)
    rs_g2[2]()
    ag_g[0]()
    z_middle(2, 2)
    z_middle(2, 1)
    ag_g[1]()
    rs_o[0]()
    ag_g[2]()
    zreduce_own(2)
    f_begin(2)
    z_middle(1, 2)
    z_middle(1, 1)

    def attb_step(img, carry):
        proj, gbi = qkv[img], gb[img]
        gmix = dot(gbi, ow[...], 1, 1).astype(BF16)
        zero = jnp.zeros((length, VEC), BF16)
        dq, dk, dv = [], [], []
        for h in range(2):
            at = VEC + h * HEAD_DIM
            q = proj[:, at : at + HEAD_DIM]
            k = proj[:, qw + at : qw + at + HEAD_DIM]
            v = proj[:, 2 * qw + at : 2 * qw + at + HEAD_DIM]
            gm = gmix[:, h * HEAD_DIM : (h + 1) * HEAD_DIM]
            p = probs[img, h]
            gpr = dot(gm, v, 1, 1)
            gs = (p * (gpr - jnp.sum(p * gpr, axis=-1, keepdims=True))).astype(BF16)
            dq.append((dot(gs, k, 1, 0) * factor).astype(BF16))
            dk.append((dot(gs, q, 0, 0) * factor).astype(BF16))
            dv.append(dot(p.astype(BF16), gm, 0, 0).astype(BF16))
        pad = jnp.zeros((length, cols - VEC - 3 * qw), BF16)
        dqkv[img] = jnp.concatenate([zero] + dq + dk + dv + [pad], axis=1)
        return carry
    lax.fori_loop(0, nimg, attb_step, 0)

    vsum[0:2] = jnp.zeros((2, width), F32)

    def gn1_part(img):
        pr = dot(dqkv[img], w[:, 0:cols], 1, 1)
        hat, _ = normalize(xall[img].astype(F32))
        vsum[0:1] = vsum[0:1] + jnp.sum(pr * hat, axis=0, keepdims=True)
        vsum[1:2] = vsum[1:2] + jnp.sum(pr, axis=0, keepdims=True)
        part[img] = pr.astype(BF16)

    rs_g1 = rscatter(3, part, r1, (dx, dy, rx, ry), gn1_part)
    rs_g1[0]()
    for n in range(2, 6):
        vsum[n : n + 1] = sums[n]
    vsum[6:8] = jnp.zeros((2, width), F32)

    def gqkv_step(t, carry):
        r = pl.ds(pl.multiple_of(t * rtile, rtile), rtile)
        acc = jnp.zeros((rtile, cols), F32)
        for img in range(nimg):
            acc = acc + dot(n1[img, :, r], dqkv[img], 0, 0)
        vcol = jnp.transpose(jnp.concatenate([vsum[:, r], jnp.zeros((120, rtile), F32)], axis=0), (1, 0))
        g[r, 0:128] = (acc[:, 0:128] + vcol).astype(BF16)
        g[r, 128 : cols - 128] = acc[:, 128 : cols - 128].astype(BF16)
        g[r, cols - 128 : cols] = (acc[:, cols - 128 :] + gin_tail[r].astype(F32)).astype(BF16)
        return carry
    lax.fori_loop(0, 3, gqkv_step, 0)
    z_ends(0)

    gacc = jnp.zeros((qw, width), F32)
    for img in range(nimg):
        gacc = gacc + dot(mix[img], gb[img], 0, 0)
    og[0:qw] = gacc.astype(BF16)
    bsum = jnp.zeros((1, cols), F32)
    for img in range(nimg):
        bsum = bsum + jnp.sum(dqkv[img].astype(F32), axis=0, keepdims=True)
    og[qw:, 0:cols] = jnp.broadcast_to(bsum, (16, cols)).astype(BF16)
    og[qw:, cols:] = jnp.zeros((16, width - cols), BF16)

    def zo_send(to_right):
        n = 0 if to_right else 1
        return rc(og, rbo.at[n], zo_s.at[n], zo_r.at[n], right if to_right else left)

    def zo_add(n):
        rc(rbo.at[n], rbo.at[n], zo_s.at[n], zo_r.at[n], core_n).wait_recv()
        og[...] = (og[...].astype(F32) + rbo[n].astype(F32)).astype(BF16)

    pl.when((z == 0) & (z < s))(lambda: zo_send(True).start())
    pl.when((z == nz - 1) & (z > s))(lambda: zo_send(False).start())

    def ib_send(to_right):
        n = 0 if to_right else 1
        return rc(isb.at[1 + n], ibx.at[n], ib_s.at[n], ib_r.at[n], right if to_right else left)

    def ib_recv(n):
        rc(ibx.at[n], ibx.at[n], ib_s.at[n], ib_r.at[n], core_n).wait_recv()

    def ib_first():
        isb[1] = isb[0]
        isb[2] = isb[0]
    ib_first()
    pl.when(z == 0)(lambda: ib_send(True).start())
    pl.when(z == nz - 1)(lambda: ib_send(False).start())

    f_spread(2)
    zreduce_own(1)
    f_begin(1)
    f_relay(2)
    z_middle(0, 2)
    z_middle(0, 1)

    def zo_mid_r():
        zo_add(0)
        zo_send(True).start()

    def zo_mid_l():
        zo_add(1)
        zo_send(False).start()
    pl.when((z > 0) & (z < s))(zo_mid_r)
    pl.when((z < nz - 1) & (z > s))(zo_mid_l)

    def ib_mid(n):
        ib_recv(n)
        isb[1 + n] = isb[0] + ibx[n]
        pl.when((has_r if n == 0 else has_l))(lambda: ib_send(n == 0).start())
    pl.when(has_l)(lambda: ib_mid(0))
    pl.when(has_r)(lambda: ib_mid(1))

    for i in range(2):
        gn1 = rs_g1[1](i)
        hat, inv = normalize(tok[i].astype(F32))
        gtok_ref[i] = (gh_s[i] + norm_back(gn1, g1, hat, inv)).astype(BF16)
        out_ref[i] = (hid_s[i] + rs_o[1](i) + out_b).astype(BF16)

    f_spread(1)

    def o_here():
        pl.when(has_l)(lambda: zo_add(0))
        pl.when(has_r)(lambda: zo_add(1))
        ograd[...] = og[...]
        rc(ograd, ograd, zo_s.at[2], zo_r.at[2], x_n).start()
        rc(ograd, ograd, zo_s.at[3], zo_r.at[3], core_n).start()
    pl.when(z == s)(o_here)

    isb[0] = (isb[1] + isb[2]) - isb[0]
    ibgrad[rank] = isb[0]
    rc(isb.at[0], ibgrad.at[rank], ib_s.at[2], ib_r.at[2], y_n).start()
    rc(isb.at[0], ibgrad.at[2 * s + 1 - y], ib_s.at[2], ib_r.at[2], y_n).wait_recv()

    def ib_two(n, first, dev):
        return rc(ibgrad.at[pl.ds(first, 2)], ibgrad.at[pl.ds(first, 2)], ib_s.at[n], ib_r.at[n], dev)
    ib_two(3, 2 * s, x_n).start()
    ib_two(4, 2 * s, core_n).start()
    ib_two(3, 2 * ((s + 2) % 4), x_n).wait_recv()
    ib_two(5, 2 * ((s + 2) % 4), core_n).start()

    f_relay(1)

    def o_x():
        rc(ograd, ograd, zo_s.at[2], zo_r.at[2], x_n).wait_recv()
        rc(ograd, ograd, zo_s.at[3], zo_r.at[3], core_n).start()
    pl.when((s + 2) % 4 == z)(o_x)
    pl.when((s + 1 - 2 * c == z) | ((s + 1 - 2 * c + 2) % 4 == z))(
        lambda: rc(ograd, ograd, zo_s.at[3], zo_r.at[3], core_n).wait_recv())

    zreduce_own(0)
    f_begin(0)
    f_spread(0)
    f_relay(0)

    for ch in range(3):
        gather_drain(ch)
        zdrain(ch)
        f_end(ch)
    o_drain()
    for a in (ag_x, ag_c, ag_n, ag_g):
        a[3]()
    rs_o[2]()
    rs_g1[2]()
    pl.when(z < s)(lambda: zo_send(True).wait_send())
    pl.when(z > s)(lambda: zo_send(False).wait_send())

    def o_out_done(n):
        rc(ograd, ograd, zo_s.at[n], zo_r.at[n], core_n).wait_send()
    pl.when(z == s)(lambda: o_out_done(2))
    pl.when((z == s) | ((s + 2) % 4 == z))(lambda: o_out_done(3))
    pl.when(has_r)(lambda: ib_send(True).wait_send())
    pl.when(has_l)(lambda: ib_send(False).wait_send())
    rc(isb.at[0], ibgrad.at[rank], ib_s.at[2], ib_r.at[2], y_n).wait_send()
    ib_two(4, 2 * (s + 1 - 2 * c), core_n).wait_recv()
    ib_two(5, 2 * ((s + 1 - 2 * c + 2) % 4), core_n).wait_recv()
    for n in (3, 4, 5):
        ib_two(n, 0, core_n).wait_send()


def layer_fast(
    tokens, cotangent, ln1_gain, ln1_shift, q_weight, q_bias, k_weight, v_weight, v_bias,
    o_weight, o_bias, ln2_gain, ln2_shift, in_weight, in_bias, out_weight, out_bias,
):
    sq, ns = lax.axis_index("seq"), lax.axis_size("seq")
    ndp = lax.axis_size("dp")
    nz, ranks = ndp // 2, 2 * ns
    images, own_len, width = tokens.shape
    ff = in_weight.shape[1]
    hid, ffp = width // ranks, ff // ranks
    rows = q_weight.shape[0]
    y = lax.axis_index("dp") % 2

    def two(mat, n):
        part = lax.dynamic_slice_in_dim(mat, sq * 2 * n, 2 * n, axis=1)
        return part.reshape(rows, 2, n).transpose(1, 0, 2)

    vec = jnp.stack([ln1_gain, ln1_shift, q_bias, v_bias, o_bias, ln2_gain, ln2_shift, out_bias], axis=1)
    out_rows = lax.dynamic_slice_in_dim(out_weight, sq * 2 * ffp, 2 * ffp, axis=0)
    wp = jnp.concatenate(
        [jnp.broadcast_to(vec, (2, rows, VEC)), two(q_weight, hid), two(k_weight, hid), two(v_weight, hid),
         two(in_weight, ffp), out_rows.reshape(2, ffp, rows).transpose(0, 2, 1)], axis=2)
    total = 3 * 512
    used = VEC + 3 * hid + 2 * ffp
    wp = jnp.pad(wp, ((0, 0), (0, 0), (0, total - used)))
    in_at = VEC + 3 * hid
    off_in = in_at % 128
    win = (ffp + 127) // 128 * 128
    inb = lax.dynamic_slice_in_dim(in_bias, (2 * sq + y) * ffp, ffp).astype(F32)
    inb = jnp.broadcast_to(jnp.pad(inb, (off_in, win - ffp - off_in)), (8, win))
    vmem = pl.BlockSpec(memory_space=pltpu.VMEM)
    nimg, length, cols = 2 * images, own_len * ns, 512
    tall = (nimg, length, width)
    half = (own_len, width)
    D = pltpu.SemaphoreType.DMA
    V = pltpu.VMEM
    scratch = dict(
        w=V((2 * nz * rows, total), BF16), ow=V((hid, width), BF16), xall=V(tall, BF16), call=V(tall, BF16),
        n1=V(tall, BF16), n2=V(tall, BF16), gb=V(tall, BF16), qkv=V((nimg, length, cols), BF16),
        probs=V((nimg, 2, length, length), F32), mix=V((nimg, length, hid), BF16),
        act=V((nimg, length, win), BF16), slope=V((nimg, length, win), F32), gp=V((nimg, length, win), BF16),
        part=V(tall, BF16), part2=V(tall, BF16), r1=V((nimg, 2) + half, BF16), r1b=V((nimg, 2) + half, BF16),
        dx=V(half, BF16), dy=V(half, BF16), rx=V((2,) + half, BF16), ry=V((2,) + half, BF16),
        dxb=V(half, BF16), dyb=V(half, BF16), rxb=V((2,) + half, BF16), ryb=V((2,) + half, BF16),
        hid_s=V((2,) + half, F32), hat2_s=V((2,) + half, F32), inv2_s=V((2, own_len, 128), F32),
        gh_s=V((2,) + half, F32), n2own=V((8, 128), BF16), gbown=V((8, 128), BF16), vecs=V((VEC, width), F32),
        g=V((2 * nz * rows, total), BF16), rb=V((3, nz + 1, 2, rows, cols), BF16),
        rbo=V((2, hid + 16, width), BF16), gin_tail=V((width, 128), BF16), gout_tail=V((width, 128), BF16),
        dqkv=V((nimg, length, cols), BF16), vsum=V((8, width), F32), ibx=V((2, 8, win), F32),
        isb=V((3, 8, win), F32), og=V((hid + 16, width), BF16),
        gy_s=D((3,)), gzr_s=D((3, nz, 2)), gzl_s=D((3, nz, 2)), g_r=D((3, nz, 2)), o_s=D((2,)), o_r=D((1,)),
        ag_s=D((4, 14)), ag_r=D((4, 14)), rs_s=D((4, 14)), rs_r=D((4, 14)), z_s=D((3, nz, 2)),
        z_r=D((3, nz + 1, 2)), zo_s=D((4,)), zo_r=D((4,)), f_s=D((3, 4)), f_r=D((3, 4)), ib_s=D((6,)),
        ib_r=D((6,)),
    )
    out, gtok, fg, og, ib = pl.pallas_call(
        functools.partial(layer_kernel, nz, hid, ffp),
        out_shape=(
            jax.ShapeDtypeStruct(tokens.shape, BF16), jax.ShapeDtypeStruct(tokens.shape, BF16),
            jax.ShapeDtypeStruct((ranks, rows, total), BF16), jax.ShapeDtypeStruct((hid + 16, width), BF16),
            jax.ShapeDtypeStruct((ranks, 8, win), F32),
        ),
        in_specs=[vmem] * 5,
        out_specs=[vmem] * 5,
        scratch_shapes=list(scratch.values()),
        compiler_params=pltpu.CompilerParams(
            collective_id=0, has_side_effects=True, vmem_limit_bytes=64000 * 1024),
    )(wp, o_weight, tokens, cotangent, inb)
    f = fg.astype(F32)

    def spread(lo, n):
        return f[:, :, lo : lo + n].transpose(1, 0, 2).reshape(rows, ranks * n)

    gq, gk, gv = [spread(VEC + i * hid, hid) for i in range(3)]
    gin = spread(in_at, ffp)
    gout = f[:, :, in_at + ffp : used].transpose(0, 2, 1).reshape(ff, rows)
    vs = jnp.sum(f[:, :, 0:VEC], axis=0)
    go = og[:hid].astype(F32)
    gqb = og[hid, VEC : VEC + hid].astype(F32)
    gvb = og[hid, VEC + 2 * hid : VEC + 3 * hid].astype(F32)
    gib = ib[:, 0, off_in : off_in + ffp].reshape(ff)
    return (out, gtok, vs[:, 0], vs[:, 1], gq, gqb, gk, gv, gvb, go, vs[:, 4], vs[:, 2], vs[:, 3], gin, gib,
            gout, vs[:, 5])


def mm(a, b, ca, cb):
    return lax.dot_general(a, b, (((ca,), (cb,)), ((), ())), preferred_element_type=F32)


def on_device(
    tokens, cotangent, ln1_gain, ln1_shift, q_weight, q_bias, k_weight, v_weight, v_bias,
    o_weight, o_bias, ln2_gain, ln2_shift, in_weight, in_bias, out_weight, out_bias,
):
    part = lax.axis_index("seq")
    parts = lax.axis_size("seq")
    groups = lax.axis_size("dp")
    images, own_len, width = tokens.shape
    ff = in_weight.shape[1]
    hid = width // parts
    ffp = ff // parts
    heads = HEADS // parts
    length = own_len * parts
    rows = images * length

    def cols(w, n):
        return lax.dynamic_slice_in_dim(w, part * n, n, axis=1)

    vecs = jnp.stack(
        [ln1_gain, ln1_shift, q_bias, v_bias, o_bias, ln2_gain, ln2_shift, out_bias]
    )
    vecs = lax.all_gather(vecs, "dp", axis=1, tiled=True).astype(F32)
    g1, s1, qb, vb, ob, g2, s2, outb = [vecs[i] for i in range(8)]
    x = lax.all_gather(tokens, "seq", axis=1, tiled=True).reshape(rows, width)
    cot = lax.all_gather(cotangent, "seq", axis=1, tiled=True).reshape(rows, width)
    qkv = jnp.concatenate([cols(q_weight, hid), cols(k_weight, hid), cols(v_weight, hid)], axis=1)
    qkv = lax.all_gather(qkv, "dp", axis=0, tiled=True)
    o_w = lax.all_gather(o_weight, "dp", axis=0, tiled=True)
    o_w = lax.dynamic_slice_in_dim(o_w, part * hid, hid, axis=0)
    in_w = lax.all_gather(cols(in_weight, ffp), "dp", axis=0, tiled=True)
    out_w = lax.dynamic_slice_in_dim(out_weight, part * ffp, ffp, axis=0)
    out_w = lax.all_gather(out_w.T, "dp", axis=0, tiled=True)
    qb_own = lax.dynamic_slice_in_dim(qb, part * hid, hid)
    vb_own = lax.dynamic_slice_in_dim(vb, part * hid, hid)
    inb_own = lax.dynamic_slice_in_dim(in_bias, part * ffp, ffp).astype(F32)

    def scatter_tokens(partial):
        return lax.psum_scatter(
            partial.astype(BF16).reshape(images, length, width),
            "seq", scatter_dimension=1, tiled=True,
        ).astype(F32)

    hat1, _ = normalize(x.astype(F32))
    normed1 = (hat1 * g1 + s1).astype(BF16)
    proj = mm(normed1, qkv, 1, 0)
    queries = (proj[:, :hid] + qb_own).astype(BF16).reshape(images, length, heads, HEAD_DIM)
    keys = proj[:, hid : 2 * hid].astype(BF16).reshape(images, length, heads, HEAD_DIM)
    values = (proj[:, 2 * hid :] + vb_own).astype(BF16).reshape(images, length, heads, HEAD_DIM)
    factor = 1.0 / math.sqrt(HEAD_DIM)
    ein = lambda s, a, b: jnp.einsum(s, a, b, preferred_element_type=F32)
    scores = ein("iqhd,ikhd->ihqk", queries, keys) * factor
    top = jnp.max(scores, axis=-1, keepdims=True)
    expo = jnp.exp(scores - top)
    probs = expo / jnp.sum(expo, axis=-1, keepdims=True)
    probs_low = probs.astype(BF16)
    mixed = ein("ihqk,ikhd->iqhd", probs_low, values).astype(BF16).reshape(rows, hid)
    start = tokens.astype(F32)
    hidden = start + scatter_tokens(mm(mixed, o_w, 1, 0)) + ob
    hat2, r2 = normalize(hidden)
    normed2 = (hat2 * g2 + s2).astype(BF16)
    normed2 = lax.all_gather(normed2, "seq", axis=1, tiled=True).reshape(rows, width)
    pre = mm(normed2, in_w, 1, 0) + inb_own
    act, slope = gelu_parts(pre)
    act = act.astype(BF16)
    out = hidden + scatter_tokens(mm(act, out_w, 1, 1)) + outb
    d_out_w = mm(cot, act, 0, 0)
    cot_own = cotangent.astype(F32)
    grad_pre = (mm(cot, out_w, 1, 0) * slope).astype(BF16)
    d_in_w = mm(normed2, grad_pre, 0, 0)
    d_in_b = jnp.sum(grad_pre.astype(F32), axis=0)
    grad_n2 = scatter_tokens(mm(grad_pre, in_w, 1, 1))
    grad_hidden = cot_own + norm_back(grad_n2, g2, hat2, r2)
    branch_own = grad_hidden.astype(BF16)
    branch = lax.all_gather(branch_own, "seq", axis=1, tiled=True).reshape(rows, width)
    d_o_w = mm(mixed, branch, 0, 0)
    grad_mixed = mm(branch, o_w, 1, 1).astype(BF16).reshape(images, length, heads, HEAD_DIM)
    grad_probs = ein("iqhd,ikhd->ihqk", grad_mixed, values)
    row_dot = jnp.sum(probs * grad_probs, axis=-1, keepdims=True)
    grad_scores = (probs * (grad_probs - row_dot)).astype(BF16)
    grad_q = (ein("ihqk,ikhd->iqhd", grad_scores, keys) * factor).astype(BF16).reshape(rows, hid)
    grad_k = (ein("ihqk,iqhd->ikhd", grad_scores, queries) * factor).astype(BF16).reshape(rows, hid)
    grad_v = ein("ihqk,iqhd->ikhd", probs_low, grad_mixed).astype(BF16).reshape(rows, hid)
    grad_qkv = jnp.concatenate([grad_q, grad_k, grad_v], axis=1)
    d_qkv = mm(normed1, grad_qkv, 0, 0)
    d_qb = jnp.sum(grad_q.astype(F32), axis=0)
    d_vb = jnp.sum(grad_v.astype(F32), axis=0)
    grad_n1 = scatter_tokens(mm(grad_qkv, qkv, 1, 1))
    hat1o, r1o = normalize(start)
    grad_tokens = grad_hidden + norm_back(grad_n1, g1, hat1o, r1o)
    wide = jnp.concatenate([d_qkv, d_in_w, d_out_w], axis=1).astype(BF16)
    wide = lax.psum_scatter(wide, "dp", scatter_dimension=0, tiled=True)
    wide = lax.all_gather(wide, "seq", axis=0, tiled=False).astype(F32)

    def spread(lo, n):
        return wide[:, :, lo : lo + n].transpose(1, 0, 2).reshape(width // groups, n * parts)

    gq, gk, gv = [spread(i * hid, hid) for i in range(3)]
    gin = spread(3 * hid, ffp)
    gout = wide[:, :, 3 * hid + ffp :].transpose(0, 2, 1).reshape(ff, width // groups)
    o_full = lax.all_gather(
        lax.psum_scatter(d_o_w.astype(BF16), "dp", scatter_dimension=1, tiled=True),
        "seq", axis=0, tiled=True,
    )
    go = lax.all_to_all(o_full, "dp", split_axis=0, concat_axis=1, tiled=True).astype(F32)
    own_sums = jnp.stack([
        jnp.sum(grad_n1 * hat1o, axis=(0, 1)), jnp.sum(grad_n1, axis=(0, 1)),
        jnp.sum(grad_n2 * hat2, axis=(0, 1)), jnp.sum(grad_n2, axis=(0, 1)),
        jnp.sum(branch_own.astype(F32), axis=(0, 1)), jnp.sum(cot_own, axis=(0, 1)),
        lax.dynamic_update_slice_in_dim(jnp.zeros(width, F32), d_qb, part * hid, 0),
        lax.dynamic_update_slice_in_dim(jnp.zeros(width, F32), d_vb, part * hid, 0),
    ])
    bias_in = lax.dynamic_update_slice_in_dim(jnp.zeros(ff, F32), d_in_b, part * ffp, 0)
    total = lax.psum(jnp.concatenate([own_sums.reshape(-1), bias_in]), ("dp", "seq"))
    vec_part = total[: 8 * width].reshape(8, groups, width // groups)
    vec_part = lax.dynamic_index_in_dim(vec_part, lax.axis_index("dp"), axis=1, keepdims=False)
    bias_total = total[8 * width :]
    return (
        out.astype(BF16), grad_tokens.astype(BF16), vec_part[0], vec_part[1], gq, vec_part[6],
        gk, gv, vec_part[7], go, vec_part[4], vec_part[2], vec_part[3], gin, bias_total, gout,
        vec_part[5],
    )


def solution(mesh):
    fast = mesh.shape["dp"] == 2 * mesh.shape["seq"]
    rows, vec = P("dp", None), P("dp")
    tok = P("dp", "seq", None)
    return jax.shard_map(
        layer_fast if fast else on_device,
        mesh=mesh,
        in_specs=(tok, tok, vec, vec, rows, vec, rows, rows, vec, rows, vec, vec, vec, rows,
                  P(), P(None, "dp"), vec),
        out_specs=(tok, tok, vec, vec, rows, vec, rows, rows, vec, rows, vec, vec, vec, rows,
                   P(), P(None, "dp"), vec),
        check_vma=False,
    )
```

```python
import functools
import math

import jax
import jax.numpy as jnp
from jax import lax
from jax.experimental import pallas as pl
from jax.experimental.pallas import tpu as pltpu
from jax.sharding import PartitionSpec as P

BF16, F32 = jnp.bfloat16, jnp.float32
HEADS, HEAD_DIM = 16, 72
eps_norm = 1e-06
gelu_coef = 0.7978845608028654
gelu_cube = 0.044715
MESH = pl.DeviceIdType.MESH
VEC = 8


def normalize(values):
    row_mean = jnp.mean(values, axis=-1, keepdims=True)
    centred = values - row_mean
    inverse = lax.rsqrt(jnp.mean(centred * centred, axis=-1, keepdims=True) + eps_norm)
    return centred * inverse, inverse


def norm_back(grad_normed, gain_vec, scaled, inverse):
    grad_scaled = grad_normed * gain_vec
    centred_grad = grad_scaled - jnp.mean(grad_scaled, axis=-1, keepdims=True)
    return inverse * (
        centred_grad - scaled * jnp.mean(grad_scaled * scaled, axis=-1, keepdims=True)
    )


def gelu_parts(pre_act):
    tanh_val = jnp.tanh(gelu_coef * (pre_act + gelu_cube * pre_act * pre_act * pre_act))
    value_part = 0.5 * pre_act * (1.0 + tanh_val)
    slope_part = 0.5 * (1.0 + tanh_val) + 0.5 * pre_act * (
        1.0 - tanh_val * tanh_val
    ) * gelu_coef * (1.0 + 3.0 * gelu_cube * pre_act * pre_act)
    return value_part, slope_part


def dot(a, b, ca, cb):
    return lax.dot_general(a, b, (((ca,), (cb,)), ((), ())), preferred_element_type=F32)


def layer_kernel(
    nz, hid, ffp,
    wp, vin, ow_own, tok, cot_in, inb,
    out_ref, gtok_ref, q_out, k_out, v_out, in_out, out_out, o_out, vec_out, ib_out,
    fgrad, ograd, ibgrad, st_q, st_k, st_v, st_in, st_out, vslab,
    w, ow, xall, call, n1, n2, gb, qkv, probs, mix, act, slope, gp, part, part2, r1, r1b,
    dx, dy, rx, ry, dxb, dyb, rxb, ryb, hid_s, hat2_s, inv2_s, gh_s, vecs, g, rb, rbo, gin_tail,
    gout_tail, dqkv, vsum, ibx, isb, og, qbs, qbx,
    gy_s, gzr_s, gzl_s, g_r, o_s, o_r, ag_s, ag_r, rs_s, rs_r, z_s, z_r, zo_s, zo_r, f_s, f_r,
    ib_s, ib_r, qb_s, qb_r, v_s, v_r, st_s,
):
    d, s = lax.axis_index("dp"), lax.axis_index("seq")
    z, y = d // 2, d % 2
    x, c = s // 2, s % 2
    rank = 2 * s + y
    own_len = tok.shape[1]
    nimg, length, width = xall.shape
    rows8 = wp.shape[1]
    plane = 2 * rows8
    cols = 512
    qw = hid
    in_at = VEC + 3 * qw
    in_win = in_at // 128 * 128
    out_at = in_at + ffp
    out_win = out_at // 128 * 128
    win = (ffp + 127) // 128 * 128
    off_in, off_out = in_at - in_win, out_at - out_win
    shift = off_out - off_in
    core_n, x_n, y_n = (d, s + 1 - 2 * c), (d, (s + 2) % 4), (d + 1 - 2 * y, s)
    right, left = (d + 2, s), (d - 2, s)
    has_r, has_l = z < nz - 1, z > 0
    factor = 1.0 / math.sqrt(HEAD_DIM)

    def rc(src, dst, ss, rs, dev):
        return pltpu.make_async_remote_copy(
            src_ref=src, dst_ref=dst, send_sem=ss, recv_sem=rs, device_id=dev, device_id_type=MESH
        )

    barrier = pltpu.get_barrier_semaphore()
    column = [((d + 2 * k) % (2 * nz), s) for k in range(1, nz)]
    for dev in [core_n, x_n, y_n] + column:
        pl.semaphore_signal(barrier, inc=1, device_id=dev, device_id_type=MESH)
    pl.semaphore_wait(barrier, 3 + len(column))

    def wrows(origin, sub):
        return pl.ds(pl.multiple_of(origin * plane + sub * rows8, 16), rows8)

    def wslab(ch, origin, sub):
        return w.at[wrows(origin, sub), pl.ds(ch * cols, cols)]

    def wsend(ch, origin, sub, src, to_right):
        sems = gzr_s if to_right else gzl_s
        return rc(src, wslab(ch, origin, sub), sems.at[ch, origin, sub], g_r.at[ch, origin, sub],
                  right if to_right else left)

    def wrecv(ch, origin, sub):
        slab = wslab(ch, origin, sub)
        rc(slab, slab, g_r.at[ch, origin, sub], g_r.at[ch, origin, sub], core_n).wait_recv()

    def gather_own(ch):
        src = wp.at[y, :, pl.ds(ch * cols, cols)]
        pl.when(has_r)(lambda: wsend(ch, z, y, src, True).start())
        pl.when(has_l)(lambda: wsend(ch, z, y, src, False).start())
        w[wrows(z, y), ch * cols : (ch + 1) * cols] = wp[y, :, ch * cols : (ch + 1) * cols]

    def gather_swap(ch):
        rc(wp.at[1 - y, :, pl.ds(ch * cols, cols)], wslab(ch, z, y), gy_s.at[ch], g_r.at[ch, z, y],
           y_n).start()

    def gather_other(ch):
        wrecv(ch, z, 1 - y)
        src = wslab(ch, z, 1 - y)
        pl.when(has_r)(lambda: wsend(ch, z, 1 - y, src, True).start())
        pl.when(has_l)(lambda: wsend(ch, z, 1 - y, src, False).start())

    def gather_hop(ch, k):
        def from_left():
            for sub in range(2):
                wrecv(ch, z - k, sub)
                pl.when(has_r)(lambda: wsend(ch, z - k, sub, wslab(ch, z - k, sub), True).start())

        def from_right():
            for sub in range(2):
                wrecv(ch, z + k, sub)
                pl.when(has_l)(lambda: wsend(ch, z + k, sub, wslab(ch, z + k, sub), False).start())

        pl.when(z - k >= 0)(from_left)
        pl.when(z + k < nz)(from_right)

    def gather_hop1(ch, k, sub):
        def from_left():
            wrecv(ch, z - k, sub)
            pl.when(has_r)(lambda: wsend(ch, z - k, sub, wslab(ch, z - k, sub), True).start())

        def from_right():
            wrecv(ch, z + k, sub)
            pl.when(has_l)(lambda: wsend(ch, z + k, sub, wslab(ch, z + k, sub), False).start())

        pl.when(z - k >= 0)(from_left)
        pl.when(z + k < nz)(from_right)

    def gather_drain(ch):
        for k in range(nz):
            for sub in range(2):
                pl.when((z - k >= 0) & has_r)(
                    lambda: wsend(ch, z - k, sub, wslab(ch, z - k, sub), True).wait_send())
                pl.when((z + k < nz) & has_l)(
                    lambda: wsend(ch, z + k, sub, wslab(ch, z + k, sub), False).wait_send())
        rc(wp.at[1 - y, :, pl.ds(ch * cols, cols)], wslab(ch, z, y), gy_s.at[ch], g_r.at[ch, z, y],
           y_n).wait_send()

    def osend(to_right):
        return rc(ow, ow, o_s.at[0 if to_right else 1], o_r.at[0], right if to_right else left)

    def o_own():
        def go():
            ow[...] = ow_own[...]
            pl.when(has_r)(lambda: rc(ow_own, ow, o_s.at[0], o_r.at[0], right).start())
            pl.when(has_l)(lambda: rc(ow_own, ow, o_s.at[1], o_r.at[0], left).start())
        pl.when(z == s)(go)

    def o_pass(k):
        def go():
            rc(ow, ow, o_r.at[0], o_r.at[0], core_n).wait_recv()
            pl.when((z > s) & has_r)(lambda: osend(True).start())
            pl.when((z < s) & has_l)(lambda: osend(False).start())
        pl.when((z == s + k) | (z == s - k))(go)

    def o_drain():
        pl.when((z >= s) & has_r)(lambda: osend(True).wait_send())
        pl.when((z <= s) & has_l)(lambda: osend(False).wait_send())

    def agather(inst, dst):
        ss, rr = ag_s.at[inst], ag_r.at[inst]

        def blk(yy, sq, i):
            return dst.at[2 * yy + i, pl.ds(pl.multiple_of(sq * own_len, 16), own_len)]

        sx, sp = (s + 2) % 4, s + 1 - 2 * c
        spx = (sp + 2) % 4

        def msg(n, block, dev):
            return rc(block, block, ss.at[n], rr.at[n], dev)

        mine = [blk(y, s, i) for i in range(2)]
        xs = [blk(y, sx, i) for i in range(2)]
        ys = [blk(1 - y, s, i) for i in range(2)]
        dg = [blk(1 - y, sx, i) for i in range(2)]
        sends = [msg(0, mine[0], x_n), msg(1, mine[1], x_n), msg(2, ys[1], x_n),
                 msg(3, mine[0], y_n), msg(4, mine[1], y_n), msg(5, xs[0], y_n)]
        sends += [msg(6 + i, mine[i], core_n) for i in range(2)]
        sends += [msg(8 + i, xs[i], core_n) for i in range(2)]
        sends += [msg(10 + i, ys[i], core_n) for i in range(2)]
        sends += [msg(12 + i, dg[i], core_n) for i in range(2)]
        recvs = [msg(0, xs[0], x_n), msg(1, xs[1], x_n), msg(2, dg[1], x_n),
                 msg(3, ys[0], y_n), msg(4, ys[1], y_n), msg(5, dg[0], y_n)]
        recvs += [msg(6 + i, blk(y, sp, i), core_n) for i in range(2)]
        recvs += [msg(8 + i, blk(y, spx, i), core_n) for i in range(2)]
        recvs += [msg(10 + i, blk(1 - y, sp, i), core_n) for i in range(2)]
        recvs += [msg(12 + i, blk(1 - y, spx, i), core_n) for i in range(2)]

        def begin():
            for n in (0, 4, 1, 3, 6, 7):
                sends[n].start()

        def relay():
            recvs[0].wait_recv()
            sends[5].start()
            recvs[4].wait_recv()
            sends[2].start()
            sends[8].start()
            sends[11].start()
            recvs[1].wait_recv()
            sends[9].start()
            recvs[3].wait_recv()
            sends[10].start()

        def finish():
            recvs[2].wait_recv()
            sends[13].start()
            recvs[5].wait_recv()
            sends[12].start()
            for n in range(6, 14):
                recvs[n].wait_recv()

        def drain():
            for m in sends:
                m.wait_send()

        return begin, relay, finish, drain

    def rscatter(inst, pt, ra, bufs, produce):
        bdx, bdy, brx, bry = bufs
        ss, rr = rs_s.at[inst], rs_r.at[inst]
        xo = 1 - x

        def image(it):
            return (2 * (1 - y) + it) % 4

        def rows(xx, cc):
            return pl.ds(pl.multiple_of((2 * xx + cc) * own_len, 16), own_len)

        def swap(it, xx):
            img = image(it)
            return rc(pt.at[img, rows(xx, 1 - c)], ra.at[img, xx], ss.at[2 * it + xx],
                      rr.at[2 * it + xx], core_n)

        def run():
            def step(it, carry):
                produce(image(it))
                swap(it, xo).start()
                swap(it, x).start()
                return carry
            lax.fori_loop(0, nimg, step, 0)

            def add(it, xx):
                swap(it, xx).wait_recv()
                img = image(it)
                ra[img, xx] = (ra[img, xx].astype(F32) + pt[img, rows(xx, c)].astype(F32)).astype(BF16)
                return ra.at[img, xx]

            msgs = [
                (8, lambda: rc(ra.at[image(0), xo], bdx, ss.at[8], rr.at[8], x_n)),
                (9, lambda: rc(ra.at[image(1), xo], bdy, ss.at[9], rr.at[9], y_n)),
                (10, lambda: rc(ra.at[image(1), x], bry.at[1], ss.at[10], rr.at[10], y_n)),
                (11, lambda: rc(ra.at[image(2), xo], brx.at[0], ss.at[11], rr.at[11], x_n)),
                (12, lambda: rc(ra.at[image(0), x], bry.at[0], ss.at[12], rr.at[12], y_n)),
                (13, lambda: rc(ra.at[image(3), xo], brx.at[1], ss.at[13], rr.at[13], x_n)),
            ]
            m = [f() for _, f in msgs]
            add(0, xo)
            m[0].start()
            add(1, xo)
            m[1].start()
            add(1, x)
            m[2].start()
            add(2, xo)
            m[3].start()
            add(0, x)
            add(3, xo)
            m[0].wait_recv()
            ra[image(0), x] = (ra[image(0), x].astype(F32) + bdx[...].astype(F32)).astype(BF16)
            m[4].start()
            m[1].wait_recv()
            ra[image(3), xo] = (ra[image(3), xo].astype(F32) + bdy[...].astype(F32)).astype(BF16)
            m[5].start()
            add(2, x)
            add(3, x)

        def result(i):
            rc(brx.at[i], brx.at[i], ss.at[11 + 2 * i], rr.at[11 + 2 * i], x_n).wait_recv()
            rc(bry.at[i], bry.at[i], ss.at[12 - 2 * i], rr.at[12 - 2 * i], y_n).wait_recv()
            return (ra[image(2 + i), x].astype(F32) + brx[i].astype(F32)) + bry[i].astype(F32)

        def drain():
            for it in range(nimg):
                swap(it, 0).wait_send()
                swap(it, 1).wait_send()
            for n in range(8, 14):
                rc(bdx, bdx, ss.at[n], rr.at[n], x_n).wait_send()

        return run, result, drain

    def rb_at(ch, slot, sub):
        return rb.at[ch, slot, sub]

    def gslab(ch, dest, sub):
        return g.at[wrows(dest, sub), pl.ds(ch * cols, cols)]

    def zsend(ch, k, sub, to_right):
        dest = z + k if to_right else z - k
        slot = nz if k == 1 and not to_right else dest
        return rc(gslab(ch, dest, sub), rb_at(ch, slot, sub), z_s.at[ch, dest, sub], z_r.at[ch, slot, sub],
                  right if to_right else left)

    def zadd(ch, dest, slot, sub):
        rc(rb_at(ch, slot, sub), rb_at(ch, slot, sub), z_r.at[ch, slot, sub], z_r.at[ch, slot, sub],
           core_n).wait_recv()
        r, cs = wrows(dest, sub), slice(ch * cols, (ch + 1) * cols)
        g[r, cs] = (g[r, cs].astype(F32) + rb[ch, slot, sub].astype(F32)).astype(BF16)

    def zreduce_hop(ch, k):
        def to_right():
            for sub in range(2):
                pl.when(has_l)(lambda: zadd(ch, z + k, z + k, sub))
                zsend(ch, k, sub, True).start()

        def to_left():
            for sub in range(2):
                pl.when(has_r)(lambda: zadd(ch, z - k, z - k, sub))
                zsend(ch, k, sub, False).start()

        pl.when(z + k < nz)(to_right)
        pl.when(z - k >= 0)(to_left)

    def zreduce_own(ch):
        for sub in range(2):
            pl.when(has_l)(lambda: zadd(ch, z, z, sub))
            pl.when(has_r)(lambda: zadd(ch, z, nz, sub))

    def zdrain(ch):
        for k in range(1, nz):
            for sub in range(2):
                pl.when(z + k < nz)(lambda: zsend(ch, k, sub, True).wait_send())
                pl.when(z - k >= 0)(lambda: zsend(ch, k, sub, False).wait_send())

    def f_swap(ch):
        src = g.at[wrows(z, 1 - y), pl.ds(ch * cols, cols)]
        return rc(src, fgrad.at[rank, :, pl.ds(ch * cols, cols)], f_s.at[ch, 0], f_r.at[ch, 0], y_n)

    def f_msg(ch, n, slot, dev):
        piece = fgrad.at[slot, :, pl.ds(ch * cols, cols)]
        return rc(piece, piece, f_s.at[ch, n], f_r.at[ch, n], dev)

    sx, sp = (s + 2) % 4, s + 1 - 2 * c
    spx = (sp + 2) % 4

    def f_begin(ch):
        f_swap(ch).start()
        fgrad[rank, :, ch * cols : (ch + 1) * cols] = g[wrows(z, y), ch * cols : (ch + 1) * cols]
        f_msg(ch, 1, rank, x_n).start()
        f_msg(ch, 3, rank, core_n).start()

    def f_spread(ch):
        other = 2 * s + 1 - y
        f_msg(ch, 0, other, y_n).wait_recv()
        f_msg(ch, 2, other, x_n).start()
        f_msg(ch, 4, other, core_n).start()

    def f_relay(ch):
        f_msg(ch, 1, 2 * sx + y, x_n).wait_recv()
        f_msg(ch, 5, 2 * sx + y, core_n).start()
        f_msg(ch, 2, 2 * sx + 1 - y, x_n).wait_recv()
        f_msg(ch, 6, 2 * sx + 1 - y, core_n).start()

    def f_end(ch):
        f_msg(ch, 3, 2 * sp + y, core_n).wait_recv()
        f_msg(ch, 4, 2 * sp + 1 - y, core_n).wait_recv()
        f_msg(ch, 5, 2 * spx + y, core_n).wait_recv()
        f_msg(ch, 6, 2 * spx + 1 - y, core_n).wait_recv()

    def f_drain(ch):
        f_swap(ch).wait_send()
        for n in range(1, 7):
            f_msg(ch, n, rank, core_n).wait_send()

    def z_middle(ch, k):
        pl.when((z > 0) & (z < nz - 1))(lambda: zreduce_hop(ch, k))

    def z_ends(ch):
        for k in range(nz - 1, 0, -1):
            pl.when((z == 0) | (z == nz - 1))(lambda: zreduce_hop(ch, k))

    def zo_send(to_right):
        n = 0 if to_right else 1
        return rc(og, rbo.at[n], zo_s.at[n], zo_r.at[n], right if to_right else left)

    def zo_add(n):
        rc(rbo.at[n], rbo.at[n], zo_s.at[n], zo_r.at[n], core_n).wait_recv()
        og[...] = (og[...].astype(F32) + rbo[n].astype(F32)).astype(BF16)

    def zo_mid_r():
        zo_add(0)
        zo_send(True).start()

    def zo_mid_l():
        zo_add(1)
        zo_send(False).start()

    def qb_send():
        return rc(qbs, qbx.at[z], qb_s.at[0], qb_r.at[z], (2 * s + y, s))

    def qb_begin():
        bsum = jnp.zeros((1, cols), F32)
        for img in range(nimg):
            bsum = bsum + jnp.sum(dqkv[img].astype(F32), axis=0, keepdims=True)
        qbs[...] = jnp.broadcast_to(bsum, (8, cols))
        pl.when(z != s)(lambda: qb_send().start())

    def o_here():
        pl.when(has_l)(lambda: zo_add(0))
        pl.when(has_r)(lambda: zo_add(1))
        total = qbs[...]
        for k in range(1, nz):
            zz = (z + k) % nz
            rc(qbs, qbx.at[zz], qb_s.at[0], qb_r.at[zz], core_n).wait_recv()
            total = total + qbx[zz]
        og[qw:, 0:cols] = jnp.concatenate([total, total], axis=0).astype(BF16)
        ograd[...] = og[...]
        rc(ograd, ograd, zo_s.at[2], zo_r.at[2], x_n).start()
        rc(ograd, ograd, zo_s.at[3], zo_r.at[3], core_n).start()

    def o_x():
        rc(ograd, ograd, zo_s.at[2], zo_r.at[2], x_n).wait_recv()
        rc(ograd, ograd, zo_s.at[3], zo_r.at[3], core_n).start()

    def o_end():
        pl.when((sp == z) | (spx == z))(
            lambda: rc(ograd, ograd, zo_s.at[3], zo_r.at[3], core_n).wait_recv())

    def o_out_done(n):
        rc(ograd, ograd, zo_s.at[n], zo_r.at[n], core_n).wait_send()

    def ib_send(k):
        return rc(isb, ibx.at[z], ib_s.at[k - 1], ib_r.at[z], ((d + 2 * k) % (2 * nz), s))

    def ib_begin():
        ib = jnp.zeros((1, win), F32)
        for img in range(nimg):
            ib = ib + jnp.sum(gp[img].astype(F32), axis=0, keepdims=True)
        isb[...] = jnp.broadcast_to(ib, (8, win))
        for k in range(1, nz):
            ib_send(k).start()

    def ib_msg(n, slot, dev):
        return rc(ibgrad.at[slot], ibgrad.at[slot], ib_s.at[n], ib_r.at[n], dev)

    def ib_pass():
        ibsum = isb[...]
        for k in range(1, nz):
            zz = (z + k) % nz
            rc(isb, ibx.at[zz], ib_s.at[0], ib_r.at[zz], core_n).wait_recv()
            ibsum = ibsum + ibx[zz]
        ibgrad[rank] = ibsum
        ib_msg(nz, rank, y_n).start()
        ib_msg(nz + 1, rank, x_n).start()
        ib_msg(nz + 3, rank, core_n).start()

    def ib_end():
        other = 2 * s + 1 - y
        ib_msg(nz, other, y_n).wait_recv()
        ib_msg(nz + 2, other, x_n).start()
        ib_msg(nz + 4, other, core_n).start()
        ib_msg(nz + 1, 2 * sx + y, x_n).wait_recv()
        ib_msg(nz + 5, 2 * sx + y, core_n).start()
        ib_msg(nz + 2, 2 * sx + 1 - y, x_n).wait_recv()
        ib_msg(nz + 6, 2 * sx + 1 - y, core_n).start()
        ib_msg(nz + 3, 2 * sp + y, core_n).wait_recv()
        ib_msg(nz + 4, 2 * sp + 1 - y, core_n).wait_recv()
        ib_msg(nz + 5, 2 * spx + y, core_n).wait_recv()
        ib_msg(nz + 6, 2 * spx + 1 - y, core_n).wait_recv()

    def vec_send(k):
        return rc(vin, vslab.at[y, z], v_s.at[k - 1], v_r.at[z], ((d + 2 * k) % (2 * nz), s))

    def vec_cross():
        return rc(vslab.at[y], vslab.at[y], v_s.at[nz - 1], v_r.at[nz], y_n)

    def vec_begin():
        for k in range(1, nz):
            vec_send(k).start()
        vslab[y, z] = vin[...]

    def vec_pass():
        for k in range(1, nz):
            zz = (z + k) % nz
            rc(vin, vslab.at[y, zz], v_s.at[0], v_r.at[zz], core_n).wait_recv()
        vec_cross().start()

    def vec_end():
        rc(vslab.at[1 - y], vslab.at[1 - y], v_s.at[0], v_r.at[nz], y_n).wait_recv()
        for zz in range(nz):
            for yy in range(2):
                at = (2 * zz + yy) * rows8
                vecs[:, at : at + rows8] = vslab[yy, zz].astype(F32)[0:VEC, 0:rows8]

    def vec_drain():
        for k in range(1, nz):
            vec_send(k).wait_send()
        vec_cross().wait_send()

    nrank = fgrad.shape[0]
    stores = [(st_q, q_out, 0), (st_k, k_out, 1), (st_v, v_out, 2), (st_in, in_out, 3),
              (st_out, out_out, 4), (ograd, o_out, 5)]

    def emit_out():
        for t in range(nrank):
            piece = fgrad[t, :, out_at : out_at + ffp].astype(F32)
            st_out[t * ffp : (t + 1) * ffp] = jnp.transpose(piece, (1, 0)).astype(BF16)
            st_in[:, t * ffp + cols - in_at : (t + 1) * ffp] = fgrad[t, :, cols : in_at + ffp]
        pltpu.make_async_copy(st_out, out_out, st_s.at[4]).start()

    def emit_rest():
        pltpu.make_async_copy(ograd, o_out, st_s.at[5]).start()
        for t in range(nrank):
            for n, st in enumerate((st_q, st_k, st_v)):
                st[:, t * qw : (t + 1) * qw] = fgrad[t, :, VEC + n * qw : VEC + (n + 1) * qw]
            st_in[:, t * ffp : t * ffp + cols - in_at] = fgrad[t, :, in_at:cols]
        for stage, dst, n in stores[:4]:
            pltpu.make_async_copy(stage, dst, st_s.at[n]).start()
        vcols = jnp.zeros((rows8, 128), F32)
        for t in range(nrank):
            vcols = vcols + fgrad[t, :, 0:128].astype(F32)
        vec_out[0:VEC] = jnp.transpose(vcols, (1, 0))[0:VEC]
        vec_out[6:7] = ograd[qw : qw + 8, VEC : VEC + qw].astype(F32)[0:1]
        vec_out[7:8] = ograd[qw : qw + 8, VEC + 2 * qw : VEC + 3 * qw].astype(F32)[0:1]
        for t in range(nrank):
            ib_out[0:1, t * ffp : (t + 1) * ffp] = ibgrad[t, 0:1, off_in : off_in + ffp]

    gather_swap(0)
    own_rows = pl.ds(pl.multiple_of(s * own_len, 16), own_len)
    for i in range(2):
        xall[2 * y + i, own_rows] = tok[i]
    ag_x = agather(0, xall)
    ag_c = agather(1, call)
    ag_x[0]()
    gather_own(0)
    vec_begin()
    for i in range(2):
        call[2 * y + i, own_rows] = cot_in[i]
    gather_other(0)
    o_own()
    gather_hop1(0, 1, y)
    vec_pass()
    ag_x[1]()
    gather_hop1(0, 1, 1 - y)
    gather_hop1(0, 2, y)
    o_pass(1)
    ag_x[2]()
    vec_end()
    g1, s1 = vecs[0:1], vecs[1:2]
    o_b, g2, s2, out_b = vecs[4:5], vecs[5:6], vecs[6:7], vecs[7:8]

    def ln1_step(b, carry):
        img, r = b // 4, pl.ds(pl.multiple_of((b % 4) * 64, 64), 64)
        hat, _ = normalize(xall[img, r].astype(F32))
        n1[img, r] = (hat * g1 + s1).astype(BF16)
        return carry

    gather_hop1(0, 2, 1 - y)
    o_pass(2)
    gather_own(1)
    gather_swap(1)
    ag_c[0]()
    lax.fori_loop(0, 4 * nimg, ln1_step, 0)
    gather_hop(0, 3)
    gather_other(1)

    lane = lax.broadcasted_iota(jnp.int32, (1, cols), 1)
    qb = pltpu.roll(vecs[...], (VEC - rank * qw + width) % width, 1)[2:3, :cols]
    vb = pltpu.roll(vecs[...], (VEC + 2 * qw - rank * qw + width) % width, 1)[3:4, :cols]
    qkv_bias = jnp.where((lane >= VEC) & (lane < VEC + qw), qb, 0.0) + jnp.where(
        (lane >= VEC + 2 * qw) & (lane < VEC + 3 * qw), vb, 0.0)

    def att_step(img, carry):
        proj = dot(n1[img], w[:, 0:cols], 1, 0) + qkv_bias
        proj = proj.astype(BF16)
        qkv[img] = proj
        outs = []
        for h in range(2):
            at = VEC + h * HEAD_DIM
            q = proj[:, at : at + HEAD_DIM]
            k = proj[:, qw + at : qw + at + HEAD_DIM]
            v = proj[:, 2 * qw + at : 2 * qw + at + HEAD_DIM]
            sc = dot(q, k, 1, 1) * factor
            e = jnp.exp(sc - jnp.max(sc, axis=-1, keepdims=True))
            p = e / jnp.sum(e, axis=-1, keepdims=True)
            probs[img, h] = p
            outs.append(dot(p.astype(BF16), v, 1, 0).astype(BF16))
        mix[img] = jnp.concatenate(outs, axis=1)
        return carry

    lax.fori_loop(0, 2, att_step, 0)
    ag_c[1]()
    gather_hop(1, 1)
    lax.fori_loop(2, nimg, att_step, 0)
    o_pass(3)
    ag_c[2]()
    gather_swap(2)

    def o_part(img):
        part[img] = dot(mix[img], ow[...], 1, 0).astype(BF16)

    rs_h = rscatter(0, part, r1, (dx, dy, rx, ry), o_part)
    rs_h[0]()
    gather_hop(1, 2)
    gather_own(2)
    gather_other(2)
    rs_h[2]()
    ag_n = agather(2, n2)
    for i in range(2):
        hidden = tok[i].astype(F32) + rs_h[1](i) + o_b
        hid_s[i] = hidden
        hat, inv = normalize(hidden)
        hat2_s[i] = hat
        inv2_s[i] = jnp.broadcast_to(inv, (own_len, 128))
        n2[2 * y + i, own_rows] = (hat * g2 + s2).astype(BF16)
    ag_n[0]()
    ag_n[1]()
    gather_hop(1, 3)
    gather_hop(2, 1)
    ag_n[2]()

    wlane = lax.broadcasted_iota(jnp.int32, (1, win), 1)
    valid = (wlane >= off_out) & (wlane < off_out + ffp)

    def in_step(img, carry):
        pre = dot(n2[img], w[:, in_win : in_win + win], 1, 0) + inb[0:1]
        a, sl = gelu_parts(pre)
        act[img] = jnp.where(valid, pltpu.roll(a, shift, 1), 0.0).astype(BF16)
        slope[img] = jnp.where(valid, pltpu.roll(sl, shift, 1), 0.0)
        return carry
    lax.fori_loop(0, 2, in_step, 0)
    gather_hop(2, 2)
    lax.fori_loop(2, nimg, in_step, 0)

    rtile = width // 3

    def gout_step(t, carry):
        r = pl.ds(pl.multiple_of(t * rtile, rtile), rtile)
        acc = jnp.zeros((rtile, win), F32)
        for img in range(nimg):
            acc = acc + dot(call[img, :, r], act[img], 0, 0)
        gout_tail[r] = acc[:, 0 : 2 * cols - out_win].astype(BF16)
        g[r, 2 * cols : 3 * cols] = acc[:, 2 * cols - out_win :].astype(BF16)
        return carry
    lax.fori_loop(0, 3, gout_step, 0)
    z_ends(2)
    gather_hop(2, 3)

    def gp_step(img, carry):
        ga = dot(call[img], w[:, out_win : out_win + win], 1, 0) * slope[img]
        gp[img] = pltpu.roll(ga, win - shift, 1).astype(BF16)
        return carry
    lax.fori_loop(0, nimg, gp_step, 0)

    def gn2_part(img):
        part[img] = dot(gp[img], w[:, in_win : in_win + win], 1, 1).astype(BF16)

    rs_g2 = rscatter(2, part, r1, (dx, dy, rx, ry), gn2_part)
    rs_g2[0]()
    z_middle(2, 2)

    def gin_step(t, carry):
        r = pl.ds(pl.multiple_of(t * rtile, rtile), rtile)
        acc = jnp.zeros((rtile, win), F32)
        for img in range(nimg):
            acc = acc + dot(n2[img, :, r], gp[img], 0, 0)
        lo = cols - in_win
        gin_tail[r] = acc[:, 0:lo].astype(BF16)
        g[r, cols : 2 * cols - 128] = acc[:, lo : win - 128].astype(BF16)
        g[r, 2 * cols - 128 : 2 * cols] = (acc[:, win - 128 :] + gout_tail[r].astype(F32)).astype(BF16)
        return carry

    sums = [jnp.zeros((1, width), F32) for _ in range(6)]
    ag_g = agather(3, gb)
    for i in range(2):
        gn2 = rs_g2[1](i)
        hat = hat2_s[i]
        sums[2] = sums[2] + jnp.sum(gn2 * hat, axis=0, keepdims=True)
        sums[3] = sums[3] + jnp.sum(gn2, axis=0, keepdims=True)
        up = cot_in[i].astype(F32)
        gh = up + norm_back(gn2, g2, hat, inv2_s[i][:, 0:1])
        gh_s[i] = gh
        low = gh.astype(BF16)
        gb[2 * y + i, own_rows] = low
        sums[4] = sums[4] + jnp.sum(low.astype(F32), axis=0, keepdims=True)
        sums[5] = sums[5] + jnp.sum(up, axis=0, keepdims=True)
    rs_g2[2]()
    ag_g[0]()
    for n in range(2, 6):
        vsum[n : n + 1] = sums[n]
    vsum[6:8] = jnp.zeros((2, width), F32)
    vsum[0:2] = jnp.zeros((2, width), F32)
    lax.fori_loop(0, 3, gin_step, 0)
    z_ends(1)
    ib_begin()
    ag_g[1]()
    z_middle(2, 1)
    ag_g[2]()

    gacc = jnp.zeros((qw, width), F32)
    for img in range(nimg):
        gacc = gacc + dot(mix[img], gb[img], 0, 0)
    og[0:qw] = gacc.astype(BF16)
    og[qw:] = jnp.zeros((16, width), BF16)
    pl.when((z == 0) & (z < s))(lambda: zo_send(True).start())
    pl.when((z == nz - 1) & (z > s))(lambda: zo_send(False).start())
    z_middle(1, 2)

    def attb_step(img, carry):
        proj, gbi = qkv[img], gb[img]
        gmix = dot(gbi, ow[...], 1, 1).astype(BF16)
        zero = jnp.zeros((length, VEC), BF16)
        dq, dk, dv = [], [], []
        for h in range(2):
            at = VEC + h * HEAD_DIM
            q = proj[:, at : at + HEAD_DIM]
            k = proj[:, qw + at : qw + at + HEAD_DIM]
            v = proj[:, 2 * qw + at : 2 * qw + at + HEAD_DIM]
            gm = gmix[:, h * HEAD_DIM : (h + 1) * HEAD_DIM]
            p = probs[img, h]
            gpr = dot(gm, v, 1, 1)
            gs = (p * (gpr - jnp.sum(p * gpr, axis=-1, keepdims=True))).astype(BF16)
            dq.append((dot(gs, k, 1, 0) * factor).astype(BF16))
            dk.append((dot(gs, q, 0, 0) * factor).astype(BF16))
            dv.append(dot(p.astype(BF16), gm, 0, 0).astype(BF16))
        pad = jnp.zeros((length, cols - VEC - 3 * qw), BF16)
        dqkv[img] = jnp.concatenate([zero] + dq + dk + dv + [pad], axis=1)
        pr = dot(dqkv[img], w[:, 0:cols], 1, 1)
        hat, _ = normalize(xall[img].astype(F32))
        vsum[0:1] = vsum[0:1] + jnp.sum(pr * hat, axis=0, keepdims=True)
        vsum[1:2] = vsum[1:2] + jnp.sum(pr, axis=0, keepdims=True)
        part[img] = pr.astype(BF16)
        return carry

    def gn1_part(img):
        pass
    rs_g1 = rscatter(3, part, r1, (dx, dy, rx, ry), gn1_part)

    def gqkv_step(t, carry):
        r = pl.ds(pl.multiple_of(t * rtile, rtile), rtile)
        acc = jnp.zeros((rtile, cols), F32)
        for img in range(nimg):
            acc = acc + dot(n1[img, :, r], dqkv[img], 0, 0)
        vcol = jnp.transpose(jnp.concatenate([vsum[:, r], jnp.zeros((120, rtile), F32)], axis=0), (1, 0))
        g[r, 0:128] = (acc[:, 0:128] + vcol).astype(BF16)
        g[r, 128 : cols - 128] = acc[:, 128 : cols - 128].astype(BF16)
        g[r, cols - 128 : cols] = (acc[:, cols - 128 :] + gin_tail[r].astype(F32)).astype(BF16)
        return carry

    lax.fori_loop(0, nimg, attb_step, 0)
    z_middle(1, 1)
    qb_begin()
    lax.fori_loop(0, 3, gqkv_step, 0)
    z_ends(0)
    zreduce_own(2)
    f_begin(2)
    rs_g1[0]()
    z_middle(0, 2)
    ib_pass()
    f_spread(2)
    pl.when((z == 1) & (z < s))(zo_mid_r)
    pl.when((z == nz - 2) & (z > s))(zo_mid_l)
    zreduce_own(1)
    f_begin(1)

    for i in range(2):
        gn1 = rs_g1[1](i)
        hat, inv = normalize(tok[i].astype(F32))
        gtok_ref[i] = (gh_s[i] + norm_back(gn1, g1, hat, inv)).astype(BF16)
    z_middle(0, 1)
    pl.when((z > 1) & (z < s))(zo_mid_r)
    pl.when((z < nz - 2) & (z > s))(zo_mid_l)
    f_relay(2)
    f_spread(1)

    def out_part(img):
        part2[img] = dot(act[img], w[:, out_win : out_win + win], 1, 1).astype(BF16)

    rs_o = rscatter(1, part2, r1b, (dxb, dyb, rxb, ryb), out_part)
    rs_o[0]()
    zreduce_own(0)
    f_begin(0)
    f_relay(1)
    pl.when(z == s)(o_here)
    f_spread(0)
    for i in range(2):
        out_ref[i] = (hid_s[i] + rs_o[1](i) + out_b).astype(BF16)
    ib_end()
    pl.when((s + 2) % 4 == z)(o_x)
    f_end(2)
    f_end(1)
    emit_out()
    f_relay(0)
    o_end()
    f_end(0)
    emit_rest()

    for ch in range(3):
        gather_drain(ch)
        zdrain(ch)
        f_drain(ch)
    o_drain()
    vec_drain()
    for a in (ag_x, ag_c, ag_n, ag_g):
        a[3]()
    rs_o[2]()
    rs_g1[2]()
    pl.when(z < s)(lambda: zo_send(True).wait_send())
    pl.when(z > s)(lambda: zo_send(False).wait_send())
    pl.when(z == s)(lambda: o_out_done(2))
    pl.when((z == s) | ((s + 2) % 4 == z))(lambda: o_out_done(3))
    pl.when(z != s)(lambda: qb_send().wait_send())
    for k in range(1, nz):
        ib_send(k).wait_send()
    for n in range(7):
        ib_msg(nz + n, rank, core_n).wait_send()
    for stage, dst, n in stores:
        pltpu.make_async_copy(stage, dst, st_s.at[n]).wait()


def layer_fast(
    tokens, cotangent, ln1_gain, ln1_shift, q_weight, q_bias, k_weight, v_weight, v_bias,
    o_weight, o_bias, ln2_gain, ln2_shift, in_weight, in_bias, out_weight, out_bias,
):
    sq, ns = lax.axis_index("seq"), lax.axis_size("seq")
    ndp = lax.axis_size("dp")
    nz, ranks = ndp // 2, 2 * ns
    images, own_len, width = tokens.shape
    ff = in_weight.shape[1]
    hid, ffp = width // ranks, ff // ranks
    rows = q_weight.shape[0]
    y = lax.axis_index("dp") % 2

    def two(mat, n):
        part = lax.dynamic_slice_in_dim(mat, sq * 2 * n, 2 * n, axis=1)
        return part.reshape(rows, 2, n).transpose(1, 0, 2)

    vec = jnp.concatenate([ln1_gain, ln1_shift, q_bias, v_bias, o_bias, ln2_gain, ln2_shift, out_bias])
    vec = jnp.pad(vec.reshape(VEC, rows), ((0, 8), (0, -rows % 128)))
    out_rows = lax.dynamic_slice_in_dim(out_weight, sq * 2 * ffp, 2 * ffp, axis=0)
    wp = jnp.concatenate(
        [jnp.zeros((2, rows, VEC), BF16), two(q_weight, hid), two(k_weight, hid), two(v_weight, hid),
         two(in_weight, ffp), out_rows.reshape(2, ffp, rows).transpose(0, 2, 1)], axis=2)
    total = 3 * 512
    used = VEC + 3 * hid + 2 * ffp
    wp = jnp.pad(wp, ((0, 0), (0, 0), (0, total - used)))
    in_at = VEC + 3 * hid
    off_in = in_at % 128
    win = (ffp + 127) // 128 * 128
    inb = lax.dynamic_slice_in_dim(in_bias, (2 * sq + y) * ffp, ffp).astype(F32)
    inb = jnp.broadcast_to(jnp.pad(inb, (off_in, win - ffp - off_in)), (8, win))
    vmem = pl.BlockSpec(memory_space=pltpu.VMEM)
    nimg, length, cols = 2 * images, own_len * ns, 512
    tall = (nimg, length, width)
    half = (own_len, width)
    D = pltpu.SemaphoreType.DMA
    V = pltpu.VMEM
    scratch = dict(
        fgrad=V((ranks, rows, total), BF16), ograd=V((hid + 16, width), BF16), ibgrad=V((ranks, 8, win), F32),
        st_q=V((rows, width), BF16), st_k=V((rows, width), BF16), st_v=V((rows, width), BF16),
        st_in=V((rows, ff), BF16), st_out=V((ff, rows), BF16), vslab=V((2, nz) + vec.shape, BF16),
        w=V((2 * nz * rows, total), BF16), ow=V((hid, width), BF16), xall=V(tall, BF16), call=V(tall, BF16),
        n1=V(tall, BF16), n2=V(tall, BF16), gb=V(tall, BF16), qkv=V((nimg, length, cols), BF16),
        probs=V((nimg, 2, length, length), F32), mix=V((nimg, length, hid), BF16),
        act=V((nimg, length, win), BF16), slope=V((nimg, length, win), F32), gp=V((nimg, length, win), BF16),
        part=V(tall, BF16), part2=V(tall, BF16), r1=V((nimg, 2) + half, BF16), r1b=V((nimg, 2) + half, BF16),
        dx=V(half, BF16), dy=V(half, BF16), rx=V((2,) + half, BF16), ry=V((2,) + half, BF16),
        dxb=V(half, BF16), dyb=V(half, BF16), rxb=V((2,) + half, BF16), ryb=V((2,) + half, BF16),
        hid_s=V((2,) + half, F32), hat2_s=V((2,) + half, F32), inv2_s=V((2, own_len, 128), F32),
        gh_s=V((2,) + half, F32), vecs=V((VEC, width), F32),
        g=V((2 * nz * rows, total), BF16), rb=V((3, nz + 1, 2, rows, cols), BF16),
        rbo=V((2, hid + 16, width), BF16), gin_tail=V((width, 128), BF16), gout_tail=V((width, 128), BF16),
        dqkv=V((nimg, length, cols), BF16), vsum=V((8, width), F32), ibx=V((nz, 8, win), F32),
        isb=V((8, win), F32), og=V((hid + 16, width), BF16),
        qbs=V((8, cols), F32), qbx=V((nz, 8, cols), F32),
        gy_s=D((3,)), gzr_s=D((3, nz, 2)), gzl_s=D((3, nz, 2)), g_r=D((3, nz, 2)), o_s=D((2,)), o_r=D((1,)),
        ag_s=D((4, 14)), ag_r=D((4, 14)), rs_s=D((4, 14)), rs_r=D((4, 14)), z_s=D((3, nz, 2)),
        z_r=D((3, nz + 1, 2)), zo_s=D((4,)), zo_r=D((4,)), f_s=D((3, 7)), f_r=D((3, 7)), ib_s=D((nz + 7,)),
        ib_r=D((nz + 7,)), qb_s=D((1,)), qb_r=D((nz,)), v_s=D((nz,)),
        v_r=D((nz + 1,)), st_s=D((6,)),
    )
    hbm = pl.BlockSpec(memory_space=pl.ANY)
    out, gtok, gq, gk, gv, gin, gout, go, gvec, gib = pl.pallas_call(
        functools.partial(layer_kernel, nz, hid, ffp),
        out_shape=(
            jax.ShapeDtypeStruct(tokens.shape, BF16), jax.ShapeDtypeStruct(tokens.shape, BF16),
            jax.ShapeDtypeStruct((rows, width), BF16), jax.ShapeDtypeStruct((rows, width), BF16),
            jax.ShapeDtypeStruct((rows, width), BF16), jax.ShapeDtypeStruct((rows, ff), BF16),
            jax.ShapeDtypeStruct((ff, rows), BF16), jax.ShapeDtypeStruct((hid + 16, width), BF16),
            jax.ShapeDtypeStruct((VEC, rows), F32), jax.ShapeDtypeStruct((1, ff), F32),
        ),
        in_specs=[vmem] * 6,
        out_specs=[vmem, vmem] + [hbm] * 6 + [vmem, vmem],
        scratch_shapes=list(scratch.values()),
        compiler_params=pltpu.CompilerParams(
            collective_id=0, has_side_effects=True, vmem_limit_bytes=65000 * 1024),
    )(wp, vec, o_weight, tokens, cotangent, inb)
    gq, gk, gv, gin, gout, go = [a.astype(F32) for a in (gq, gk, gv, gin, gout, go[:hid])]
    return (out, gtok, gvec[0], gvec[1], gq, gvec[6], gk, gv, gvec[7], go, gvec[4], gvec[2], gvec[3], gin,
            gib.reshape(ff), gout, gvec[5])


def mm(a, b, ca, cb):
    return lax.dot_general(a, b, (((ca,), (cb,)), ((), ())), preferred_element_type=F32)


def on_device(
    tokens, cotangent, ln1_gain, ln1_shift, q_weight, q_bias, k_weight, v_weight, v_bias,
    o_weight, o_bias, ln2_gain, ln2_shift, in_weight, in_bias, out_weight, out_bias,
):
    part = lax.axis_index("seq")
    parts = lax.axis_size("seq")
    groups = lax.axis_size("dp")
    images, own_len, width = tokens.shape
    ff = in_weight.shape[1]
    hid = width // parts
    ffp = ff // parts
    heads = HEADS // parts
    length = own_len * parts
    rows = images * length

    def cols(w, n):
        return lax.dynamic_slice_in_dim(w, part * n, n, axis=1)

    vecs = jnp.stack(
        [ln1_gain, ln1_shift, q_bias, v_bias, o_bias, ln2_gain, ln2_shift, out_bias]
    )
    vecs = lax.all_gather(vecs, "dp", axis=1, tiled=True).astype(F32)
    g1, s1, qb, vb, ob, g2, s2, outb = [vecs[i] for i in range(8)]
    x = lax.all_gather(tokens, "seq", axis=1, tiled=True).reshape(rows, width)
    cot = lax.all_gather(cotangent, "seq", axis=1, tiled=True).reshape(rows, width)
    qkv = jnp.concatenate([cols(q_weight, hid), cols(k_weight, hid), cols(v_weight, hid)], axis=1)
    qkv = lax.all_gather(qkv, "dp", axis=0, tiled=True)
    o_w = lax.all_gather(o_weight, "dp", axis=0, tiled=True)
    o_w = lax.dynamic_slice_in_dim(o_w, part * hid, hid, axis=0)
    in_w = lax.all_gather(cols(in_weight, ffp), "dp", axis=0, tiled=True)
    out_w = lax.dynamic_slice_in_dim(out_weight, part * ffp, ffp, axis=0)
    out_w = lax.all_gather(out_w.T, "dp", axis=0, tiled=True)
    qb_own = lax.dynamic_slice_in_dim(qb, part * hid, hid)
    vb_own = lax.dynamic_slice_in_dim(vb, part * hid, hid)
    inb_own = lax.dynamic_slice_in_dim(in_bias, part * ffp, ffp).astype(F32)

    def scatter_tokens(partial):
        return lax.psum_scatter(
            partial.astype(BF16).reshape(images, length, width),
            "seq", scatter_dimension=1, tiled=True,
        ).astype(F32)

    hat1, _ = normalize(x.astype(F32))
    normed1 = (hat1 * g1 + s1).astype(BF16)
    proj = mm(normed1, qkv, 1, 0)
    queries = (proj[:, :hid] + qb_own).astype(BF16).reshape(images, length, heads, HEAD_DIM)
    keys = proj[:, hid : 2 * hid].astype(BF16).reshape(images, length, heads, HEAD_DIM)
    values = (proj[:, 2 * hid :] + vb_own).astype(BF16).reshape(images, length, heads, HEAD_DIM)
    factor = 1.0 / math.sqrt(HEAD_DIM)
    ein = lambda s, a, b: jnp.einsum(s, a, b, preferred_element_type=F32)
    scores = ein("iqhd,ikhd->ihqk", queries, keys) * factor
    top = jnp.max(scores, axis=-1, keepdims=True)
    expo = jnp.exp(scores - top)
    probs = expo / jnp.sum(expo, axis=-1, keepdims=True)
    probs_low = probs.astype(BF16)
    mixed = ein("ihqk,ikhd->iqhd", probs_low, values).astype(BF16).reshape(rows, hid)
    start = tokens.astype(F32)
    hidden = start + scatter_tokens(mm(mixed, o_w, 1, 0)) + ob
    hat2, r2 = normalize(hidden)
    normed2 = (hat2 * g2 + s2).astype(BF16)
    normed2 = lax.all_gather(normed2, "seq", axis=1, tiled=True).reshape(rows, width)
    pre = mm(normed2, in_w, 1, 0) + inb_own
    act, slope = gelu_parts(pre)
    act = act.astype(BF16)
    out = hidden + scatter_tokens(mm(act, out_w, 1, 1)) + outb
    d_out_w = mm(cot, act, 0, 0)
    cot_own = cotangent.astype(F32)
    grad_pre = (mm(cot, out_w, 1, 0) * slope).astype(BF16)
    d_in_w = mm(normed2, grad_pre, 0, 0)
    d_in_b = jnp.sum(grad_pre.astype(F32), axis=0)
    grad_n2 = scatter_tokens(mm(grad_pre, in_w, 1, 1))
    grad_hidden = cot_own + norm_back(grad_n2, g2, hat2, r2)
    branch_own = grad_hidden.astype(BF16)
    branch = lax.all_gather(branch_own, "seq", axis=1, tiled=True).reshape(rows, width)
    d_o_w = mm(mixed, branch, 0, 0)
    grad_mixed = mm(branch, o_w, 1, 1).astype(BF16).reshape(images, length, heads, HEAD_DIM)
    grad_probs = ein("iqhd,ikhd->ihqk", grad_mixed, values)
    row_dot = jnp.sum(probs * grad_probs, axis=-1, keepdims=True)
    grad_scores = (probs * (grad_probs - row_dot)).astype(BF16)
    grad_q = (ein("ihqk,ikhd->iqhd", grad_scores, keys) * factor).astype(BF16).reshape(rows, hid)
    grad_k = (ein("ihqk,iqhd->ikhd", grad_scores, queries) * factor).astype(BF16).reshape(rows, hid)
    grad_v = ein("ihqk,iqhd->ikhd", probs_low, grad_mixed).astype(BF16).reshape(rows, hid)
    grad_qkv = jnp.concatenate([grad_q, grad_k, grad_v], axis=1)
    d_qkv = mm(normed1, grad_qkv, 0, 0)
    d_qb = jnp.sum(grad_q.astype(F32), axis=0)
    d_vb = jnp.sum(grad_v.astype(F32), axis=0)
    grad_n1 = scatter_tokens(mm(grad_qkv, qkv, 1, 1))
    hat1o, r1o = normalize(start)
    grad_tokens = grad_hidden + norm_back(grad_n1, g1, hat1o, r1o)
    wide = jnp.concatenate([d_qkv, d_in_w, d_out_w], axis=1).astype(BF16)
    wide = lax.psum_scatter(wide, "dp", scatter_dimension=0, tiled=True)
    wide = lax.all_gather(wide, "seq", axis=0, tiled=False).astype(F32)

    def spread(lo, n):
        return wide[:, :, lo : lo + n].transpose(1, 0, 2).reshape(width // groups, n * parts)

    gq, gk, gv = [spread(i * hid, hid) for i in range(3)]
    gin = spread(3 * hid, ffp)
    gout = wide[:, :, 3 * hid + ffp :].transpose(0, 2, 1).reshape(ff, width // groups)
    o_full = lax.all_gather(
        lax.psum_scatter(d_o_w.astype(BF16), "dp", scatter_dimension=1, tiled=True),
        "seq", axis=0, tiled=True,
    )
    go = lax.all_to_all(o_full, "dp", split_axis=0, concat_axis=1, tiled=True).astype(F32)
    own_sums = jnp.stack([
        jnp.sum(grad_n1 * hat1o, axis=(0, 1)), jnp.sum(grad_n1, axis=(0, 1)),
        jnp.sum(grad_n2 * hat2, axis=(0, 1)), jnp.sum(grad_n2, axis=(0, 1)),
        jnp.sum(branch_own.astype(F32), axis=(0, 1)), jnp.sum(cot_own, axis=(0, 1)),
        lax.dynamic_update_slice_in_dim(jnp.zeros(width, F32), d_qb, part * hid, 0),
        lax.dynamic_update_slice_in_dim(jnp.zeros(width, F32), d_vb, part * hid, 0),
    ])
    bias_in = lax.dynamic_update_slice_in_dim(jnp.zeros(ff, F32), d_in_b, part * ffp, 0)
    total = lax.psum(jnp.concatenate([own_sums.reshape(-1), bias_in]), ("dp", "seq"))
    vec_part = total[: 8 * width].reshape(8, groups, width // groups)
    vec_part = lax.dynamic_index_in_dim(vec_part, lax.axis_index("dp"), axis=1, keepdims=False)
    bias_total = total[8 * width :]
    return (
        out.astype(BF16), grad_tokens.astype(BF16), vec_part[0], vec_part[1], gq, vec_part[6],
        gk, gv, vec_part[7], go, vec_part[4], vec_part[2], vec_part[3], gin, bias_total, gout,
        vec_part[5],
    )


def solution(mesh):
    fast = mesh.shape["dp"] == 2 * mesh.shape["seq"]
    rows, vec = P("dp", None), P("dp")
    tok = P("dp", "seq", None)
    return jax.shard_map(
        layer_fast if fast else on_device,
        mesh=mesh,
        in_specs=(tok, tok, vec, vec, rows, vec, rows, rows, vec, rows, vec, vec, vec, rows,
                  P(), P(None, "dp"), vec),
        out_specs=(tok, tok, vec, vec, rows, vec, rows, rows, vec, rows, vec, vec, vec, rows,
                   P(), P(None, "dp"), vec),
        check_vma=False,
    )
```

```python
import functools
import math

import jax
import jax.numpy as jnp
from jax import lax
from jax.experimental import pallas as pl
from jax.experimental.pallas import tpu as pltpu
from jax.sharding import PartitionSpec as P

BF16, F32 = jnp.bfloat16, jnp.float32
HEADS, HEAD_DIM = 16, 72
eps_norm = 1e-06
gelu_coef = 0.7978845608028654
gelu_cube = 0.044715
MESH = pl.DeviceIdType.MESH
VEC = 8


def normalize(values):
    row_mean = jnp.mean(values, axis=-1, keepdims=True)
    centred = values - row_mean
    inverse = lax.rsqrt(jnp.mean(centred * centred, axis=-1, keepdims=True) + eps_norm)
    return centred * inverse, inverse


def norm_back(grad_normed, gain_vec, scaled, inverse):
    grad_scaled = grad_normed * gain_vec
    centred_grad = grad_scaled - jnp.mean(grad_scaled, axis=-1, keepdims=True)
    return inverse * (
        centred_grad - scaled * jnp.mean(grad_scaled * scaled, axis=-1, keepdims=True)
    )


def gelu_parts(pre_act):
    tanh_val = jnp.tanh(gelu_coef * (pre_act + gelu_cube * pre_act * pre_act * pre_act))
    value_part = 0.5 * pre_act * (1.0 + tanh_val)
    slope_part = 0.5 * (1.0 + tanh_val) + 0.5 * pre_act * (
        1.0 - tanh_val * tanh_val
    ) * gelu_coef * (1.0 + 3.0 * gelu_cube * pre_act * pre_act)
    return value_part, slope_part


def dot(a, b, ca, cb):
    return lax.dot_general(a, b, (((ca,), (cb,)), ((), ())), preferred_element_type=F32)


def layer_kernel(
    nz, hid, ffp,
    tok, cot_in, q_in, k_in, v_in, in_in, out_in, ow_in, inb_in, vin0, vin1, vin2, vin3, vin4, vin5, vin6, vin7,
    out_ref, gtok_ref, q_out, k_out, v_out, in_out, out_out, o_out, vec_out, ib_out,
    wp, fgrad, ograd, ibgrad, st_q, st_k, st_v, st_in, st_out, vslab, inb, inflat, inrow, vflat0, vflat1, vflat2, vflat3, vflat4, vflat5, vflat6, vflat7, vrows, st_o, st_g, st_vec, st_ib,
    w, ow, xall, call, n1, n2, gb, qkv, probs, mix, act, slope, gp, part, part2, r1, r1b,
    dx, dy, rx, ry, dxb, dyb, rxb, ryb, hid_s, hat2_s, inv2_s, gh_s, vecs, g, rb, rbh, rbo, gin_tail,
    gout_tail, dqkv, vsum, ibx, isb, og, qbs, qbx,
    gy_s, gz_s, gzl_s, g_r, o_s, o_r, ag_s, ag_r, rs_s, rs_r, z_s, z_r, zo_s, zo_r, f_s, f_r,
    ib_s, ib_r, qb_s, qb_r, v_s, v_r, st_s, ld_s,
):
    d, s = lax.axis_index("dp"), lax.axis_index("seq")
    z, y = d // 2, d % 2
    x, c = s // 2, s % 2
    rank = 2 * s + y
    nimg, length, width = xall.shape
    own_len = dx.shape[0]
    rows8 = wp.shape[1]
    plane = 2 * rows8
    cols = 512
    qw = hid
    in_at = VEC + 3 * qw
    in_win = in_at // 128 * 128
    out_at = in_at + ffp
    out_win = out_at // 128 * 128
    win = (ffp + 127) // 128 * 128
    off_in, off_out = in_at - in_win, out_at - out_win
    shift = off_out - off_in
    core_n, x_n, y_n = (d, s + 1 - 2 * c), (d, (s + 2) % 4), (d + 1 - 2 * y, s)
    right, left = (d + 2, s), (d - 2, s)
    has_r, has_l = z < nz - 1, z > 0
    sg = 1 - 2 * (z // 2)
    is_end = (z == 0) | (z == nz - 1)
    middle = (z > 0) & (z < nz - 1)
    factor = 1.0 / math.sqrt(HEAD_DIM)

    def plane_at(k):
        return z + sg * k

    def away(k):
        return (d + 2 * sg * k, s)

    def rc(src, dst, ss, rs, dev):
        return pltpu.make_async_remote_copy(
            src_ref=src, dst_ref=dst, send_sem=ss, recv_sem=rs, device_id=dev, device_id_type=MESH
        )

    barrier = pltpu.get_barrier_semaphore()
    column = [((d + 2 * k) % (2 * nz), s) for k in range(1, nz)]
    for dev in [core_n, x_n, y_n] + column:
        pl.semaphore_signal(barrier, inc=1, device_id=dev, device_id_type=MESH)

    own_rows = pl.ds(pl.multiple_of(s * own_len, 16), own_len)
    vflat = (vflat0, vflat1, vflat2, vflat3, vflat4, vflat5, vflat6, vflat7)
    vec_loads = list(zip((vin0, vin1, vin2, vin3, vin4, vin5, vin6, vin7), vflat))
    loads = [pltpu.make_async_copy(a, b, ld_s.at[n]) for n, (a, b) in enumerate(
        vec_loads + [(q_in, st_q), (k_in, st_k), (v_in, st_v), (in_in, st_in),
         (tok.at[0], xall.at[2 * y, own_rows]), (tok.at[1], xall.at[2 * y + 1, own_rows]), (out_in, st_out),
         (cot_in.at[0], call.at[2 * y, own_rows]), (cot_in.at[1], call.at[2 * y + 1, own_rows]),
         (inb_in, inflat)])]
    for cp in loads:
        cp.start()
    load_o = pltpu.make_async_copy(ow_in, ow, ld_s.at[len(loads)])
    pl.when(z == s)(lambda: load_o.start())

    def build_first():
        def go(k):
            for j in range(2):
                t = 2 * k + j
                wp[j, :, 0:128] = jnp.zeros((rows8, 128), BF16)
                for n, st in enumerate((st_q, st_k, st_v)):
                    wp[j, :, VEC + n * qw : VEC + (n + 1) * qw] = st[:, t * qw : (t + 1) * qw]
                wp[j, :, in_at:cols] = st_in[:, t * ffp : t * ffp + cols - in_at]
        for k in range(4):
            pl.when(s == k)(functools.partial(go, k))

    def build_rest():
        def go(k):
            for j in range(2):
                t = 2 * k + j
                wp[j, :, 3 * cols - 128 :] = jnp.zeros((rows8, 128), BF16)
                wp[j, :, cols : in_at + ffp] = st_in[:, t * ffp + cols - in_at : (t + 1) * ffp]
                wp[j, :, out_at : out_at + ffp] = st_out[:, t * ffp : (t + 1) * ffp]
        for k in range(4):
            pl.when(s == k)(functools.partial(go, k))

    def build_bias():
        def go(t):
            inb[...] = jnp.zeros_like(inb)
            inb[0:1, off_in : off_in + ffp] = inrow[0:1, t * ffp : (t + 1) * ffp]
        for t in range(8):
            pl.when(rank == t)(functools.partial(go, t))

    for cp in loads[: VEC + 6]:
        cp.wait()
    vrows[...] = jnp.zeros_like(vrows)
    for n in range(VEC):
        vrows[n : n + 1, 0:rows8] = vflat[n][...].astype(F32).reshape(1, rows8)
    vslab[y, z] = vrows[...].astype(BF16)
    build_first()
    pl.semaphore_wait(barrier, 3 + len(column))

    def wrows(origin, sub):
        return pl.ds(pl.multiple_of(origin * plane + sub * rows8, 16), rows8)

    def wslab(ch, origin, sub):
        return w.at[wrows(origin, sub), pl.ds(ch * cols, cols)]

    def wsend(ch, origin, sub, src, to_right, own=False):
        sems = gz_s.at[ch % 2, origin, sub] if to_right or not own else gzl_s.at[ch % 2, sub]
        return rc(src, wslab(ch, origin, sub), sems, g_r.at[ch, origin, sub],
                  right if to_right else left)

    def wrecv(ch, origin, sub):
        slab = wslab(ch, origin, sub)
        rc(slab, slab, g_r.at[ch, origin, sub], g_r.at[ch, origin, sub], core_n).wait_recv()

    def gather_own(ch):
        src = wp.at[y, :, pl.ds(ch * cols, cols)]
        pl.when(has_r)(lambda: wsend(ch, z, y, src, True).start())
        pl.when(has_l)(lambda: wsend(ch, z, y, src, False, True).start())
        w[wrows(z, y), ch * cols : (ch + 1) * cols] = wp[y, :, ch * cols : (ch + 1) * cols]

    def gather_swap(ch):
        rc(wp.at[1 - y, :, pl.ds(ch * cols, cols)], wslab(ch, z, y), gy_s.at[ch], g_r.at[ch, z, y],
           y_n).start()

    def gather_other(ch):
        wrecv(ch, z, 1 - y)
        src = wslab(ch, z, 1 - y)
        pl.when(has_r)(lambda: wsend(ch, z, 1 - y, src, True).start())
        pl.when(has_l)(lambda: wsend(ch, z, 1 - y, src, False, True).start())

    def gather_hop(ch, k):
        def from_left():
            for sub in range(2):
                wrecv(ch, z - k, sub)
                pl.when(has_r)(lambda: wsend(ch, z - k, sub, wslab(ch, z - k, sub), True).start())

        def from_right():
            for sub in range(2):
                wrecv(ch, z + k, sub)
                pl.when(has_l)(lambda: wsend(ch, z + k, sub, wslab(ch, z + k, sub), False).start())

        pl.when(z - k >= 0)(from_left)
        pl.when(z + k < nz)(from_right)

    def gather_hop1(ch, k, sub):
        def from_left():
            wrecv(ch, z - k, sub)
            pl.when(has_r)(lambda: wsend(ch, z - k, sub, wslab(ch, z - k, sub), True).start())

        def from_right():
            wrecv(ch, z + k, sub)
            pl.when(has_l)(lambda: wsend(ch, z + k, sub, wslab(ch, z + k, sub), False).start())

        pl.when(z - k >= 0)(from_left)
        pl.when(z + k < nz)(from_right)

    def gather_drain(ch):
        for k in range(nz):
            for sub in range(2):
                pl.when((z - k >= 0) & has_r)(
                    lambda: wsend(ch, z - k, sub, wslab(ch, z - k, sub), True).wait_send())
                pl.when((z + k < nz) & has_l)(
                    lambda: wsend(ch, z + k, sub, wslab(ch, z + k, sub), False, k == 0).wait_send())
        rc(wp.at[1 - y, :, pl.ds(ch * cols, cols)], wslab(ch, z, y), gy_s.at[ch], g_r.at[ch, z, y],
           y_n).wait_send()

    def osend(to_right):
        return rc(ow, ow, o_s.at[0 if to_right else 1], o_r.at[0], right if to_right else left)

    def o_own(outer):
        def go():
            load_o.wait()
            pl.when(has_r)(lambda: osend(True).start())
            pl.when(has_l)(lambda: osend(False).start())
        pl.when((z == s) & (is_end if outer else middle))(go)

    def o_pass(k):
        def go():
            osend(True).wait_recv()
            pl.when((z > s) & has_r)(lambda: osend(True).start())
            pl.when((z < s) & has_l)(lambda: osend(False).start())
        pl.when((z == s + k) | (z == s - k))(go)

    def o_drain():
        pl.when((z >= s) & has_r)(lambda: osend(True).wait_send())
        pl.when((z <= s) & has_l)(lambda: osend(False).wait_send())

    def agather(inst, dst):
        ss, rr = ag_s.at[inst % 2], ag_r.at[inst % 2]

        def blk(yy, sq, i):
            return dst.at[2 * yy + i, pl.ds(pl.multiple_of(sq * own_len, 16), own_len)]

        sx, sp = (s + 2) % 4, s + 1 - 2 * c
        spx = (sp + 2) % 4

        def msg(n, block, dev):
            return rc(block, block, ss.at[n], rr.at[n], dev)

        mine = [blk(y, s, i) for i in range(2)]
        xs = [blk(y, sx, i) for i in range(2)]
        ys = [blk(1 - y, s, i) for i in range(2)]
        dg = [blk(1 - y, sx, i) for i in range(2)]
        sends = [msg(0, mine[0], x_n), msg(1, mine[1], x_n), msg(2, ys[1], x_n),
                 msg(3, mine[0], y_n), msg(4, mine[1], y_n), msg(5, xs[0], y_n)]
        sends += [msg(6 + i, mine[i], core_n) for i in range(2)]
        sends += [msg(8 + i, xs[i], core_n) for i in range(2)]
        sends += [msg(10 + i, ys[i], core_n) for i in range(2)]
        sends += [msg(12 + i, dg[i], core_n) for i in range(2)]
        recvs = [msg(0, xs[0], x_n), msg(1, xs[1], x_n), msg(2, dg[1], x_n),
                 msg(3, ys[0], y_n), msg(4, ys[1], y_n), msg(5, dg[0], y_n)]
        recvs += [msg(6 + i, blk(y, sp, i), core_n) for i in range(2)]
        recvs += [msg(8 + i, blk(y, spx, i), core_n) for i in range(2)]
        recvs += [msg(10 + i, blk(1 - y, sp, i), core_n) for i in range(2)]
        recvs += [msg(12 + i, blk(1 - y, spx, i), core_n) for i in range(2)]

        def begin():
            for n in (0, 4, 1, 3, 6, 7):
                sends[n].start()

        def relay(parts=(0, 1, 2, 3)):
            if 0 in parts:
                recvs[0].wait_recv()
                sends[5].start()
                sends[8].start()
            if 1 in parts:
                recvs[4].wait_recv()
                sends[2].start()
                sends[11].start()
            if 2 in parts:
                recvs[1].wait_recv()
                sends[9].start()
            if 3 in parts:
                recvs[3].wait_recv()
                sends[10].start()

        def finish(parts=(0, 1)):
            if 0 in parts:
                recvs[2].wait_recv()
                sends[13].start()
                recvs[5].wait_recv()
                sends[12].start()
            if 1 in parts:
                for n in range(6, 14):
                    recvs[n].wait_recv()

        def drain():
            for m in sends:
                m.wait_send()

        return begin, relay, finish, drain

    def rscatter(inst, pt, ra, bufs, produce):
        bdx, bdy, brx, bry = bufs
        ss, rr = rs_s.at[inst % 2], rs_r.at[inst % 2]
        xo = 1 - x

        def image(it):
            return (2 * (1 - y) + it) % 4

        def rows(xx, cc):
            return pl.ds(pl.multiple_of((2 * xx + cc) * own_len, 16), own_len)

        def swap(it, xx):
            img = image(it)
            return rc(pt.at[img, rows(xx, 1 - c)], ra.at[img, xx], ss.at[2 * it + xx],
                      rr.at[2 * it + xx], core_n)

        def add(it, xx):
            swap(it, xx).wait_recv()
            img = image(it)
            ra[img, xx] = (ra[img, xx].astype(F32) + pt[img, rows(xx, c)].astype(F32)).astype(BF16)

        m = [
            rc(ra.at[image(0), xo], bdx, ss.at[8], rr.at[8], x_n),
            rc(ra.at[image(1), xo], bdy, ss.at[9], rr.at[9], y_n),
            rc(ra.at[image(1), x], bry.at[1], ss.at[10], rr.at[10], y_n),
            rc(ra.at[image(2), xo], brx.at[0], ss.at[11], rr.at[11], x_n),
            rc(ra.at[image(0), x], bry.at[0], ss.at[12], rr.at[12], y_n),
            rc(ra.at[image(3), xo], brx.at[1], ss.at[13], rr.at[13], x_n),
        ]

        def run_a():
            def step(it, carry):
                produce(image(it))
                swap(it, xo).start()
                swap(it, x).start()
                return carry
            lax.fori_loop(0, nimg, step, 0)

            add(0, xo)
            m[0].start()
            add(1, xo)
            m[1].start()
            add(1, x)
            m[2].start()
            add(2, xo)
            m[3].start()
            add(0, x)
            add(3, xo)

        def run_b():
            m[0].wait_recv()
            ra[image(0), x] = (ra[image(0), x].astype(F32) + bdx[...].astype(F32)).astype(BF16)
            m[4].start()
            m[1].wait_recv()
            ra[image(3), xo] = (ra[image(3), xo].astype(F32) + bdy[...].astype(F32)).astype(BF16)
            m[5].start()
            add(2, x)
            add(3, x)

        def result(i):
            rc(brx.at[i], brx.at[i], ss.at[11 + 2 * i], rr.at[11 + 2 * i], x_n).wait_recv()
            rc(bry.at[i], bry.at[i], ss.at[12 - 2 * i], rr.at[12 - 2 * i], y_n).wait_recv()
            return (ra[image(2 + i), x].astype(F32) + brx[i].astype(F32)) + bry[i].astype(F32)

        def drain():
            for it in range(nimg):
                swap(it, 0).wait_send()
                swap(it, 1).wait_send()
            for n in range(8, 14):
                rc(bdx, bdx, ss.at[n], rr.at[n], x_n).wait_send()

        return run_a, run_b, result, drain

    zch = [(2 * cols, cols), (cols, cols), (cols // 2, cols // 2), (0, cols // 2)]
    order = (1 - y, y)

    def rb_at(ch, slot, sub):
        return (rb if ch < 2 else rbh).at[ch % 2, slot, sub]

    def gslab(ch, dest, sub):
        return g.at[wrows(dest, sub), pl.ds(*zch[ch])]

    def zsend(ch, where, sub):
        k = (1, 2, 3, -1)[where]
        to, slot = (1, nz) if k == 3 else (k, z)
        return rc(gslab(ch, plane_at(k), sub), rb_at(ch, slot, sub), z_s.at[ch % 2, where, sub],
                  z_r.at[ch, slot, sub], away(to))

    def zadd(ch, dest, slot, sub):
        ref = rb_at(ch, slot, sub)
        rc(ref, ref, z_r.at[ch, slot, sub], z_r.at[ch, slot, sub], core_n).wait_recv()
        r, cs = wrows(dest, sub), slice(zch[ch][0], sum(zch[ch]))
        g[r, cs] = (g[r, cs].astype(F32) + ref[...].astype(F32)).astype(BF16)

    def z_first(ch):
        def outer():
            for where in (2, 1, 0):
                for sub in order:
                    zsend(ch, where, sub).start()

        def inner():
            for where in (3, 0):
                for sub in order:
                    zsend(ch, where, sub).start()
        pl.when(is_end)(outer)
        pl.when(middle)(inner)

    def z_merge(ch):
        def inner():
            for sub in order:
                zadd(ch, plane_at(2), nz, sub)
                zsend(ch, 1, sub).start()
        pl.when(middle)(inner)

    def zreduce_own(ch):
        def outer(sub):
            zadd(ch, z, plane_at(1), sub)
            zadd(ch, z, plane_at(2), sub)

        def inner(sub):
            for k in (-1, 1, 2):
                zadd(ch, z, plane_at(k), sub)
        for sub in order:
            pl.when(is_end)(functools.partial(outer, sub))
            pl.when(middle)(functools.partial(inner, sub))

    def zdrain(ch):
        for sub in range(2):
            zsend(ch, 0, sub).wait_send()
            zsend(ch, 1, sub).wait_send()
            pl.when(is_end)(lambda: zsend(ch, 2, sub).wait_send())
            pl.when(middle)(lambda: zsend(ch, 3, sub).wait_send())

    def f_swap(ch):
        src = g.at[wrows(z, 1 - y), pl.ds(*zch[ch])]
        return rc(src, fgrad.at[rank, :, pl.ds(*zch[ch])], f_s.at[ch % 2, 0], f_r.at[ch, 0], y_n)

    def f_msg(ch, n, slot, dev):
        piece = fgrad.at[slot, :, pl.ds(*zch[ch])]
        return rc(piece, piece, f_s.at[ch % 2, n], f_r.at[ch, n], dev)

    sx, sp = (s + 2) % 4, s + 1 - 2 * c
    spx = (sp + 2) % 4

    def f_begin(ch):
        f_swap(ch).start()
        cs = slice(zch[ch][0], sum(zch[ch]))
        fgrad[rank, :, cs] = g[wrows(z, y), cs]
        f_msg(ch, 1, rank, x_n).start()
        f_msg(ch, 3, rank, core_n).start()

    def f_spread(ch):
        other = 2 * s + 1 - y
        f_msg(ch, 0, other, y_n).wait_recv()
        f_msg(ch, 2, other, x_n).start()
        f_msg(ch, 4, other, core_n).start()

    def f_relay(ch):
        f_msg(ch, 1, 2 * sx + y, x_n).wait_recv()
        f_msg(ch, 5, 2 * sx + y, core_n).start()
        f_msg(ch, 2, 2 * sx + 1 - y, x_n).wait_recv()
        f_msg(ch, 6, 2 * sx + 1 - y, core_n).start()

    def f_end(ch):
        f_msg(ch, 3, 2 * sp + y, core_n).wait_recv()
        f_msg(ch, 4, 2 * sp + 1 - y, core_n).wait_recv()
        f_msg(ch, 5, 2 * spx + y, core_n).wait_recv()
        f_msg(ch, 6, 2 * spx + 1 - y, core_n).wait_recv()

    def f_drain(ch):
        f_swap(ch).wait_send()
        for n in range(1, 7):
            f_msg(ch, n, rank, core_n).wait_send()

    far_out = ((z == 0) & (s == nz - 1)) | ((z == nz - 1) & (s == 0))
    adds = middle & (plane_at(2) == s)

    def zo_send(far):
        if far:
            return rc(og, rbo.at[nz], zo_s.at[0], zo_r.at[nz], away(1))
        return rc(og, rbo.at[z], zo_s.at[0], zo_r.at[z], (2 * s + y, s))

    def zo_add(slot):
        rc(rbo.at[slot], rbo.at[slot], zo_s.at[0], zo_r.at[slot], core_n).wait_recv()
        og[...] = (og[...].astype(F32) + rbo[slot].astype(F32)).astype(BF16)

    def zo_first():
        pl.when(far_out)(lambda: zo_send(True).start())
        pl.when(jnp.logical_not(far_out | adds) & (z != s))(lambda: zo_send(False).start())

    def zo_merge():
        def go():
            zo_add(nz)
            zo_send(False).start()
        pl.when(adds)(go)

    def zo_last():
        def inner():
            for k in (-1, 1, 2):
                zo_add(plane_at(k))
        pl.when(is_end)(lambda: [zo_add(plane_at(k)) for k in (1, 2)] and None)
        pl.when(middle)(inner)

    def qb_send():
        return rc(qbs, qbx.at[z], qb_s.at[0], qb_r.at[z], (2 * s + y, s))

    def qb_begin():
        bsum = jnp.zeros((1, cols), F32)
        for img in range(nimg):
            bsum = bsum + jnp.sum(dqkv[img].astype(F32), axis=0, keepdims=True)
        qbs[...] = jnp.broadcast_to(bsum, (8, cols))
        pl.when(z != s)(lambda: qb_send().start())

    def o_here():
        zo_last()
        total = qbs[...]
        for k in range(1, nz):
            zz = (z + k) % nz
            rc(qbs, qbx.at[zz], qb_s.at[0], qb_r.at[zz], core_n).wait_recv()
            total = total + qbx[zz]
        og[qw:, 0:cols] = jnp.concatenate([total, total], axis=0).astype(BF16)
        ograd[...] = og[...]
        rc(ograd, ograd, zo_s.at[2], zo_r.at[nz + 1], x_n).start()
        rc(ograd, ograd, zo_s.at[3], zo_r.at[nz + 2], core_n).start()

    def o_x():
        rc(ograd, ograd, zo_s.at[2], zo_r.at[nz + 1], x_n).wait_recv()
        rc(ograd, ograd, zo_s.at[3], zo_r.at[nz + 2], core_n).start()

    def o_end():
        pl.when((sp == z) | (spx == z))(
            lambda: rc(ograd, ograd, zo_s.at[3], zo_r.at[nz + 2], core_n).wait_recv())

    def o_out_done(n):
        rc(ograd, ograd, zo_s.at[n], zo_r.at[0], core_n).wait_send()

    def ib_send(k):
        return rc(isb, ibx.at[z], ib_s.at[k - 1], ib_r.at[z], ((d + 2 * k) % (2 * nz), s))

    def ib_begin():
        ib = jnp.zeros((1, win), F32)
        for img in range(nimg):
            ib = ib + jnp.sum(gp[img].astype(F32), axis=0, keepdims=True)
        isb[...] = jnp.broadcast_to(ib, (8, win))
        for k in range(1, nz):
            ib_send(k).start()

    def ib_msg(n, slot, dev):
        return rc(ibgrad.at[slot], ibgrad.at[slot], ib_s.at[n], ib_r.at[n], dev)

    def ib_pass():
        ibsum = isb[...]
        for k in range(1, nz):
            zz = (z + k) % nz
            rc(isb, ibx.at[zz], ib_s.at[0], ib_r.at[zz], core_n).wait_recv()
            ibsum = ibsum + ibx[zz]
        ibgrad[rank] = ibsum
        ib_msg(nz, rank, y_n).start()
        ib_msg(nz + 1, rank, x_n).start()
        ib_msg(nz + 3, rank, core_n).start()

    def ib_mid():
        other = 2 * s + 1 - y
        ib_msg(nz, other, y_n).wait_recv()
        ib_msg(nz + 2, other, x_n).start()
        ib_msg(nz + 4, other, core_n).start()
        ib_msg(nz + 1, 2 * sx + y, x_n).wait_recv()
        ib_msg(nz + 5, 2 * sx + y, core_n).start()

    def ib_last():
        ib_msg(nz + 2, 2 * sx + 1 - y, x_n).wait_recv()
        ib_msg(nz + 6, 2 * sx + 1 - y, core_n).start()

    def ib_end():
        ib_msg(nz + 3, 2 * sp + y, core_n).wait_recv()
        ib_msg(nz + 4, 2 * sp + 1 - y, core_n).wait_recv()
        ib_msg(nz + 5, 2 * spx + y, core_n).wait_recv()
        ib_msg(nz + 6, 2 * spx + 1 - y, core_n).wait_recv()

    def vec_send(k):
        return rc(vslab.at[y, z], vslab.at[y, z], v_s.at[k - 1], v_r.at[z], ((d + 2 * k) % (2 * nz), s))

    def vec_cross():
        return rc(vslab.at[y], vslab.at[y], v_s.at[nz - 1], v_r.at[nz], y_n)

    def vec_begin():
        for k in range(1, nz):
            vec_send(k).start()

    def vec_pass():
        for k in range(1, nz):
            zz = (z + k) % nz
            rc(vslab.at[y, zz], vslab.at[y, zz], v_s.at[0], v_r.at[zz], core_n).wait_recv()
        vec_cross().start()

    def vec_end():
        rc(vslab.at[1 - y], vslab.at[1 - y], v_s.at[0], v_r.at[nz], y_n).wait_recv()
        for zz in range(nz):
            for yy in range(2):
                at = (2 * zz + yy) * rows8
                vecs[:, at : at + rows8] = vslab[yy, zz].astype(F32)[0:VEC, 0:rows8]

    def vec_drain():
        for k in range(1, nz):
            vec_send(k).wait_send()
        vec_cross().wait_send()

    nrank = fgrad.shape[0]
    stores = [pltpu.make_async_copy(a, b, st_s.at[n]) for n, (a, b) in enumerate(
        [(st_q, q_out), (st_k, k_out), (st_v, v_out), (st_in, in_out), (st_out, out_out), (ograd, o_out),
         (st_o, out_ref), (st_g, gtok_ref), (st_vec, vec_out), (st_ib, ib_out)])]

    def emit_out():
        for t in range(nrank):
            st_out[:, t * ffp : (t + 1) * ffp] = fgrad[t, :, out_at : out_at + ffp]
            st_in[:, t * ffp + cols - in_at : (t + 1) * ffp] = fgrad[t, :, cols : in_at + ffp]
        stores[4].start()

    def emit_ib():
        for t in range(nrank):
            st_ib[0:1, t * ffp : (t + 1) * ffp] = ibgrad[t, 0:1, off_in : off_in + ffp]
        stores[9].start()

    def emit_upper():
        h = cols // 2
        k_from = h - VEC - qw
        for t in range(nrank):
            st_k[:, t * qw + k_from : (t + 1) * qw] = fgrad[t, :, h : VEC + 2 * qw]
            st_v[:, t * qw : (t + 1) * qw] = fgrad[t, :, VEC + 2 * qw : VEC + 3 * qw]
            st_in[:, t * ffp : t * ffp + cols - in_at] = fgrad[t, :, in_at:cols]
        stores[2].start()
        stores[3].start()

    def emit_lower():
        h = cols // 2
        k_from = h - VEC - qw
        for t in range(nrank):
            st_q[:, t * qw : (t + 1) * qw] = fgrad[t, :, VEC : VEC + qw]
            st_k[:, t * qw : t * qw + k_from] = fgrad[t, :, VEC + qw : h]
        stores[0].start()
        stores[1].start()
        vcols = jnp.zeros((rows8, 128), F32)
        for t in range(nrank):
            vcols = vcols + fgrad[t, :, 0:128].astype(F32)
        st_vec[0:VEC] = jnp.transpose(vcols, (1, 0))[0:VEC]
        st_vec[6:7] = ograd[qw : qw + 8, VEC : VEC + qw].astype(F32)[0:1]
        st_vec[7:8] = ograd[qw : qw + 8, VEC + 2 * qw : VEC + 3 * qw].astype(F32)[0:1]
        stores[8].start()

    gather_swap(0)
    ag_x = agather(0, xall)
    ag_c = agather(1, call)
    ag_x[0]()
    vec_begin()
    gather_own(0)
    for cp in loads[VEC + 6 :]:
        cp.wait()
    build_rest()
    inrow[...] = inflat[...].astype(F32).reshape(inrow.shape)
    build_bias()
    gather_other(0)
    o_own(True)
    gather_hop1(0, 1, y)
    ag_x[1]((0, 1))
    gather_hop1(0, 1, 1 - y)
    gather_hop1(0, 2, y)
    vec_pass()
    ag_x[1]((2, 3))
    gather_swap(1)
    ag_c[0]()
    ag_x[2]((0,))
    gather_hop1(0, 2, 1 - y)
    o_own(False)
    ag_x[2]((1,))
    vec_end()
    g1, s1 = vecs[0:1], vecs[1:2]
    o_b, g2, s2, out_b = vecs[4:5], vecs[5:6], vecs[6:7], vecs[7:8]

    def ln1_step(b, carry):
        img, r = b // 4, pl.ds(pl.multiple_of((b % 4) * 64, 64), 64)
        hat, _ = normalize(xall[img, r].astype(F32))
        n1[img, r] = (hat * g1 + s1).astype(BF16)
        return carry

    lax.fori_loop(0, 2 * nimg, ln1_step, 0)
    o_pass(1)
    gather_own(1)
    lax.fori_loop(2 * nimg, 4 * nimg, ln1_step, 0)
    gather_other(1)
    gather_hop(0, 3)

    lane = lax.broadcasted_iota(jnp.int32, (1, cols), 1)
    qb = pltpu.roll(vecs[...], (VEC - rank * qw + width) % width, 1)[2:3, :cols]
    vb = pltpu.roll(vecs[...], (VEC + 2 * qw - rank * qw + width) % width, 1)[3:4, :cols]
    qkv_bias = jnp.where((lane >= VEC) & (lane < VEC + qw), qb, 0.0) + jnp.where(
        (lane >= VEC + 2 * qw) & (lane < VEC + 3 * qw), vb, 0.0)

    def att_step(img, carry):
        proj = dot(n1[img], w[:, 0:cols], 1, 0) + qkv_bias
        proj = proj.astype(BF16)
        qkv[img] = proj
        outs = []
        for h in range(2):
            at = VEC + h * HEAD_DIM
            q = proj[:, at : at + HEAD_DIM]
            k = proj[:, qw + at : qw + at + HEAD_DIM]
            v = proj[:, 2 * qw + at : 2 * qw + at + HEAD_DIM]
            sc = dot(q, k, 1, 1) * factor
            e = jnp.exp(sc - jnp.max(sc, axis=-1, keepdims=True))
            p = e / jnp.sum(e, axis=-1, keepdims=True)
            probs[img, h] = p
            outs.append(dot(p.astype(BF16), v, 1, 0).astype(BF16))
        mix[img] = jnp.concatenate(outs, axis=1)
        return carry

    lax.fori_loop(0, 2, att_step, 0)
    o_pass(2)
    ag_c[1]()
    gather_swap(2)
    gather_hop(1, 1)
    lax.fori_loop(2, nimg, att_step, 0)
    o_pass(3)

    def o_part(img):
        part[img] = dot(mix[img], ow[...], 1, 0).astype(BF16)

    rs_h = rscatter(0, part, r1, (dx, dy, rx, ry), o_part)
    rs_h[0]()
    gather_hop(1, 2)
    gather_drain(0)
    gather_own(2)
    gather_other(2)
    rs_h[1]()
    ag_c[2]()
    gather_hop(2, 1)
    rs_h[3]()
    ag_x[3]()
    ag_n = agather(2, n2)
    for i in range(2):
        hidden = xall[2 * y + i, own_rows].astype(F32) + rs_h[2](i) + o_b
        hid_s[i] = hidden
        hat, inv = normalize(hidden)
        hat2_s[i] = hat
        inv2_s[i] = jnp.broadcast_to(inv, (own_len, 128))
        n2[2 * y + i, own_rows] = (hat * g2 + s2).astype(BF16)
    ag_n[0]()
    ag_n[1]()
    gather_hop(1, 3)
    gather_hop(2, 2)
    ag_n[2]()

    wlane = lax.broadcasted_iota(jnp.int32, (1, win), 1)
    valid = (wlane >= off_out) & (wlane < off_out + ffp)

    def in_step(img, carry):
        pre = dot(n2[img], w[:, in_win : in_win + win], 1, 0) + inb[0:1]
        a, sl = gelu_parts(pre)
        act[img] = jnp.where(valid, pltpu.roll(a, shift, 1), 0.0).astype(BF16)
        slope[img] = jnp.where(valid, pltpu.roll(sl, shift, 1), 0.0)
        return carry
    lax.fori_loop(0, nimg, in_step, 0)

    rtile = width // 3

    def gout_step(t, carry):
        r = pl.ds(pl.multiple_of(t * rtile, rtile), rtile)
        acc = jnp.zeros((rtile, win), F32)
        for img in range(nimg):
            acc = acc + dot(call[img, :, r], act[img], 0, 0)
        gout_tail[r] = acc[:, 0 : 2 * cols - out_win].astype(BF16)
        g[r, 2 * cols : 3 * cols] = acc[:, 2 * cols - out_win :].astype(BF16)
        return carry
    lax.fori_loop(0, 3, gout_step, 0)
    z_first(0)
    gather_hop(2, 3)

    def gp_step(img, carry):
        ga = dot(call[img], w[:, out_win : out_win + win], 1, 0) * slope[img]
        gp[img] = pltpu.roll(ga, win - shift, 1).astype(BF16)
        return carry
    lax.fori_loop(0, nimg, gp_step, 0)
    ib_begin()

    def gn2_part(img):
        part[img] = dot(gp[img], w[:, in_win : in_win + win], 1, 1).astype(BF16)

    rs_g2 = rscatter(2, part, r1, (dx, dy, rx, ry), gn2_part)
    rs_g2[0]()

    def gin_step(t, carry):
        r = pl.ds(pl.multiple_of(t * rtile, rtile), rtile)
        acc = jnp.zeros((rtile, win), F32)
        for img in range(nimg):
            acc = acc + dot(n2[img, :, r], gp[img], 0, 0)
        lo = cols - in_win
        gin_tail[r] = acc[:, 0:lo].astype(BF16)
        g[r, cols : 2 * cols - 128] = acc[:, lo : win - 128].astype(BF16)
        g[r, 2 * cols - 128 : 2 * cols] = (acc[:, win - 128 :] + gout_tail[r].astype(F32)).astype(BF16)
        return carry

    lax.fori_loop(0, 3, gin_step, 0)
    z_first(1)
    z_merge(0)
    rs_g2[1]()

    sums = [jnp.zeros((1, width), F32) for _ in range(6)]
    ag_g = agather(3, gb)
    for i in range(2):
        gn2 = rs_g2[2](i)
        hat = hat2_s[i]
        sums[2] = sums[2] + jnp.sum(gn2 * hat, axis=0, keepdims=True)
        sums[3] = sums[3] + jnp.sum(gn2, axis=0, keepdims=True)
        up = call[2 * y + i, own_rows].astype(F32)
        gh = up + norm_back(gn2, g2, hat, inv2_s[i][:, 0:1])
        gh_s[i] = gh
        low = gh.astype(BF16)
        gb[2 * y + i, own_rows] = low
        sums[4] = sums[4] + jnp.sum(low.astype(F32), axis=0, keepdims=True)
        sums[5] = sums[5] + jnp.sum(up, axis=0, keepdims=True)
    rs_g2[3]()
    ag_c[3]()
    ag_g[0]()
    for n in range(2, 6):
        vsum[n : n + 1] = sums[n]
    vsum[6:8] = jnp.zeros((2, width), F32)
    vsum[0:2] = jnp.zeros((2, width), F32)
    ag_g[1]()
    ag_g[2]()

    gacc = jnp.zeros((qw, width), F32)
    for img in range(nimg):
        gacc = gacc + dot(mix[img], gb[img], 0, 0)
    og[0:qw] = gacc.astype(BF16)
    og[qw:] = jnp.zeros((16, width), BF16)
    zo_first()
    z_merge(1)
    zreduce_own(0)
    f_begin(0)

    def attb_step(img, carry):
        proj, gbi = qkv[img], gb[img]
        gmix = dot(gbi, ow[...], 1, 1).astype(BF16)
        zero = jnp.zeros((length, VEC), BF16)
        dq, dk, dv = [], [], []
        for h in range(2):
            at = VEC + h * HEAD_DIM
            q = proj[:, at : at + HEAD_DIM]
            k = proj[:, qw + at : qw + at + HEAD_DIM]
            v = proj[:, 2 * qw + at : 2 * qw + at + HEAD_DIM]
            gm = gmix[:, h * HEAD_DIM : (h + 1) * HEAD_DIM]
            p = probs[img, h]
            gpr = dot(gm, v, 1, 1)
            gs = (p * (gpr - jnp.sum(p * gpr, axis=-1, keepdims=True))).astype(BF16)
            dq.append((dot(gs, k, 1, 0) * factor).astype(BF16))
            dk.append((dot(gs, q, 0, 0) * factor).astype(BF16))
            dv.append(dot(p.astype(BF16), gm, 0, 0).astype(BF16))
        pad = jnp.zeros((length, cols - VEC - 3 * qw), BF16)
        dqkv[img] = jnp.concatenate([zero] + dq + dk + dv + [pad], axis=1)
        pr = dot(dqkv[img], w[:, 0:cols], 1, 1)
        hat, _ = normalize(xall[img].astype(F32))
        vsum[0:1] = vsum[0:1] + jnp.sum(pr * hat, axis=0, keepdims=True)
        vsum[1:2] = vsum[1:2] + jnp.sum(pr, axis=0, keepdims=True)
        part[img] = pr.astype(BF16)
        return carry

    def gn1_part(img):
        pass
    rs_g1 = rscatter(4, part, r1, (dx, dy, rx, ry), gn1_part)

    def gqkv_step(t, carry):
        r = pl.ds(pl.multiple_of(t * rtile, rtile), rtile)
        acc = jnp.zeros((rtile, cols), F32)
        for img in range(nimg):
            acc = acc + dot(n1[img, :, r], dqkv[img], 0, 0)
        vcol = jnp.transpose(jnp.concatenate([vsum[:, r], jnp.zeros((120, rtile), F32)], axis=0), (1, 0))
        g[r, 0:128] = (acc[:, 0:128] + vcol).astype(BF16)
        g[r, 128 : cols - 128] = acc[:, 128 : cols - 128].astype(BF16)
        g[r, cols - 128 : cols] = (acc[:, cols - 128 :] + gin_tail[r].astype(F32)).astype(BF16)
        return carry

    lax.fori_loop(0, 2, attb_step, 0)
    f_spread(0)
    ib_pass()
    lax.fori_loop(2, nimg, attb_step, 0)
    ib_mid()
    qb_begin()
    lax.fori_loop(0, 3, gqkv_step, 0)
    zo_merge()
    zdrain(0)
    zdrain(1)
    z_first(2)
    z_first(3)
    ib_last()
    rs_g1[0]()
    f_relay(0)
    rs_g1[1]()
    z_merge(2)
    zreduce_own(1)
    f_begin(1)

    for i in range(2):
        gn1 = rs_g1[2](i)
        hat, inv = normalize(xall[2 * y + i, own_rows].astype(F32))
        st_g[i] = (gh_s[i] + norm_back(gn1, g1, hat, inv)).astype(BF16)
    stores[7].start()
    z_merge(3)

    def out_part(img):
        part2[img] = dot(act[img], w[:, out_win : out_win + win], 1, 1).astype(BF16)

    rs_o = rscatter(1, part2, r1b, (dxb, dyb, rxb, ryb), out_part)
    rs_o[0]()
    f_spread(1)
    f_drain(0)
    zreduce_own(2)
    f_begin(2)
    rs_o[1]()
    f_relay(1)
    f_spread(2)
    f_drain(1)
    zreduce_own(3)
    f_begin(3)
    pl.when(z == s)(o_here)
    f_end(0)
    f_end(1)
    emit_out()
    f_relay(2)
    f_spread(3)
    for i in range(2):
        st_o[i] = (hid_s[i] + rs_o[2](i) + out_b).astype(BF16)
    stores[6].start()
    pl.when((s + 2) % 4 == z)(o_x)
    ib_end()
    emit_ib()
    f_end(2)
    emit_upper()
    o_end()
    stores[5].start()
    f_relay(3)
    f_end(3)
    emit_lower()

    for ch in (1, 2):
        gather_drain(ch)
    for ch in (2, 3):
        zdrain(ch)
        f_drain(ch)
    o_drain()
    vec_drain()
    for a in (ag_n, ag_g):
        a[3]()
    rs_o[3]()
    rs_g1[3]()
    pl.when(z != s)(lambda: zo_send(False).wait_send())
    pl.when(z == s)(lambda: o_out_done(2))
    pl.when((z == s) | ((s + 2) % 4 == z))(lambda: o_out_done(3))
    pl.when(z != s)(lambda: qb_send().wait_send())
    for k in range(1, nz):
        ib_send(k).wait_send()
    for n in range(7):
        ib_msg(nz + n, rank, core_n).wait_send()
    for cp in stores:
        cp.wait()


def widen_kernel(n_mat, n_copy, n_row, *refs):
    n = n_mat + n_copy + n_row
    src, refs = refs[:n], refs[n:]
    big, refs = refs[: n_mat + n_copy], refs[n_mat + n_copy :]
    n_flat = (len(refs) - 2 - n - n_mat) // 2
    flat_out, refs = refs[:n_flat], refs[n_flat:]
    held, refs = refs[:n], refs[n:]
    wide, refs = refs[:n_mat], refs[n_mat:]
    flat, (in_s, out_s) = refs[:n_flat], refs[n_flat:]
    got = [pltpu.make_async_copy(src[i], held[i], in_s.at[i]) for i in range(n)]
    put = [pltpu.make_async_copy(wide[i] if i < n_mat else held[i], big[i], out_s.at[i])
           for i in range(n_mat + n_copy)]
    put_flat = [pltpu.make_async_copy(flat[i], flat_out[i], out_s.at[n_mat + n_copy + i]) for i in range(n_flat)]
    for cp in got:
        cp.start()
    for i in range(n_mat + n_copy):
        got[i].wait()
        if i < n_mat:
            rows = wide[i].shape[0]
            for r in range(0, rows, 48):
                wide[i][r : r + 48] = held[i][r : r + 48].astype(F32)
        put[i].start()
    at = 0
    for i in range(n_mat + n_copy, n):
        got[i].wait()
        for r in range(held[i].shape[0]):
            flat[at][...] = held[i][r : r + 1].reshape(held[i].shape[1])
            put_flat[at].start()
            at += 1
    for cp in put + put_flat:
        cp.wait()


def widen(mats, rows, others, tables):
    hbm = pl.BlockSpec(memory_space=pl.ANY)
    arrays = list(mats) + list(others) + list(tables)
    n = len(arrays)
    flat = [jax.ShapeDtypeStruct((t.shape[1],), F32) for t in tables for _ in range(t.shape[0])]
    shapes = [jax.ShapeDtypeStruct((rows, m.shape[1]), F32) for m in mats]
    shapes += [jax.ShapeDtypeStruct(o.shape, o.dtype) for o in others] + flat
    return pl.pallas_call(
        functools.partial(widen_kernel, len(mats), len(others), len(tables)),
        out_shape=tuple(shapes),
        in_specs=[hbm] * n,
        out_specs=[hbm] * len(shapes),
        scratch_shapes=[pltpu.VMEM(a.shape, a.dtype) for a in arrays]
        + [pltpu.VMEM((rows, m.shape[1]), F32) for m in mats]
        + [pltpu.VMEM(f.shape, F32) for f in flat]
        + [pltpu.SemaphoreType.DMA((n,)), pltpu.SemaphoreType.DMA((len(shapes),))],
    )(*arrays)


def layer_fast(
    tokens, cotangent, ln1_gain, ln1_shift, q_weight, q_bias, k_weight, v_weight, v_bias,
    o_weight, o_bias, ln2_gain, ln2_shift, in_weight, in_bias, out_weight, out_bias,
):
    ns, ndp = lax.axis_size("seq"), lax.axis_size("dp")
    nz, ranks = ndp // 2, 2 * ns
    images, own_len, width = tokens.shape
    ff = in_weight.shape[1]
    hid, ffp = width // ranks, ff // ranks
    rows = q_weight.shape[0]
    vec = [ln1_gain, ln1_shift, q_bias, v_bias, o_bias, ln2_gain, ln2_shift, out_bias]
    slab = (2 * VEC, (rows + 127) // 128 * 128)
    total = 3 * 512
    win = (ffp + 127) // 128 * 128
    nimg, length, cols = 2 * images, own_len * ns, 512
    tall = (nimg, length, width)
    half = (own_len, width)
    D = pltpu.SemaphoreType.DMA
    V = pltpu.VMEM
    scratch = dict(
        wp=V((2, rows, total), BF16), fgrad=V((ranks, rows, total), BF16), ograd=V((hid + 16, width), BF16),
        ibgrad=V((ranks, 8, win), F32), st_q=V((rows, width), BF16), st_k=V((rows, width), BF16),
        st_v=V((rows, width), BF16), st_in=V((rows, ff), BF16), st_out=V((rows, ff), BF16),
        vslab=V((2, nz) + slab, BF16), inb=V((8, win), F32), inflat=V((ff,), BF16), inrow=V((1, ff), F32),
        **{f"vflat{n}": V((rows,), BF16) for n in range(VEC)}, vrows=V(slab, F32),
        st_o=V((2,) + half, BF16), st_g=V((2,) + half, BF16), st_vec=V((VEC, rows), F32), st_ib=V((1, ff), F32),
        w=V((2 * nz * rows, total), BF16), ow=V((hid, width), BF16), xall=V(tall, BF16), call=V(tall, BF16),
        n1=V(tall, BF16), n2=V(tall, BF16), gb=V(tall, BF16), qkv=V((nimg, length, cols), BF16),
        probs=V((nimg, 2, length, length), F32), mix=V((nimg, length, hid), BF16),
        act=V((nimg, length, win), BF16), slope=V((nimg, length, win), F32), gp=V((nimg, length, win), BF16),
        part=V(tall, BF16), part2=V(tall, BF16), r1=V((nimg, 2) + half, BF16), r1b=V((nimg, 2) + half, BF16),
        dx=V(half, BF16), dy=V(half, BF16), rx=V((2,) + half, BF16), ry=V((2,) + half, BF16),
        dxb=V(half, BF16), dyb=V(half, BF16), rxb=V((2,) + half, BF16), ryb=V((2,) + half, BF16),
        hid_s=V((2,) + half, F32), hat2_s=V((2,) + half, F32), inv2_s=V((2, own_len, 128), F32),
        gh_s=V((2,) + half, F32), vecs=V((VEC, width), F32),
        g=V((2 * nz * rows, total), BF16), rb=V((2, nz + 1, 2, rows, cols), BF16),
        rbh=V((2, nz + 1, 2, rows, cols // 2), BF16),
        rbo=V((nz + 1, hid + 16, width), BF16), gin_tail=V((width, 128), BF16), gout_tail=V((width, 128), BF16),
        dqkv=V((nimg, length, cols), BF16), vsum=V((8, width), F32), ibx=V((nz, 8, win), F32),
        isb=V((8, win), F32), og=V((hid + 16, width), BF16),
        qbs=V((8, cols), F32), qbx=V((nz, 8, cols), F32),
        gy_s=D((3,)), gz_s=D((2, nz, 2)), gzl_s=D((2, 2)), g_r=D((3, nz, 2)), o_s=D((nz - 1,)), o_r=D((1,)),
        ag_s=D((2, 14)), ag_r=D((2, 14)), rs_s=D((2, 14)), rs_r=D((2, 14)), z_s=D((2, 4, 2)),
        z_r=D((4, nz + 1, 2)), zo_s=D((4,)), zo_r=D((nz + 3,)), f_s=D((2, 7)), f_r=D((4, 7)), ib_s=D((nz + 7,)),
        ib_r=D((nz + 7,)), qb_s=D((1,)), qb_r=D((nz,)), v_s=D((nz,)),
        v_r=D((nz + 1,)), st_s=D((10,)), ld_s=D((20,)),
    )
    hbm = pl.BlockSpec(memory_space=pl.ANY)
    out, gtok, gq, gk, gv, gin, gout, go, gvec, gib = pl.pallas_call(
        functools.partial(layer_kernel, nz, hid, ffp),
        out_shape=(
            jax.ShapeDtypeStruct(tokens.shape, BF16), jax.ShapeDtypeStruct(tokens.shape, BF16),
            jax.ShapeDtypeStruct((rows, width), BF16), jax.ShapeDtypeStruct((rows, width), BF16),
            jax.ShapeDtypeStruct((rows, width), BF16), jax.ShapeDtypeStruct((rows, ff), BF16),
            jax.ShapeDtypeStruct((rows, ff), BF16), jax.ShapeDtypeStruct((hid + 16, width), BF16),
            jax.ShapeDtypeStruct((VEC, rows), F32), jax.ShapeDtypeStruct((1, ff), F32),
        ),
        in_specs=[hbm] * (9 + VEC),
        out_specs=[hbm] * 10,
        scratch_shapes=list(scratch.values()),
        compiler_params=pltpu.CompilerParams(
            collective_id=0, has_side_effects=True, vmem_limit_bytes=65000 * 1024),
    )(tokens, cotangent, q_weight, k_weight, v_weight, in_weight, out_weight.T, o_weight, in_bias, *vec)
    (gin, gout, gq, gk, gv, go, out, gtok, d_g1, d_s1, d_g2, d_s2, d_ob, d_outb, d_qb, d_vb, gib) = widen(
        [gin, gout, gq, gk, gv, go], rows, [out, gtok], [gvec, gib])
    return (out, gtok, d_g1, d_s1, gq, d_qb, gk, gv, d_vb, go, d_ob, d_g2, d_s2, gin, gib, gout.T, d_outb)


def mm(a, b, ca, cb):
    return lax.dot_general(a, b, (((ca,), (cb,)), ((), ())), preferred_element_type=F32)


def on_device(
    tokens, cotangent, ln1_gain, ln1_shift, q_weight, q_bias, k_weight, v_weight, v_bias,
    o_weight, o_bias, ln2_gain, ln2_shift, in_weight, in_bias, out_weight, out_bias,
):
    part = lax.axis_index("seq")
    parts = lax.axis_size("seq")
    groups = lax.axis_size("dp")
    images, own_len, width = tokens.shape
    ff = in_weight.shape[1]
    hid = width // parts
    ffp = ff // parts
    heads = HEADS // parts
    length = own_len * parts
    rows = images * length

    def cols(w, n):
        return lax.dynamic_slice_in_dim(w, part * n, n, axis=1)

    vecs = jnp.stack(
        [ln1_gain, ln1_shift, q_bias, v_bias, o_bias, ln2_gain, ln2_shift, out_bias]
    )
    vecs = lax.all_gather(vecs, "dp", axis=1, tiled=True).astype(F32)
    g1, s1, qb, vb, ob, g2, s2, outb = [vecs[i] for i in range(8)]
    x = lax.all_gather(tokens, "seq", axis=1, tiled=True).reshape(rows, width)
    cot = lax.all_gather(cotangent, "seq", axis=1, tiled=True).reshape(rows, width)
    qkv = jnp.concatenate([cols(q_weight, hid), cols(k_weight, hid), cols(v_weight, hid)], axis=1)
    qkv = lax.all_gather(qkv, "dp", axis=0, tiled=True)
    o_w = lax.all_gather(o_weight, "dp", axis=0, tiled=True)
    o_w = lax.dynamic_slice_in_dim(o_w, part * hid, hid, axis=0)
    in_w = lax.all_gather(cols(in_weight, ffp), "dp", axis=0, tiled=True)
    out_w = lax.dynamic_slice_in_dim(out_weight, part * ffp, ffp, axis=0)
    out_w = lax.all_gather(out_w.T, "dp", axis=0, tiled=True)
    qb_own = lax.dynamic_slice_in_dim(qb, part * hid, hid)
    vb_own = lax.dynamic_slice_in_dim(vb, part * hid, hid)
    inb_own = lax.dynamic_slice_in_dim(in_bias, part * ffp, ffp).astype(F32)

    def scatter_tokens(partial):
        return lax.psum_scatter(
            partial.astype(BF16).reshape(images, length, width),
            "seq", scatter_dimension=1, tiled=True,
        ).astype(F32)

    hat1, _ = normalize(x.astype(F32))
    normed1 = (hat1 * g1 + s1).astype(BF16)
    proj = mm(normed1, qkv, 1, 0)
    queries = (proj[:, :hid] + qb_own).astype(BF16).reshape(images, length, heads, HEAD_DIM)
    keys = proj[:, hid : 2 * hid].astype(BF16).reshape(images, length, heads, HEAD_DIM)
    values = (proj[:, 2 * hid :] + vb_own).astype(BF16).reshape(images, length, heads, HEAD_DIM)
    factor = 1.0 / math.sqrt(HEAD_DIM)
    ein = lambda s, a, b: jnp.einsum(s, a, b, preferred_element_type=F32)
    scores = ein("iqhd,ikhd->ihqk", queries, keys) * factor
    top = jnp.max(scores, axis=-1, keepdims=True)
    expo = jnp.exp(scores - top)
    probs = expo / jnp.sum(expo, axis=-1, keepdims=True)
    probs_low = probs.astype(BF16)
    mixed = ein("ihqk,ikhd->iqhd", probs_low, values).astype(BF16).reshape(rows, hid)
    start = tokens.astype(F32)
    hidden = start + scatter_tokens(mm(mixed, o_w, 1, 0)) + ob
    hat2, r2 = normalize(hidden)
    normed2 = (hat2 * g2 + s2).astype(BF16)
    normed2 = lax.all_gather(normed2, "seq", axis=1, tiled=True).reshape(rows, width)
    pre = mm(normed2, in_w, 1, 0) + inb_own
    act, slope = gelu_parts(pre)
    act = act.astype(BF16)
    out = hidden + scatter_tokens(mm(act, out_w, 1, 1)) + outb
    d_out_w = mm(cot, act, 0, 0)
    cot_own = cotangent.astype(F32)
    grad_pre = (mm(cot, out_w, 1, 0) * slope).astype(BF16)
    d_in_w = mm(normed2, grad_pre, 0, 0)
    d_in_b = jnp.sum(grad_pre.astype(F32), axis=0)
    grad_n2 = scatter_tokens(mm(grad_pre, in_w, 1, 1))
    grad_hidden = cot_own + norm_back(grad_n2, g2, hat2, r2)
    branch_own = grad_hidden.astype(BF16)
    branch = lax.all_gather(branch_own, "seq", axis=1, tiled=True).reshape(rows, width)
    d_o_w = mm(mixed, branch, 0, 0)
    grad_mixed = mm(branch, o_w, 1, 1).astype(BF16).reshape(images, length, heads, HEAD_DIM)
    grad_probs = ein("iqhd,ikhd->ihqk", grad_mixed, values)
    row_dot = jnp.sum(probs * grad_probs, axis=-1, keepdims=True)
    grad_scores = (probs * (grad_probs - row_dot)).astype(BF16)
    grad_q = (ein("ihqk,ikhd->iqhd", grad_scores, keys) * factor).astype(BF16).reshape(rows, hid)
    grad_k = (ein("ihqk,iqhd->ikhd", grad_scores, queries) * factor).astype(BF16).reshape(rows, hid)
    grad_v = ein("ihqk,iqhd->ikhd", probs_low, grad_mixed).astype(BF16).reshape(rows, hid)
    grad_qkv = jnp.concatenate([grad_q, grad_k, grad_v], axis=1)
    d_qkv = mm(normed1, grad_qkv, 0, 0)
    d_qb = jnp.sum(grad_q.astype(F32), axis=0)
    d_vb = jnp.sum(grad_v.astype(F32), axis=0)
    grad_n1 = scatter_tokens(mm(grad_qkv, qkv, 1, 1))
    hat1o, r1o = normalize(start)
    grad_tokens = grad_hidden + norm_back(grad_n1, g1, hat1o, r1o)
    wide = jnp.concatenate([d_qkv, d_in_w, d_out_w], axis=1).astype(BF16)
    wide = lax.psum_scatter(wide, "dp", scatter_dimension=0, tiled=True)
    wide = lax.all_gather(wide, "seq", axis=0, tiled=False).astype(F32)

    def spread(lo, n):
        return wide[:, :, lo : lo + n].transpose(1, 0, 2).reshape(width // groups, n * parts)

    gq, gk, gv = [spread(i * hid, hid) for i in range(3)]
    gin = spread(3 * hid, ffp)
    gout = wide[:, :, 3 * hid + ffp :].transpose(0, 2, 1).reshape(ff, width // groups)
    o_full = lax.all_gather(
        lax.psum_scatter(d_o_w.astype(BF16), "dp", scatter_dimension=1, tiled=True),
        "seq", axis=0, tiled=True,
    )
    go = lax.all_to_all(o_full, "dp", split_axis=0, concat_axis=1, tiled=True).astype(F32)
    own_sums = jnp.stack([
        jnp.sum(grad_n1 * hat1o, axis=(0, 1)), jnp.sum(grad_n1, axis=(0, 1)),
        jnp.sum(grad_n2 * hat2, axis=(0, 1)), jnp.sum(grad_n2, axis=(0, 1)),
        jnp.sum(branch_own.astype(F32), axis=(0, 1)), jnp.sum(cot_own, axis=(0, 1)),
        lax.dynamic_update_slice_in_dim(jnp.zeros(width, F32), d_qb, part * hid, 0),
        lax.dynamic_update_slice_in_dim(jnp.zeros(width, F32), d_vb, part * hid, 0),
    ])
    bias_in = lax.dynamic_update_slice_in_dim(jnp.zeros(ff, F32), d_in_b, part * ffp, 0)
    total = lax.psum(jnp.concatenate([own_sums.reshape(-1), bias_in]), ("dp", "seq"))
    vec_part = total[: 8 * width].reshape(8, groups, width // groups)
    vec_part = lax.dynamic_index_in_dim(vec_part, lax.axis_index("dp"), axis=1, keepdims=False)
    bias_total = total[8 * width :]
    return (
        out.astype(BF16), grad_tokens.astype(BF16), vec_part[0], vec_part[1], gq, vec_part[6],
        gk, gv, vec_part[7], go, vec_part[4], vec_part[2], vec_part[3], gin, bias_total, gout,
        vec_part[5],
    )


def solution(mesh):
    fast = mesh.shape["dp"] == 2 * mesh.shape["seq"]
    rows, vec = P("dp", None), P("dp")
    tok = P("dp", "seq", None)
    return jax.shard_map(
        layer_fast if fast else on_device,
        mesh=mesh,
        in_specs=(tok, tok, vec, vec, rows, vec, rows, rows, vec, rows, vec, vec, vec, rows,
                  P(), P(None, "dp"), vec),
        out_specs=(tok, tok, vec, vec, rows, vec, rows, rows, vec, rows, vec, vec, vec, rows,
                   P(), P(None, "dp"), vec),
        check_vma=False,
    )
```

```python
import functools
import math

import jax
import jax.numpy as jnp
from jax import lax
from jax.experimental import pallas as pl
from jax.experimental.pallas import tpu as pltpu
from jax.sharding import PartitionSpec as P

BF16, F32 = jnp.bfloat16, jnp.float32
HEADS, HEAD_DIM = 16, 72
eps_norm = 1e-06
gelu_coef = 0.7978845608028654
gelu_cube = 0.044715
MESH = pl.DeviceIdType.MESH
VEC = 8


def normalize(values):
    row_mean = jnp.mean(values, axis=-1, keepdims=True)
    centred = values - row_mean
    inverse = lax.rsqrt(jnp.mean(centred * centred, axis=-1, keepdims=True) + eps_norm)
    return centred * inverse, inverse


def norm_back(grad_normed, gain_vec, scaled, inverse):
    grad_scaled = grad_normed * gain_vec
    centred_grad = grad_scaled - jnp.mean(grad_scaled, axis=-1, keepdims=True)
    return inverse * (
        centred_grad - scaled * jnp.mean(grad_scaled * scaled, axis=-1, keepdims=True)
    )


def gelu_parts(pre_act):
    square = pre_act * pre_act
    tanh_val = jnp.tanh(pre_act * (gelu_coef + gelu_coef * gelu_cube * square))
    gate = 0.5 + 0.5 * tanh_val
    value_part = pre_act * gate
    slope_part = gate + value_part * (1.0 - gate) * (2.0 * gelu_coef + 6.0 * gelu_coef * gelu_cube * square)
    return (value_part, slope_part)


def dot(a, b, ca, cb):
    return lax.dot_general(a, b, (((ca,), (cb,)), ((), ())), preferred_element_type=F32)


def layer_kernel(
    nz, hid, ffp,
    tok, cot_in, q_in, k_in, v_in, in_in, out_in, ow_in, inb_in, vin0, vin1, vin2, vin3, vin4, vin5, vin6, vin7,
    out_ref, gtok_ref, q_out, k_out, v_out, in_out, out_out, o_out, vec_out, ib_out,
    wp, fgrad, ograd, ibgrad, st_q, st_k, st_v, st_in, st_out, vslab, inb, inflat, inrow, vflat0, vflat1, vflat2, vflat3, vflat4, vflat5, vflat6, vflat7, vrows, st_o, st_g, st_vec, st_ib,
    w, ow, xall, call, n1, n2, gb, qkv, probs, mix, act, slope, gp, part, part2, r1, r1b,
    dx, dy, rx, ry, dxb, dyb, rxb, ryb, hid_s, hat2_s, inv2_s, gh_s, vecs, g, rb, rbh, rbo, gin_tail,
    gout_tail, dqkv, vsum, mean1, inv1, ibx, isb, og, qbs, qbx,
    gy_s, gz_s, gzl_s, g_r, o_s, o_r, ag_s, ag_r, rs_s, rs_r, z_s, z_r, zo_s, zo_r, f_s, f_r,
    ib_s, ib_r, qb_s, qb_r, v_s, v_r,
):
    d, s = lax.axis_index("dp"), lax.axis_index("seq")
    z, y = d // 2, d % 2
    x, c = s // 2, s % 2
    rank = 2 * s + y
    nimg, length, width = xall.shape
    own_len = dx.shape[0]
    rows8 = wp.shape[1]
    plane = 2 * rows8
    cols = 512
    qw = hid
    in_at = VEC + 3 * qw
    in_win = in_at // 128 * 128
    out_at = in_at + ffp
    out_win = out_at // 128 * 128
    win = (ffp + 127) // 128 * 128
    off_in, off_out = in_at - in_win, out_at - out_win
    shift = off_out - off_in
    core_n, x_n, y_n = (d, s + 1 - 2 * c), (d, (s + 2) % 4), (d + 1 - 2 * y, s)
    right, left = (d + 2, s), (d - 2, s)
    has_r, has_l = z < nz - 1, z > 0
    sg = 1 - 2 * (z // 2)
    is_end = (z == 0) | (z == nz - 1)
    middle = (z > 0) & (z < nz - 1)
    factor = 1.0 / math.sqrt(HEAD_DIM)

    def plane_at(k):
        return z + sg * k

    def away(k):
        return (d + 2 * sg * k, s)

    def rc(src, dst, ss, rs, dev):
        return pltpu.make_async_remote_copy(
            src_ref=src, dst_ref=dst, send_sem=ss, recv_sem=rs, device_id=dev, device_id_type=MESH
        )

    barrier = pltpu.get_barrier_semaphore()
    column = [((d + 2 * k) % (2 * nz), s) for k in range(1, nz)]
    for dev in [core_n, x_n, y_n] + column:
        pl.semaphore_signal(barrier, inc=1, device_id=dev, device_id_type=MESH)

    own_rows = pl.ds(pl.multiple_of(s * own_len, 16), own_len)
    vflat = (vflat0, vflat1, vflat2, vflat3, vflat4, vflat5, vflat6, vflat7)
    vec_loads = list(zip((vin0, vin1, vin2, vin3, vin4, vin5, vin6, vin7), vflat))
    loads = [pltpu.make_async_copy(a, b, rs_s.at[n // 14, n % 14]) for n, (a, b) in enumerate(
        vec_loads + [(q_in, st_q), (k_in, st_k), (v_in, st_v), (in_in, st_in),
         (tok.at[0], xall.at[2 * y, own_rows]), (tok.at[1], xall.at[2 * y + 1, own_rows]), (out_in, st_out),
         (cot_in.at[0], call.at[2 * y, own_rows]), (cot_in.at[1], call.at[2 * y + 1, own_rows]),
         (inb_in, inflat)])]
    for cp in loads:
        cp.start()
    load_o = pltpu.make_async_copy(ow_in, ow, rs_s.at[1, 13])
    pl.when(z == s)(lambda: load_o.start())

    def build_first():
        def go(k):
            for j in range(2):
                t = 2 * k + j
                wp[j, :, 0:128] = jnp.zeros((rows8, 128), BF16)
                for n, st in enumerate((st_q, st_k, st_v)):
                    wp[j, :, VEC + n * qw : VEC + (n + 1) * qw] = st[:, t * qw : (t + 1) * qw]
                wp[j, :, in_at:cols] = st_in[:, t * ffp : t * ffp + cols - in_at]
        for k in range(4):
            pl.when(s == k)(functools.partial(go, k))

    def build_rest():
        def go(k):
            for j in range(2):
                t = 2 * k + j
                wp[j, :, 3 * cols - 128 :] = jnp.zeros((rows8, 128), BF16)
                wp[j, :, cols : in_at + ffp] = st_in[:, t * ffp + cols - in_at : (t + 1) * ffp]
                wp[j, :, out_at : out_at + ffp] = st_out[:, t * ffp : (t + 1) * ffp]
        for k in range(4):
            pl.when(s == k)(functools.partial(go, k))

    def build_bias():
        def go(t):
            inb[...] = jnp.zeros_like(inb)
            inb[0:1, off_in : off_in + ffp] = inrow[0:1, t * ffp : (t + 1) * ffp]
        for t in range(8):
            pl.when(rank == t)(functools.partial(go, t))

    for cp in loads[: VEC + 6]:
        cp.wait()
    vrows[...] = jnp.zeros_like(vrows)
    for n in range(VEC):
        vrows[n : n + 1, 0:rows8] = vflat[n][...].astype(F32).reshape(1, rows8)
    vslab[y, z] = vrows[...].astype(BF16)
    build_first()
    pl.semaphore_wait(barrier, 3 + len(column))

    def wrows(origin, sub):
        return pl.ds(pl.multiple_of(origin * plane + sub * rows8, 16), rows8)

    def wslab(ch, origin, sub):
        return w.at[wrows(origin, sub), pl.ds(ch * cols, cols)]

    def wsend(ch, origin, sub, src, to_right, own=False):
        sems = gz_s.at[ch % 2, origin, sub] if to_right or not own else gzl_s.at[ch % 2, sub]
        return rc(src, wslab(ch, origin, sub), sems, g_r.at[ch, origin, sub],
                  right if to_right else left)

    def wrecv(ch, origin, sub):
        slab = wslab(ch, origin, sub)
        rc(slab, slab, g_r.at[ch, origin, sub], g_r.at[ch, origin, sub], core_n).wait_recv()

    def gather_own(ch):
        src = wp.at[y, :, pl.ds(ch * cols, cols)]
        pl.when(has_r)(lambda: wsend(ch, z, y, src, True).start())
        pl.when(has_l)(lambda: wsend(ch, z, y, src, False, True).start())
        w[wrows(z, y), ch * cols : (ch + 1) * cols] = wp[y, :, ch * cols : (ch + 1) * cols]

    def gather_swap(ch):
        rc(wp.at[1 - y, :, pl.ds(ch * cols, cols)], wslab(ch, z, y), gy_s.at[ch], g_r.at[ch, z, y],
           y_n).start()

    def gather_other(ch):
        wrecv(ch, z, 1 - y)
        src = wslab(ch, z, 1 - y)
        pl.when(has_r)(lambda: wsend(ch, z, 1 - y, src, True).start())
        pl.when(has_l)(lambda: wsend(ch, z, 1 - y, src, False, True).start())

    def gather_hop(ch, k):
        for sub in range(2):
            gather_hop1(ch, k, sub)

    def gather_end(ch):
        for k in range(1, nz):
            for sub in range(2):
                pl.when(is_end)(lambda: wrecv(ch, plane_at(k), sub))

    def gather_hop1(ch, k, sub):
        def from_left():
            wrecv(ch, z - k, sub)
            pl.when(has_r)(lambda: wsend(ch, z - k, sub, wslab(ch, z - k, sub), True).start())

        def from_right():
            wrecv(ch, z + k, sub)
            pl.when(has_l)(lambda: wsend(ch, z + k, sub, wslab(ch, z + k, sub), False).start())

        pl.when(middle & (z - k >= 0))(from_left)
        pl.when(middle & (z + k < nz))(from_right)

    def gather_drain(ch):
        for k in range(nz):
            for sub in range(2):
                pl.when((z - k >= 0) & has_r)(
                    lambda: wsend(ch, z - k, sub, wslab(ch, z - k, sub), True).wait_send())
                pl.when((z + k < nz) & has_l)(
                    lambda: wsend(ch, z + k, sub, wslab(ch, z + k, sub), False, k == 0).wait_send())
        rc(wp.at[1 - y, :, pl.ds(ch * cols, cols)], wslab(ch, z, y), gy_s.at[ch], g_r.at[ch, z, y],
           y_n).wait_send()

    def osend(to_right):
        return rc(ow, ow, o_s.at[0 if to_right else 1], o_r.at[0], right if to_right else left)

    def o_own(when):
        def outer():
            load_o.wait()
            pl.when(has_r)(lambda: osend(True).start())
            pl.when(has_l)(lambda: osend(False).start())

        def inner():
            load_o.wait()
            pl.when(z == 1)(lambda: osend(True).start())
            pl.when(z == 2)(lambda: osend(False).start())

        def last():
            pl.when(z == 1)(lambda: osend(False).start())
            pl.when(z == 2)(lambda: osend(True).start())
        cond = is_end if when == 0 else middle
        pl.when((z == s) & cond)((outer, inner, last)[when])

    def o_take():
        osend(True).wait_recv()

    def o_pass(when):
        def go():
            o_take()
            pl.when((z > s) & has_r)(lambda: osend(True).start())
            pl.when((z < s) & has_l)(lambda: osend(False).start())
        near = (s == 0) & (z == 1) | (s == 3) & (z == 2)
        cross = (s == 1) & (z == 2) | (s == 2) & (z == 1)
        far = (s == 0) & (z == 2) | (s == 3) & (z == 1)
        pl.when((near, cross, far)[when])(go)

    def o_wait():
        pl.when((z != s) & is_end)(o_take)

    def o_drain():
        pl.when((z >= s) & has_r)(lambda: osend(True).wait_send())
        pl.when((z <= s) & has_l)(lambda: osend(False).wait_send())

    def agather(inst, dst):
        ss, rr = (rs_s.at[1], rs_r.at[1]) if inst == 1 else (ag_s, ag_r)

        def blk(yy, sq, i):
            return dst.at[2 * yy + i, pl.ds(pl.multiple_of(sq * own_len, 16), own_len)]

        sx, sp = (s + 2) % 4, s + 1 - 2 * c
        spx = (sp + 2) % 4

        def msg(n, block, dev):
            return rc(block, block, ss.at[n], rr.at[n], dev)

        mine = [blk(y, s, i) for i in range(2)]
        xs = [blk(y, sx, i) for i in range(2)]
        ys = [blk(1 - y, s, i) for i in range(2)]
        dg = [blk(1 - y, sx, i) for i in range(2)]
        sends = [msg(0, mine[0], x_n), msg(1, mine[1], x_n), msg(2, ys[1], x_n),
                 msg(3, mine[0], y_n), msg(4, mine[1], y_n), msg(5, xs[0], y_n)]
        sends += [msg(6 + i, mine[i], core_n) for i in range(2)]
        sends += [msg(8 + i, xs[i], core_n) for i in range(2)]
        sends += [msg(10 + i, ys[i], core_n) for i in range(2)]
        sends += [msg(12 + i, dg[i], core_n) for i in range(2)]
        recvs = [msg(0, xs[0], x_n), msg(1, xs[1], x_n), msg(2, dg[1], x_n),
                 msg(3, ys[0], y_n), msg(4, ys[1], y_n), msg(5, dg[0], y_n)]
        recvs += [msg(6 + i, blk(y, sp, i), core_n) for i in range(2)]
        recvs += [msg(8 + i, blk(y, spx, i), core_n) for i in range(2)]
        recvs += [msg(10 + i, blk(1 - y, sp, i), core_n) for i in range(2)]
        recvs += [msg(12 + i, blk(1 - y, spx, i), core_n) for i in range(2)]

        def begin():
            for n in (0, 4, 1, 3, 6, 7):
                sends[n].start()

        def relay(parts=(0, 1, 2, 3)):
            if 0 in parts:
                recvs[0].wait_recv()
                sends[5].start()
                sends[8].start()
            if 1 in parts:
                recvs[4].wait_recv()
                sends[2].start()
                sends[11].start()
            if 2 in parts:
                recvs[1].wait_recv()
                sends[9].start()
            if 3 in parts:
                recvs[3].wait_recv()
                sends[10].start()

        def finish(parts=(0, 1)):
            if 0 in parts:
                recvs[2].wait_recv()
                sends[13].start()
                recvs[5].wait_recv()
                sends[12].start()
            if 1 in parts:
                for n in range(6, 14):
                    recvs[n].wait_recv()

        def drain():
            for m in sends:
                m.wait_send()

        return begin, relay, finish, drain

    def rscatter(inst, pt, ra, bufs, produce):
        bdx, bdy, brx, bry = bufs
        ss, rr = rs_s.at[inst % 2], rs_r.at[inst % 2]
        xo = 1 - x

        def image(it):
            return (2 * (1 - y) + it) % 4

        def rows(xx, cc):
            return pl.ds(pl.multiple_of((2 * xx + cc) * own_len, 16), own_len)

        def swap(it, xx):
            img = image(it)
            return rc(pt.at[img, rows(xx, 1 - c)], ra.at[img, xx], ss.at[2 * it + xx],
                      rr.at[2 * it + xx], core_n)

        def add(it, xx):
            swap(it, xx).wait_recv()
            img = image(it)
            ra[img, xx] = (ra[img, xx].astype(F32) + pt[img, rows(xx, c)].astype(F32)).astype(BF16)

        m = [
            rc(ra.at[image(0), xo], bdx, ss.at[8], rr.at[8], x_n),
            rc(ra.at[image(1), xo], bdy, ss.at[9], rr.at[9], y_n),
            rc(ra.at[image(1), x], bry.at[1], ss.at[10], rr.at[10], y_n),
            rc(ra.at[image(2), xo], brx.at[0], ss.at[11], rr.at[11], x_n),
            rc(ra.at[image(0), x], bry.at[0], ss.at[12], rr.at[12], y_n),
            rc(ra.at[image(3), xo], brx.at[1], ss.at[13], rr.at[13], x_n),
        ]

        def run_a():
            def step(it, carry):
                produce(image(it))
                swap(it, xo).start()
                swap(it, x).start()
                return carry
            lax.fori_loop(0, nimg, step, 0)

        def run_c():
            add(0, xo)
            m[0].start()
            add(1, xo)
            m[1].start()
            add(1, x)
            m[2].start()
            add(2, xo)
            m[3].start()
            add(0, x)
            add(3, xo)

        def run_b():
            m[0].wait_recv()
            ra[image(0), x] = (ra[image(0), x].astype(F32) + bdx[...].astype(F32)).astype(BF16)
            m[4].start()
            m[1].wait_recv()
            ra[image(3), xo] = (ra[image(3), xo].astype(F32) + bdy[...].astype(F32)).astype(BF16)
            m[5].start()
            add(2, x)
            add(3, x)

        def result(i):
            rc(brx.at[i], brx.at[i], ss.at[11 + 2 * i], rr.at[11 + 2 * i], x_n).wait_recv()
            rc(bry.at[i], bry.at[i], ss.at[12 - 2 * i], rr.at[12 - 2 * i], y_n).wait_recv()
            return (ra[image(2 + i), x].astype(F32) + brx[i].astype(F32)) + bry[i].astype(F32)

        def drain():
            for it in range(nimg):
                swap(it, 0).wait_send()
                swap(it, 1).wait_send()
            for n in range(8, 14):
                rc(bdx, bdx, ss.at[n], rr.at[n], x_n).wait_send()

        return run_a, run_b, result, drain, run_c

    zch = [(2 * cols, cols), (cols, cols), (cols // 2, cols // 2), (0, cols // 2)]
    order = (1 - y, y)

    def rb_at(ch, slot, sub):
        return (rb if ch < 2 else rbh).at[ch % 2, slot, sub]

    def gslab(ch, dest, sub):
        return g.at[wrows(dest, sub), pl.ds(*zch[ch])]

    def zsend(ch, where, sub, outer):
        k = (1, 2, 3, -1)[where]
        to, slot = (1, (z, nz + 1, nz)[where]) if outer else (k, z)
        return rc(gslab(ch, plane_at(k), sub), rb_at(ch, slot, sub), z_s.at[(0, 1, 0, 2)[ch], where, sub],
                  z_r.at[ch, slot, sub], away(to))

    def zadd(ch, dest, slot, sub):
        ref = rb_at(ch, slot, sub)
        rc(ref, ref, z_r.at[ch, slot, sub], z_r.at[ch, slot, sub], core_n).wait_recv()
        r, cs = wrows(dest, sub), slice(zch[ch][0], sum(zch[ch]))
        g[r, cs] = (g[r, cs].astype(F32) + ref[...].astype(F32)).astype(BF16)

    def z_first(ch, parts=(2, 1, 0, 3)):
        def outer():
            for where in (2, 1, 0):
                if where in parts:
                    for sub in order:
                        zsend(ch, where, sub, True).start()

        def inner():
            if 3 in parts:
                for sub in order:
                    zsend(ch, 3, sub, False).start()
        pl.when(is_end)(outer)
        pl.when(middle)(inner)

    def z_merge(ch, where):
        def inner():
            for sub in order:
                zadd(ch, plane_at(where + 1), nz + 1 - where, sub)
                zsend(ch, where, sub, False).start()
        pl.when(middle)(inner)

    def zreduce_own(ch):
        def outer(sub):
            zadd(ch, z, plane_at(1), sub)
            zadd(ch, z, plane_at(2), sub)

        def inner(sub):
            zadd(ch, z, plane_at(-1), sub)
            zadd(ch, z, plane_at(1), sub)
        for sub in order:
            pl.when(is_end)(functools.partial(outer, sub))
            pl.when(middle)(functools.partial(inner, sub))

    def zdrain(ch):
        for sub in range(2):
            zsend(ch, 0, sub, False).wait_send()
            zsend(ch, 1, sub, False).wait_send()
            pl.when(is_end)(lambda: zsend(ch, 2, sub, True).wait_send())
            pl.when(middle)(lambda: zsend(ch, 3, sub, False).wait_send())

    def f_swap(ch):
        src = g.at[wrows(z, 1 - y), pl.ds(*zch[ch])]
        return rc(src, fgrad.at[rank, :, pl.ds(*zch[ch])], f_s.at[ch % 2, 0], f_r.at[ch, 0], y_n)

    def f_msg(ch, n, slot, dev):
        piece = fgrad.at[slot, :, pl.ds(*zch[ch])]
        return rc(piece, piece, f_s.at[ch % 2, n], f_r.at[ch, n], dev)

    sx, sp = (s + 2) % 4, s + 1 - 2 * c
    spx = (sp + 2) % 4

    def f_begin(ch):
        f_swap(ch).start()
        cs = slice(zch[ch][0], sum(zch[ch]))
        fgrad[rank, :, cs] = g[wrows(z, y), cs]
        f_msg(ch, 1, rank, x_n).start()
        f_msg(ch, 3, rank, core_n).start()

    def f_spread(ch):
        other = 2 * s + 1 - y
        f_msg(ch, 0, other, y_n).wait_recv()
        f_msg(ch, 2, other, x_n).start()
        f_msg(ch, 4, other, core_n).start()

    def f_relay(ch):
        f_msg(ch, 1, 2 * sx + y, x_n).wait_recv()
        f_msg(ch, 5, 2 * sx + y, core_n).start()
        f_msg(ch, 2, 2 * sx + 1 - y, x_n).wait_recv()
        f_msg(ch, 6, 2 * sx + 1 - y, core_n).start()

    def f_end(ch):
        f_msg(ch, 3, 2 * sp + y, core_n).wait_recv()
        f_msg(ch, 4, 2 * sp + 1 - y, core_n).wait_recv()
        f_msg(ch, 5, 2 * spx + y, core_n).wait_recv()
        f_msg(ch, 6, 2 * spx + 1 - y, core_n).wait_recv()

    def f_drain(ch):
        f_swap(ch).wait_send()
        for n in range(1, 7):
            f_msg(ch, n, rank, core_n).wait_send()

    far_out = is_end & (plane_at(0) != s) & (plane_at(1) != s)
    adds = middle & ((plane_at(1) == s) | (plane_at(2) == s))

    def zo_send(far):
        if far:
            return rc(og, rbo.at[nz], zo_s.at[0], zo_r.at[nz], away(1))
        return rc(og, rbo.at[z], zo_s.at[0], zo_r.at[z], (2 * s + y, s))

    def zo_add(slot):
        rc(rbo.at[slot], rbo.at[slot], zo_s.at[0], zo_r.at[slot], core_n).wait_recv()
        og[...] = (og[...].astype(F32) + rbo[slot].astype(F32)).astype(BF16)

    def zo_first():
        pl.when(far_out)(lambda: zo_send(True).start())
        pl.when(jnp.logical_not(far_out | adds) & (z != s))(lambda: zo_send(False).start())

    def zo_merge():
        def go():
            zo_add(nz)
            zo_send(False).start()
        pl.when(adds)(go)

    def zo_last():
        def outer():
            zo_add(plane_at(1))
            zo_add(plane_at(2))

        def inner():
            zo_add(plane_at(-1))
            zo_add(plane_at(1))
        pl.when(is_end)(outer)
        pl.when(middle)(inner)

    def qb_send():
        return rc(qbs, qbx.at[z], qb_s.at[0], qb_r.at[z], (2 * s + y, s))

    def qb_begin():
        bsum = jnp.zeros((1, cols), F32)
        for img in range(nimg):
            bsum = bsum + jnp.sum(dqkv[img].astype(F32), axis=0, keepdims=True)
        qbs[...] = jnp.broadcast_to(bsum, (8, cols))
        pl.when(z != s)(lambda: qb_send().start())

    def o_here():
        zo_last()
        total = qbs[...]
        for k in range(1, nz):
            zz = (z + k) % nz
            rc(qbs, qbx.at[zz], qb_s.at[0], qb_r.at[zz], core_n).wait_recv()
            total = total + qbx[zz]
        og[qw:, 0:cols] = jnp.concatenate([total, total], axis=0).astype(BF16)
        ograd[...] = og[...]
        rc(ograd, ograd, zo_s.at[2], zo_r.at[nz + 1], x_n).start()
        rc(ograd, ograd, zo_s.at[3], zo_r.at[nz + 2], core_n).start()

    def o_x():
        rc(ograd, ograd, zo_s.at[2], zo_r.at[nz + 1], x_n).wait_recv()
        rc(ograd, ograd, zo_s.at[3], zo_r.at[nz + 2], core_n).start()

    def o_end():
        pl.when((sp == z) | (spx == z))(
            lambda: rc(ograd, ograd, zo_s.at[3], zo_r.at[nz + 2], core_n).wait_recv())

    def o_out_done(n):
        rc(ograd, ograd, zo_s.at[n], zo_r.at[0], core_n).wait_send()

    def ib_send(k):
        return rc(isb, ibx.at[z], ib_s.at[k - 1], ib_r.at[z], ((d + 2 * k) % (2 * nz), s))

    def ib_begin():
        ib = jnp.zeros((1, win), F32)
        for img in range(nimg):
            ib = ib + jnp.sum(gp[img].astype(F32), axis=0, keepdims=True)
        isb[...] = jnp.broadcast_to(ib, (8, win))
        for k in range(1, nz):
            ib_send(k).start()

    def ib_msg(n, slot, dev):
        return rc(ibgrad.at[slot], ibgrad.at[slot], ib_s.at[n], ib_r.at[n], dev)

    def ib_pass():
        ibsum = isb[...]
        for k in range(1, nz):
            zz = (z + k) % nz
            rc(isb, ibx.at[zz], ib_s.at[0], ib_r.at[zz], core_n).wait_recv()
            ibsum = ibsum + ibx[zz]
        ibgrad[rank] = ibsum
        ib_msg(nz, rank, y_n).start()
        ib_msg(nz + 1, rank, x_n).start()
        ib_msg(nz + 3, rank, core_n).start()

    def ib_mid():
        other = 2 * s + 1 - y
        ib_msg(nz, other, y_n).wait_recv()
        ib_msg(nz + 2, other, x_n).start()
        ib_msg(nz + 4, other, core_n).start()
        ib_msg(nz + 1, 2 * sx + y, x_n).wait_recv()
        ib_msg(nz + 5, 2 * sx + y, core_n).start()

    def ib_last():
        ib_msg(nz + 2, 2 * sx + 1 - y, x_n).wait_recv()
        ib_msg(nz + 6, 2 * sx + 1 - y, core_n).start()

    def ib_end():
        ib_msg(nz + 3, 2 * sp + y, core_n).wait_recv()
        ib_msg(nz + 4, 2 * sp + 1 - y, core_n).wait_recv()
        ib_msg(nz + 5, 2 * spx + y, core_n).wait_recv()
        ib_msg(nz + 6, 2 * spx + 1 - y, core_n).wait_recv()

    def vec_send(k):
        return rc(vslab.at[y, z], vslab.at[y, z], v_s.at[k - 1], v_r.at[z], ((d + 2 * k) % (2 * nz), s))

    def vec_cross():
        return rc(vslab.at[y], vslab.at[y], v_s.at[nz - 1], v_r.at[nz], y_n)

    def vec_begin():
        for k in range(1, nz):
            vec_send(k).start()

    def vec_pass():
        for k in range(1, nz):
            zz = (z + k) % nz
            rc(vslab.at[y, zz], vslab.at[y, zz], v_s.at[0], v_r.at[zz], core_n).wait_recv()
        vec_cross().start()

    def vec_end():
        rc(vslab.at[1 - y], vslab.at[1 - y], v_s.at[0], v_r.at[nz], y_n).wait_recv()
        for zz in range(nz):
            for yy in range(2):
                at = (2 * zz + yy) * rows8
                vecs[:, at : at + rows8] = vslab[yy, zz].astype(F32)[0:VEC, 0:rows8]

    def vec_drain():
        for k in range(1, nz):
            vec_send(k).wait_send()
        vec_cross().wait_send()

    nrank = fgrad.shape[0]
    stores = [pltpu.make_async_copy(a, b, ag_s.at[n]) for n, (a, b) in enumerate(
        [(st_q, q_out), (st_k, k_out), (st_v, v_out), (st_in, in_out), (st_out, out_out), (ograd, o_out),
         (st_o, out_ref), (st_g, gtok_ref), (st_vec, vec_out), (st_ib, ib_out)])]

    def emit_out():
        for t in range(nrank):
            st_out[:, t * ffp : (t + 1) * ffp] = fgrad[t, :, out_at : out_at + ffp]
            st_in[:, t * ffp + cols - in_at : (t + 1) * ffp] = fgrad[t, :, cols : in_at + ffp]
        stores[4].start()

    def emit_ib():
        for t in range(nrank):
            st_ib[0:1, t * ffp : (t + 1) * ffp] = ibgrad[t, 0:1, off_in : off_in + ffp]
        stores[9].start()

    def emit_upper():
        h = cols // 2
        k_from = h - VEC - qw
        for t in range(nrank):
            st_k[:, t * qw + k_from : (t + 1) * qw] = fgrad[t, :, h : VEC + 2 * qw]
            st_v[:, t * qw : (t + 1) * qw] = fgrad[t, :, VEC + 2 * qw : VEC + 3 * qw]
            st_in[:, t * ffp : t * ffp + cols - in_at] = fgrad[t, :, in_at:cols]
        stores[2].start()
        stores[3].start()

    def emit_lower():
        h = cols // 2
        k_from = h - VEC - qw
        for t in range(nrank):
            st_q[:, t * qw : (t + 1) * qw] = fgrad[t, :, VEC : VEC + qw]
            st_k[:, t * qw : t * qw + k_from] = fgrad[t, :, VEC + qw : h]
        stores[0].start()
        stores[1].start()
        vcols = jnp.zeros((rows8, 128), F32)
        for t in range(nrank):
            vcols = vcols + fgrad[t, :, 0:128].astype(F32)
        st_vec[0:VEC] = jnp.transpose(vcols, (1, 0))[0:VEC]
        st_vec[6:7] = ograd[qw : qw + 8, VEC : VEC + qw].astype(F32)[0:1]
        st_vec[7:8] = ograd[qw : qw + 8, VEC + 2 * qw : VEC + 3 * qw].astype(F32)[0:1]
        stores[8].start()

    gather_swap(0)
    ag_x = agather(0, xall)
    ag_c = agather(1, call)
    ag_x[0]()
    vec_begin()
    gather_own(0)
    for cp in loads[VEC + 6 :]:
        cp.wait()
    build_rest()
    inrow[...] = inflat[...].astype(F32).reshape(inrow.shape)
    build_bias()
    gather_other(0)
    o_own(0)
    gather_hop1(0, 1, y)
    ag_x[1]((0, 1))
    gather_hop1(0, 1, 1 - y)
    o_own(1)
    gather_hop1(0, 2, y)
    vec_pass()
    ag_x[1]((2, 3))
    gather_swap(1)
    ag_c[0]()
    ag_x[2]((0,))
    gather_hop1(0, 2, 1 - y)
    o_own(2)
    o_pass(0)
    ag_x[2]((1,))
    vec_end()
    g1, s1 = vecs[0:1], vecs[1:2]
    o_b, g2, s2, out_b = vecs[4:5], vecs[5:6], vecs[6:7], vecs[7:8]

    def ln1_step(b, carry):
        img, r = b // 4, pl.ds(pl.multiple_of((b % 4) * 64, 64), 64)
        values = xall[img, r].astype(F32)
        row_mean = jnp.mean(values, axis=-1, keepdims=True)
        centred = values - row_mean
        inverse = lax.rsqrt(jnp.mean(centred * centred, axis=-1, keepdims=True) + eps_norm)
        n1[img, r] = (centred * inverse * g1 + s1).astype(BF16)
        mean1[img, r] = jnp.broadcast_to(row_mean, (64, 128))
        inv1[img, r] = jnp.broadcast_to(inverse, (64, 128))
        return carry

    lax.fori_loop(0, 4 * nimg, ln1_step, 0)
    gather_own(1)
    o_pass(1)
    o_pass(2)
    gather_other(1)
    gather_end(0)

    lane = lax.broadcasted_iota(jnp.int32, (1, cols), 1)
    qb = pltpu.roll(vecs[...], (VEC - rank * qw + width) % width, 1)[2:3, :cols]
    vb = pltpu.roll(vecs[...], (VEC + 2 * qw - rank * qw + width) % width, 1)[3:4, :cols]
    qkv_bias = jnp.where((lane >= VEC) & (lane < VEC + qw), qb, 0.0) + jnp.where(
        (lane >= VEC + 2 * qw) & (lane < VEC + 3 * qw), vb, 0.0)

    def att_step(img, carry):
        proj = dot(n1[img], w[:, 0:cols], 1, 0) + qkv_bias
        proj = proj.astype(BF16)
        qkv[img] = proj
        outs = []
        for h in range(2):
            at = VEC + h * HEAD_DIM
            q = proj[:, at : at + HEAD_DIM]
            k = proj[:, qw + at : qw + at + HEAD_DIM]
            v = proj[:, 2 * qw + at : 2 * qw + at + HEAD_DIM]
            sc = dot(q, k, 1, 1) * factor
            e = jnp.exp(sc - jnp.max(sc, axis=-1, keepdims=True))
            p = e / jnp.sum(e, axis=-1, keepdims=True)
            probs[img, h] = p
            outs.append(dot(p.astype(BF16), v, 1, 0).astype(BF16))
        mix[img] = jnp.concatenate(outs, axis=1)
        return carry

    lax.fori_loop(0, 2, att_step, 0)
    ag_c[1]()
    gather_swap(2)
    lax.fori_loop(2, nimg, att_step, 0)
    o_wait()

    def o_part(img):
        part[img] = dot(mix[img], ow[...], 1, 0).astype(BF16)

    rs_h = rscatter(0, part, r1, (dx, dy, rx, ry), o_part)
    rs_h[0]()
    rs_h[4]()
    gather_hop(1, 1)
    gather_drain(0)
    gather_own(2)
    gather_other(2)
    rs_h[1]()
    gather_hop(1, 2)
    ag_c[2]()
    rs_h[3]()
    ag_x[3]()
    ag_n = agather(2, n2)
    for i in range(2):
        hidden = xall[2 * y + i, own_rows].astype(F32) + rs_h[2](i) + o_b
        hid_s[i] = hidden
        hat, inv = normalize(hidden)
        hat2_s[i] = hat
        inv2_s[i] = jnp.broadcast_to(inv, (own_len, 128))
        n2[2 * y + i, own_rows] = (hat * g2 + s2).astype(BF16)
    ag_n[0]()
    gather_hop(2, 1)
    ag_n[1]()
    gather_end(1)
    gather_hop(2, 2)
    ag_n[2]()

    wlane = lax.broadcasted_iota(jnp.int32, (1, win), 1)
    valid = (wlane >= off_out) & (wlane < off_out + ffp)

    def in_step(img, carry):
        pre = dot(n2[img], w[:, in_win : in_win + win], 1, 0) + inb[0:1]
        a, sl = gelu_parts(pltpu.roll(pre, shift, 1))
        act[img] = jnp.where(valid, a, 0.0).astype(BF16)
        slope[img] = jnp.where(valid, sl, 0.0)
        return carry
    lax.fori_loop(0, nimg, in_step, 0)

    rtile = width // 3

    def gout_step(t, carry):
        t = 1 + sg * (1 - t)
        r = pl.ds(pl.multiple_of(t * rtile, rtile), rtile)
        acc = jnp.zeros((rtile, win), F32)
        for img in range(nimg):
            acc = acc + dot(call[img, :, r], act[img], 0, 0)
        gout_tail[r] = acc[:, 0 : 2 * cols - out_win].astype(BF16)
        g[r, 2 * cols : 3 * cols] = acc[:, 2 * cols - out_win :].astype(BF16)
        return carry
    lax.fori_loop(0, 1, gout_step, 0)
    z_first(0, (2,))
    lax.fori_loop(1, 2, gout_step, 0)
    z_first(0, (1,))
    lax.fori_loop(2, 3, gout_step, 0)
    z_first(0, (0, 3))
    gather_end(2)

    def gp_step(img, carry):
        ga = dot(call[img], w[:, out_win : out_win + win], 1, 0) * slope[img]
        gp[img] = pltpu.roll(ga, win - shift, 1).astype(BF16)
        return carry
    lax.fori_loop(0, nimg, gp_step, 0)
    ib_begin()

    def gn2_part(img):
        part[img] = dot(gp[img], w[:, in_win : in_win + win], 1, 1).astype(BF16)

    rs_g2 = rscatter(2, part, r1, (dx, dy, rx, ry), gn2_part)
    rs_g2[0]()
    rs_g2[4]()

    def gin_step(t, carry):
        r = pl.ds(pl.multiple_of(t * rtile, rtile), rtile)
        acc = jnp.zeros((rtile, win), F32)
        for img in range(nimg):
            acc = acc + dot(n2[img, :, r], gp[img], 0, 0)
        lo = cols - in_win
        gin_tail[r] = acc[:, 0:lo].astype(BF16)
        g[r, cols : 2 * cols - 128] = acc[:, lo : win - 128].astype(BF16)
        g[r, 2 * cols - 128 : 2 * cols] = (acc[:, win - 128 :] + gout_tail[r].astype(F32)).astype(BF16)
        return carry

    lax.fori_loop(0, 3, gin_step, 0)
    z_first(1)
    rs_g2[1]()
    z_merge(0, 1)

    sums = [jnp.zeros((1, width), F32) for _ in range(6)]
    ag_g = agather(3, gb)
    for i in range(2):
        gn2 = rs_g2[2](i)
        hat = hat2_s[i]
        sums[2] = sums[2] + jnp.sum(gn2 * hat, axis=0, keepdims=True)
        sums[3] = sums[3] + jnp.sum(gn2, axis=0, keepdims=True)
        up = call[2 * y + i, own_rows].astype(F32)
        gh = up + norm_back(gn2, g2, hat, inv2_s[i][:, 0:1])
        gh_s[i] = gh
        low = gh.astype(BF16)
        gb[2 * y + i, own_rows] = low
        sums[4] = sums[4] + jnp.sum(low.astype(F32), axis=0, keepdims=True)
        sums[5] = sums[5] + jnp.sum(up, axis=0, keepdims=True)
    rs_g2[3]()
    ag_c[3]()
    ag_n[3]()
    ag_g[0]()
    for n in range(2, 6):
        vsum[n : n + 1] = sums[n]
    vsum[6:8] = jnp.zeros((2, width), F32)
    vsum[0:2] = jnp.zeros((2, width), F32)
    z_merge(0, 0)

    def out_part(img):
        part2[img] = dot(act[img], w[:, out_win : out_win + win], 1, 1).astype(BF16)

    rs_o = rscatter(1, part2, r1b, (dxb, dyb, rxb, ryb), out_part)
    rs_o[0]()
    ag_g[1]()
    ag_g[2]()

    gacc = jnp.zeros((qw, width), F32)
    for img in range(nimg):
        gacc = gacc + dot(mix[img], gb[img], 0, 0)
    og[0:qw] = gacc.astype(BF16)
    og[qw:] = jnp.zeros((16, width), BF16)
    zo_first()
    ib_pass()
    zreduce_own(0)
    f_begin(0)
    rs_o[4]()

    def attb_step(img, carry):
        proj, gbi = qkv[img], gb[img]
        gmix = dot(gbi, ow[...], 1, 1).astype(BF16)
        zero = jnp.zeros((length, VEC), BF16)
        dq, dk, dv = [], [], []
        for h in range(2):
            at = VEC + h * HEAD_DIM
            q = proj[:, at : at + HEAD_DIM]
            k = proj[:, qw + at : qw + at + HEAD_DIM]
            v = proj[:, 2 * qw + at : 2 * qw + at + HEAD_DIM]
            gm = gmix[:, h * HEAD_DIM : (h + 1) * HEAD_DIM]
            p = probs[img, h]
            gpr = dot(gm, v, 1, 1)
            gs = (p * (gpr - jnp.sum(p * gpr, axis=-1, keepdims=True))).astype(BF16)
            dq.append((dot(gs, k, 1, 0) * factor).astype(BF16))
            dk.append((dot(gs, q, 0, 0) * factor).astype(BF16))
            dv.append(dot(p.astype(BF16), gm, 0, 0).astype(BF16))
        pad = jnp.zeros((length, cols - VEC - 3 * qw), BF16)
        dqkv[img] = jnp.concatenate([zero] + dq + dk + dv + [pad], axis=1)
        part[img] = dot(dqkv[img], w[:, 0:cols], 1, 1).astype(BF16)
        return carry

    def ln1_sum_step(img, carry):
        pr = part[img].astype(F32)
        hat = (xall[img].astype(F32) - mean1[img][:, 0:1]) * inv1[img][:, 0:1]
        vsum[0:1] = vsum[0:1] + jnp.sum(pr * hat, axis=0, keepdims=True)
        vsum[1:2] = vsum[1:2] + jnp.sum(pr, axis=0, keepdims=True)
        return carry

    def vcol_step(t, carry):
        r = pl.ds(pl.multiple_of(t * rtile, rtile), rtile)
        vcol = jnp.transpose(jnp.concatenate([vsum[:, r], jnp.zeros((120, rtile), F32)], axis=0), (1, 0))
        g[r, 0:128] = (g[r, 0:128].astype(F32) + vcol).astype(BF16)
        return carry

    def gn1_part(img):
        pass
    rs_g1 = rscatter(4, part, r1, (dx, dy, rx, ry), gn1_part)

    def gqkv_step(t, carry):
        r = pl.ds(pl.multiple_of(t * rtile, rtile), rtile)
        acc = jnp.zeros((rtile, cols), F32)
        for img in range(nimg):
            acc = acc + dot(n1[img, :, r], dqkv[img], 0, 0)
        g[r, 0 : cols - 128] = acc[:, 0 : cols - 128].astype(BF16)
        g[r, cols - 128 : cols] = (acc[:, cols - 128 :] + gin_tail[r].astype(F32)).astype(BF16)
        return carry

    lax.fori_loop(0, 2, attb_step, 0)
    f_spread(0)
    ib_mid()
    z_merge(1, 1)
    lax.fori_loop(2, nimg, attb_step, 0)
    rs_o[1]()
    qb_begin()
    lax.fori_loop(0, 3, gqkv_step, 0)
    zdrain(0)
    z_first(2)
    rs_g1[0]()
    rs_g1[4]()
    z_merge(1, 0)
    lax.fori_loop(0, nimg, ln1_sum_step, 0)
    lax.fori_loop(0, 3, vcol_step, 0)
    z_first(3)
    f_relay(0)
    ib_last()
    rs_g1[1]()
    zo_merge()
    zreduce_own(1)
    f_begin(1)
    z_merge(2, 1)
    f_spread(1)
    z_merge(2, 0)

    for i in range(2):
        gn1 = rs_g1[2](i)
        hat, inv = normalize(xall[2 * y + i, own_rows].astype(F32))
        st_g[i] = (gh_s[i] + norm_back(gn1, g1, hat, inv)).astype(BF16)
    ag_g[3]()
    stores[7].start()
    f_relay(1)
    pl.when(z == s)(o_here)
    z_merge(3, 1)
    z_merge(3, 0)
    f_drain(0)
    zreduce_own(2)
    f_begin(2)
    f_spread(2)
    f_drain(1)
    zreduce_own(3)
    f_begin(3)
    f_end(0)
    f_end(1)
    emit_out()
    f_relay(2)
    f_spread(3)
    for i in range(2):
        st_o[i] = (hid_s[i] + rs_o[2](i) + out_b).astype(BF16)
    stores[6].start()
    pl.when((s + 2) % 4 == z)(o_x)
    ib_end()
    emit_ib()
    f_end(2)
    emit_upper()
    o_end()
    stores[5].start()
    f_relay(3)
    f_end(3)
    emit_lower()

    for ch in (1, 2):
        gather_drain(ch)
    for ch in (1, 2, 3):
        zdrain(ch)
    for ch in (2, 3):
        f_drain(ch)
    o_drain()
    vec_drain()
    rs_o[3]()
    rs_g1[3]()
    pl.when(z != s)(lambda: zo_send(False).wait_send())
    pl.when(z == s)(lambda: o_out_done(2))
    pl.when((z == s) | ((s + 2) % 4 == z))(lambda: o_out_done(3))
    pl.when(z != s)(lambda: qb_send().wait_send())
    for k in range(1, nz):
        ib_send(k).wait_send()
    for n in range(7):
        ib_msg(nz + n, rank, core_n).wait_send()
    for cp in stores:
        cp.wait()


def widen_kernel(n_mat, n_copy, n_row, *refs):
    n = n_mat + n_copy + n_row
    src, refs = refs[:n], refs[n:]
    big, refs = refs[: n_mat + n_copy], refs[n_mat + n_copy :]
    n_flat = (len(refs) - 2 - n - n_mat) // 2
    flat_out, refs = refs[:n_flat], refs[n_flat:]
    held, refs = refs[:n], refs[n:]
    wide, refs = refs[:n_mat], refs[n_mat:]
    flat, (in_s, out_s) = refs[:n_flat], refs[n_flat:]
    got = [pltpu.make_async_copy(src[i], held[i], in_s.at[i]) for i in range(n)]
    put = [pltpu.make_async_copy(wide[i] if i < n_mat else held[i], big[i], out_s.at[i])
           for i in range(n_mat + n_copy)]
    put_flat = [pltpu.make_async_copy(flat[i], flat_out[i], out_s.at[n_mat + n_copy + i]) for i in range(n_flat)]
    for cp in got:
        cp.start()
    for i in range(n_mat + n_copy):
        got[i].wait()
        if i < n_mat:
            rows = wide[i].shape[0]
            for r in range(0, rows, 48):
                wide[i][r : r + 48] = held[i][r : r + 48].astype(F32)
        put[i].start()
    at = 0
    for i in range(n_mat + n_copy, n):
        got[i].wait()
        for r in range(held[i].shape[0]):
            flat[at][...] = held[i][r : r + 1].reshape(held[i].shape[1])
            put_flat[at].start()
            at += 1
    for cp in put + put_flat:
        cp.wait()


def widen(mats, rows, others, tables):
    hbm = pl.BlockSpec(memory_space=pl.ANY)
    arrays = list(mats) + list(others) + list(tables)
    n = len(arrays)
    flat = [jax.ShapeDtypeStruct((t.shape[1],), F32) for t in tables for _ in range(t.shape[0])]
    shapes = [jax.ShapeDtypeStruct((rows, m.shape[1]), F32) for m in mats]
    shapes += [jax.ShapeDtypeStruct(o.shape, o.dtype) for o in others] + flat
    return pl.pallas_call(
        functools.partial(widen_kernel, len(mats), len(others), len(tables)),
        out_shape=tuple(shapes),
        in_specs=[hbm] * n,
        out_specs=[hbm] * len(shapes),
        scratch_shapes=[pltpu.VMEM(a.shape, a.dtype) for a in arrays]
        + [pltpu.VMEM((rows, m.shape[1]), F32) for m in mats]
        + [pltpu.VMEM(f.shape, F32) for f in flat]
        + [pltpu.SemaphoreType.DMA((n,)), pltpu.SemaphoreType.DMA((len(shapes),))],
    )(*arrays)


def layer_fast(
    tokens, cotangent, ln1_gain, ln1_shift, q_weight, q_bias, k_weight, v_weight, v_bias,
    o_weight, o_bias, ln2_gain, ln2_shift, in_weight, in_bias, out_weight, out_bias,
):
    ns, ndp = lax.axis_size("seq"), lax.axis_size("dp")
    nz, ranks = ndp // 2, 2 * ns
    images, own_len, width = tokens.shape
    ff = in_weight.shape[1]
    hid, ffp = width // ranks, ff // ranks
    rows = q_weight.shape[0]
    vec = [ln1_gain, ln1_shift, q_bias, v_bias, o_bias, ln2_gain, ln2_shift, out_bias]
    slab = (2 * VEC, (rows + 127) // 128 * 128)
    total = 3 * 512
    win = (ffp + 127) // 128 * 128
    nimg, length, cols = 2 * images, own_len * ns, 512
    tall = (nimg, length, width)
    half = (own_len, width)
    D = pltpu.SemaphoreType.DMA
    V = pltpu.VMEM
    scratch = dict(
        wp=V((2, rows, total), BF16), fgrad=V((ranks, rows, total), BF16), ograd=V((hid + 16, width), BF16),
        ibgrad=V((ranks, 8, win), F32), st_q=V((rows, width), BF16), st_k=V((rows, width), BF16),
        st_v=V((rows, width), BF16), st_in=V((rows, ff), BF16), st_out=V((rows, ff), BF16),
        vslab=V((2, nz) + slab, BF16), inb=V((8, win), F32), inflat=V((ff,), BF16), inrow=V((1, ff), F32),
        **{f"vflat{n}": V((rows,), BF16) for n in range(VEC)}, vrows=V(slab, F32),
        st_o=V((2,) + half, BF16), st_g=V((2,) + half, BF16), st_vec=V((VEC, rows), F32), st_ib=V((1, ff), F32),
        w=V((2 * nz * rows, total), BF16), ow=V((hid, width), BF16), xall=V(tall, BF16), call=V(tall, BF16),
        n1=V(tall, BF16), n2=V(tall, BF16), gb=V(tall, BF16), qkv=V((nimg, length, cols), BF16),
        probs=V((nimg, 2, length, length), F32), mix=V((nimg, length, hid), BF16),
        act=V((nimg, length, win), BF16), slope=V((nimg, length, win), F32), gp=V((nimg, length, win), BF16),
        part=V(tall, BF16), part2=V(tall, BF16), r1=V((nimg, 2) + half, BF16), r1b=V((nimg, 2) + half, BF16),
        dx=V(half, BF16), dy=V(half, BF16), rx=V((2,) + half, BF16), ry=V((2,) + half, BF16),
        dxb=V(half, BF16), dyb=V(half, BF16), rxb=V((2,) + half, BF16), ryb=V((2,) + half, BF16),
        hid_s=V((2,) + half, F32), hat2_s=V((2,) + half, F32), inv2_s=V((2, own_len, 128), F32),
        gh_s=V((2,) + half, F32), vecs=V((VEC, width), F32),
        g=V((2 * nz * rows, total), BF16), rb=V((2, nz + 2, 2, rows, cols), BF16),
        rbh=V((2, nz + 2, 2, rows, cols // 2), BF16),
        rbo=V((nz + 1, hid + 16, width), BF16), gin_tail=V((width, 128), BF16), gout_tail=V((width, 128), BF16),
        dqkv=V((nimg, length, cols), BF16), vsum=V((8, width), F32),
        mean1=V((nimg, length, 128), F32), inv1=V((nimg, length, 128), F32), ibx=V((nz, 8, win), F32),
        isb=V((8, win), F32), og=V((hid + 16, width), BF16),
        qbs=V((8, cols), F32), qbx=V((nz, 8, cols), F32),
        gy_s=D((3,)), gz_s=D((2, nz, 2)), gzl_s=D((2, 2)), g_r=D((3, nz, 2)), o_s=D((nz - 1,)), o_r=D((1,)),
        ag_s=D((14,)), ag_r=D((14,)), rs_s=D((2, 14)), rs_r=D((2, 14)), z_s=D((3, 4, 2)),
        z_r=D((4, nz + 2, 2)), zo_s=D((4,)), zo_r=D((nz + 3,)), f_s=D((2, 7)), f_r=D((4, 7)), ib_s=D((nz + 7,)),
        ib_r=D((nz + 7,)), qb_s=D((1,)), qb_r=D((nz,)), v_s=D((nz,)),
        v_r=D((nz + 1,)),
    )
    hbm = pl.BlockSpec(memory_space=pl.ANY)
    out, gtok, gq, gk, gv, gin, gout, go, gvec, gib = pl.pallas_call(
        functools.partial(layer_kernel, nz, hid, ffp),
        out_shape=(
            jax.ShapeDtypeStruct(tokens.shape, BF16), jax.ShapeDtypeStruct(tokens.shape, BF16),
            jax.ShapeDtypeStruct((rows, width), BF16), jax.ShapeDtypeStruct((rows, width), BF16),
            jax.ShapeDtypeStruct((rows, width), BF16), jax.ShapeDtypeStruct((rows, ff), BF16),
            jax.ShapeDtypeStruct((rows, ff), BF16), jax.ShapeDtypeStruct((hid + 16, width), BF16),
            jax.ShapeDtypeStruct((VEC, rows), F32), jax.ShapeDtypeStruct((1, ff), F32),
        ),
        in_specs=[hbm] * (9 + VEC),
        out_specs=[hbm] * 10,
        scratch_shapes=list(scratch.values()),
        compiler_params=pltpu.CompilerParams(
            collective_id=0, has_side_effects=True, vmem_limit_bytes=65000 * 1024),
    )(tokens, cotangent, q_weight, k_weight, v_weight, in_weight, out_weight.T, o_weight, in_bias, *vec)
    (gin, gout, gq, gk, gv, go, out, gtok, d_g1, d_s1, d_g2, d_s2, d_ob, d_outb, d_qb, d_vb, gib) = widen(
        [gin, gout, gq, gk, gv, go], rows, [out, gtok], [gvec, gib])
    return (out, gtok, d_g1, d_s1, gq, d_qb, gk, gv, d_vb, go, d_ob, d_g2, d_s2, gin, gib, gout.T, d_outb)


def mm(a, b, ca, cb):
    return lax.dot_general(a, b, (((ca,), (cb,)), ((), ())), preferred_element_type=F32)


def on_device(
    tokens, cotangent, ln1_gain, ln1_shift, q_weight, q_bias, k_weight, v_weight, v_bias,
    o_weight, o_bias, ln2_gain, ln2_shift, in_weight, in_bias, out_weight, out_bias,
):
    part = lax.axis_index("seq")
    parts = lax.axis_size("seq")
    groups = lax.axis_size("dp")
    images, own_len, width = tokens.shape
    ff = in_weight.shape[1]
    hid = width // parts
    ffp = ff // parts
    heads = HEADS // parts
    length = own_len * parts
    rows = images * length

    def cols(w, n):
        return lax.dynamic_slice_in_dim(w, part * n, n, axis=1)

    vecs = jnp.stack(
        [ln1_gain, ln1_shift, q_bias, v_bias, o_bias, ln2_gain, ln2_shift, out_bias]
    )
    vecs = lax.all_gather(vecs, "dp", axis=1, tiled=True).astype(F32)
    g1, s1, qb, vb, ob, g2, s2, outb = [vecs[i] for i in range(8)]
    x = lax.all_gather(tokens, "seq", axis=1, tiled=True).reshape(rows, width)
    cot = lax.all_gather(cotangent, "seq", axis=1, tiled=True).reshape(rows, width)
    qkv = jnp.concatenate([cols(q_weight, hid), cols(k_weight, hid), cols(v_weight, hid)], axis=1)
    qkv = lax.all_gather(qkv, "dp", axis=0, tiled=True)
    o_w = lax.all_gather(o_weight, "dp", axis=0, tiled=True)
    o_w = lax.dynamic_slice_in_dim(o_w, part * hid, hid, axis=0)
    in_w = lax.all_gather(cols(in_weight, ffp), "dp", axis=0, tiled=True)
    out_w = lax.dynamic_slice_in_dim(out_weight, part * ffp, ffp, axis=0)
    out_w = lax.all_gather(out_w.T, "dp", axis=0, tiled=True)
    qb_own = lax.dynamic_slice_in_dim(qb, part * hid, hid)
    vb_own = lax.dynamic_slice_in_dim(vb, part * hid, hid)
    inb_own = lax.dynamic_slice_in_dim(in_bias, part * ffp, ffp).astype(F32)

    def scatter_tokens(partial):
        return lax.psum_scatter(
            partial.astype(BF16).reshape(images, length, width),
            "seq", scatter_dimension=1, tiled=True,
        ).astype(F32)

    hat1, _ = normalize(x.astype(F32))
    normed1 = (hat1 * g1 + s1).astype(BF16)
    proj = mm(normed1, qkv, 1, 0)
    queries = (proj[:, :hid] + qb_own).astype(BF16).reshape(images, length, heads, HEAD_DIM)
    keys = proj[:, hid : 2 * hid].astype(BF16).reshape(images, length, heads, HEAD_DIM)
    values = (proj[:, 2 * hid :] + vb_own).astype(BF16).reshape(images, length, heads, HEAD_DIM)
    factor = 1.0 / math.sqrt(HEAD_DIM)
    ein = lambda s, a, b: jnp.einsum(s, a, b, preferred_element_type=F32)
    scores = ein("iqhd,ikhd->ihqk", queries, keys) * factor
    top = jnp.max(scores, axis=-1, keepdims=True)
    expo = jnp.exp(scores - top)
    probs = expo / jnp.sum(expo, axis=-1, keepdims=True)
    probs_low = probs.astype(BF16)
    mixed = ein("ihqk,ikhd->iqhd", probs_low, values).astype(BF16).reshape(rows, hid)
    start = tokens.astype(F32)
    hidden = start + scatter_tokens(mm(mixed, o_w, 1, 0)) + ob
    hat2, r2 = normalize(hidden)
    normed2 = (hat2 * g2 + s2).astype(BF16)
    normed2 = lax.all_gather(normed2, "seq", axis=1, tiled=True).reshape(rows, width)
    pre = mm(normed2, in_w, 1, 0) + inb_own
    act, slope = gelu_parts(pre)
    act = act.astype(BF16)
    out = hidden + scatter_tokens(mm(act, out_w, 1, 1)) + outb
    d_out_w = mm(cot, act, 0, 0)
    cot_own = cotangent.astype(F32)
    grad_pre = (mm(cot, out_w, 1, 0) * slope).astype(BF16)
    d_in_w = mm(normed2, grad_pre, 0, 0)
    d_in_b = jnp.sum(grad_pre.astype(F32), axis=0)
    grad_n2 = scatter_tokens(mm(grad_pre, in_w, 1, 1))
    grad_hidden = cot_own + norm_back(grad_n2, g2, hat2, r2)
    branch_own = grad_hidden.astype(BF16)
    branch = lax.all_gather(branch_own, "seq", axis=1, tiled=True).reshape(rows, width)
    d_o_w = mm(mixed, branch, 0, 0)
    grad_mixed = mm(branch, o_w, 1, 1).astype(BF16).reshape(images, length, heads, HEAD_DIM)
    grad_probs = ein("iqhd,ikhd->ihqk", grad_mixed, values)
    row_dot = jnp.sum(probs * grad_probs, axis=-1, keepdims=True)
    grad_scores = (probs * (grad_probs - row_dot)).astype(BF16)
    grad_q = (ein("ihqk,ikhd->iqhd", grad_scores, keys) * factor).astype(BF16).reshape(rows, hid)
    grad_k = (ein("ihqk,iqhd->ikhd", grad_scores, queries) * factor).astype(BF16).reshape(rows, hid)
    grad_v = ein("ihqk,iqhd->ikhd", probs_low, grad_mixed).astype(BF16).reshape(rows, hid)
    grad_qkv = jnp.concatenate([grad_q, grad_k, grad_v], axis=1)
    d_qkv = mm(normed1, grad_qkv, 0, 0)
    d_qb = jnp.sum(grad_q.astype(F32), axis=0)
    d_vb = jnp.sum(grad_v.astype(F32), axis=0)
    grad_n1 = scatter_tokens(mm(grad_qkv, qkv, 1, 1))
    hat1o, r1o = normalize(start)
    grad_tokens = grad_hidden + norm_back(grad_n1, g1, hat1o, r1o)
    wide = jnp.concatenate([d_qkv, d_in_w, d_out_w], axis=1).astype(BF16)
    wide = lax.psum_scatter(wide, "dp", scatter_dimension=0, tiled=True)
    wide = lax.all_gather(wide, "seq", axis=0, tiled=False).astype(F32)

    def spread(lo, n):
        return wide[:, :, lo : lo + n].transpose(1, 0, 2).reshape(width // groups, n * parts)

    gq, gk, gv = [spread(i * hid, hid) for i in range(3)]
    gin = spread(3 * hid, ffp)
    gout = wide[:, :, 3 * hid + ffp :].transpose(0, 2, 1).reshape(ff, width // groups)
    o_full = lax.all_gather(
        lax.psum_scatter(d_o_w.astype(BF16), "dp", scatter_dimension=1, tiled=True),
        "seq", axis=0, tiled=True,
    )
    go = lax.all_to_all(o_full, "dp", split_axis=0, concat_axis=1, tiled=True).astype(F32)
    own_sums = jnp.stack([
        jnp.sum(grad_n1 * hat1o, axis=(0, 1)), jnp.sum(grad_n1, axis=(0, 1)),
        jnp.sum(grad_n2 * hat2, axis=(0, 1)), jnp.sum(grad_n2, axis=(0, 1)),
        jnp.sum(branch_own.astype(F32), axis=(0, 1)), jnp.sum(cot_own, axis=(0, 1)),
        lax.dynamic_update_slice_in_dim(jnp.zeros(width, F32), d_qb, part * hid, 0),
        lax.dynamic_update_slice_in_dim(jnp.zeros(width, F32), d_vb, part * hid, 0),
    ])
    bias_in = lax.dynamic_update_slice_in_dim(jnp.zeros(ff, F32), d_in_b, part * ffp, 0)
    total = lax.psum(jnp.concatenate([own_sums.reshape(-1), bias_in]), ("dp", "seq"))
    vec_part = total[: 8 * width].reshape(8, groups, width // groups)
    vec_part = lax.dynamic_index_in_dim(vec_part, lax.axis_index("dp"), axis=1, keepdims=False)
    bias_total = total[8 * width :]
    return (
        out.astype(BF16), grad_tokens.astype(BF16), vec_part[0], vec_part[1], gq, vec_part[6],
        gk, gv, vec_part[7], go, vec_part[4], vec_part[2], vec_part[3], gin, bias_total, gout,
        vec_part[5],
    )


def solution(mesh):
    fast = mesh.shape["dp"] == 2 * mesh.shape["seq"]
    rows, vec = P("dp", None), P("dp")
    tok = P("dp", "seq", None)
    return jax.shard_map(
        layer_fast if fast else on_device,
        mesh=mesh,
        in_specs=(tok, tok, vec, vec, rows, vec, rows, rows, vec, rows, vec, vec, vec, rows,
                  P(), P(None, "dp"), vec),
        out_specs=(tok, tok, vec, vec, rows, vec, rows, rows, vec, rows, vec, vec, vec, rows,
                   P(), P(None, "dp"), vec),
        check_vma=False,
    )
```

```python
import functools
import math

import jax
import jax.numpy as jnp
from jax import lax
from jax.experimental import pallas as pl
from jax.experimental.pallas import tpu as pltpu
from jax.sharding import PartitionSpec as P

BF16, F32 = jnp.bfloat16, jnp.float32
HEADS, HEAD_DIM = 16, 72
eps_norm = 1e-06
gelu_coef = 0.7978845608028654
gelu_cube = 0.044715
MESH = pl.DeviceIdType.MESH
VEC = 8


def normalize(values):
    row_mean = jnp.mean(values, axis=-1, keepdims=True)
    centred = values - row_mean
    inverse = lax.rsqrt(jnp.mean(centred * centred, axis=-1, keepdims=True) + eps_norm)
    return centred * inverse, inverse


def norm_back(grad_normed, gain_vec, scaled, inverse):
    grad_scaled = grad_normed * gain_vec
    centred_grad = grad_scaled - jnp.mean(grad_scaled, axis=-1, keepdims=True)
    return inverse * (
        centred_grad - scaled * jnp.mean(grad_scaled * scaled, axis=-1, keepdims=True)
    )


def gelu_parts(pre_act):
    square = pre_act * pre_act
    tanh_val = jnp.tanh(pre_act * (gelu_coef + gelu_coef * gelu_cube * square))
    gate = 0.5 + 0.5 * tanh_val
    value_part = pre_act * gate
    slope_part = gate + value_part * (1.0 - gate) * (2.0 * gelu_coef + 6.0 * gelu_coef * gelu_cube * square)
    return (value_part, slope_part)


def dot(a, b, ca, cb):
    return lax.dot_general(a, b, (((ca,), (cb,)), ((), ())), preferred_element_type=F32)


def layer_kernel(
    nz, hid, ffp,
    tok, cot_in, q_in, k_in, v_in, in_in, out_in, ow_in, inb_in, vin0, vin1, vin2, vin3, vin4, vin5, vin6, vin7,
    out_ref, gtok_ref, q_out, k_out, v_out, in_out, out_out, o_out, vec_out, ib_out,
    wp, fgrad, ograd, ibgrad, st_q, st_k, st_v, st_in, st_out, vslab, inb, inflat, inrow, vflat0, vflat1, vflat2, vflat3, vflat4, vflat5, vflat6, vflat7, vrows, st_o, st_g, st_vec, st_ib,
    w, ow, xall, call, n1, n2, gb, qkv, probs, mix, act, slope, gp, part, part2, r1, r1b,
    dx, dy, rx, ry, dxb, dyb, rxb, ryb, hid_s, hat2_s, inv2_s, gh_s, vecs, g, rb, rbh, rbo, gin_tail,
    gout_tail, dqkv, vsum, mean1, inv1, ibx, isb, og, qbs, qbx,
    gy_s, gz_s, gzl_s, g_r, o_s, o_r, ag_s, ag_r, rs_s, rs_r, z_s, z_r, zo_s, zo_r, f_s, f_r,
    ib_s, ib_r, qb_s, qb_r, v_s, v_r,
):
    d, s = lax.axis_index("dp"), lax.axis_index("seq")
    z, y = d // 2, d % 2
    x, c = s // 2, s % 2
    rank = 2 * s + y
    nimg, length, width = xall.shape
    own_len = dx.shape[0]
    rows8 = wp.shape[1]
    plane = 2 * rows8
    cols = 512
    qw = hid
    in_at = VEC + 3 * qw
    in_win = in_at // 128 * 128
    out_at = in_at + ffp
    out_win = out_at // 128 * 128
    win = (ffp + 127) // 128 * 128
    off_in, off_out = in_at - in_win, out_at - out_win
    shift = off_out - off_in
    core_n, x_n, y_n = (d, s + 1 - 2 * c), (d, (s + 2) % 4), (d + 1 - 2 * y, s)
    right, left = (d + 2, s), (d - 2, s)
    has_r, has_l = z < nz - 1, z > 0
    sg = 1 - 2 * (z // 2)
    is_end = (z == 0) | (z == nz - 1)
    middle = (z > 0) & (z < nz - 1)
    factor = 1.0 / math.sqrt(HEAD_DIM)

    def plane_at(k):
        return z + sg * k

    def away(k):
        return (d + 2 * sg * k, s)

    def rc(src, dst, ss, rs, dev):
        return pltpu.make_async_remote_copy(
            src_ref=src, dst_ref=dst, send_sem=ss, recv_sem=rs, device_id=dev, device_id_type=MESH
        )

    barrier = pltpu.get_barrier_semaphore()
    column = [((d + 2 * k) % (2 * nz), s) for k in range(1, nz)]
    for dev in [core_n, x_n, y_n] + column:
        pl.semaphore_signal(barrier, inc=1, device_id=dev, device_id_type=MESH)

    own_rows = pl.ds(pl.multiple_of(s * own_len, 16), own_len)
    vflat = (vflat0, vflat1, vflat2, vflat3, vflat4, vflat5, vflat6, vflat7)
    vec_loads = list(zip((vin0, vin1, vin2, vin3, vin4, vin5, vin6, vin7), vflat))
    loads = [pltpu.make_async_copy(a, b, rs_s.at[n // 14, n % 14]) for n, (a, b) in enumerate(
        vec_loads + [(q_in, st_q), (k_in, st_k), (v_in, st_v), (in_in, st_in),
         (tok.at[0], xall.at[2 * y, own_rows]), (tok.at[1], xall.at[2 * y + 1, own_rows]), (out_in, st_out),
         (cot_in.at[0], call.at[2 * y, own_rows]), (cot_in.at[1], call.at[2 * y + 1, own_rows]),
         (inb_in, inflat)])]
    for cp in loads:
        cp.start()
    load_o = pltpu.make_async_copy(ow_in, ow, rs_s.at[1, 13])
    pl.when(z == s)(lambda: load_o.start())

    def build_first():
        def go(k):
            for j in range(2):
                t = 2 * k + j
                wp[j, :, 0:128] = jnp.zeros((rows8, 128), BF16)
                for n, st in enumerate((st_q, st_k, st_v)):
                    wp[j, :, VEC + n * qw : VEC + (n + 1) * qw] = st[:, t * qw : (t + 1) * qw]
                wp[j, :, in_at:cols] = st_in[:, t * ffp : t * ffp + cols - in_at]
        for k in range(4):
            pl.when(s == k)(functools.partial(go, k))

    def build_rest():
        def go(k):
            for j in range(2):
                t = 2 * k + j
                wp[j, :, 3 * cols - 128 :] = jnp.zeros((rows8, 128), BF16)
                wp[j, :, cols : in_at + ffp] = st_in[:, t * ffp + cols - in_at : (t + 1) * ffp]
                wp[j, :, out_at : out_at + ffp] = st_out[:, t * ffp : (t + 1) * ffp]
        for k in range(4):
            pl.when(s == k)(functools.partial(go, k))

    def build_bias():
        def go(t):
            inb[...] = jnp.zeros_like(inb)
            inb[0:1, off_in : off_in + ffp] = inrow[0:1, t * ffp : (t + 1) * ffp]
        for t in range(8):
            pl.when(rank == t)(functools.partial(go, t))

    for cp in loads[: VEC + 6]:
        cp.wait()
    vrows[...] = jnp.zeros_like(vrows)
    for n in range(VEC):
        vrows[n : n + 1, 0:rows8] = vflat[n][...].astype(F32).reshape(1, rows8)
    vslab[y, z] = vrows[...].astype(BF16)
    build_first()
    pl.semaphore_wait(barrier, 3 + len(column))

    def wrows(origin, sub):
        return pl.ds(pl.multiple_of(origin * plane + sub * rows8, 16), rows8)

    def wslab(ch, origin, sub):
        return w.at[wrows(origin, sub), pl.ds(ch * cols, cols)]

    def wsend(ch, origin, sub, src, to_right, own=False):
        sems = gz_s.at[ch % 2, origin, sub] if to_right or not own else gzl_s.at[ch % 2, sub]
        return rc(src, wslab(ch, origin, sub), sems, g_r.at[ch, origin, sub],
                  right if to_right else left)

    def wrecv(ch, origin, sub):
        slab = wslab(ch, origin, sub)
        rc(slab, slab, g_r.at[ch, origin, sub], g_r.at[ch, origin, sub], core_n).wait_recv()

    def gather_own(ch):
        src = wp.at[y, :, pl.ds(ch * cols, cols)]
        pl.when(has_r)(lambda: wsend(ch, z, y, src, True).start())
        pl.when(has_l)(lambda: wsend(ch, z, y, src, False, True).start())
        w[wrows(z, y), ch * cols : (ch + 1) * cols] = wp[y, :, ch * cols : (ch + 1) * cols]

    def gather_swap(ch):
        rc(wp.at[1 - y, :, pl.ds(ch * cols, cols)], wslab(ch, z, y), gy_s.at[ch], g_r.at[ch, z, y],
           y_n).start()

    def gather_other(ch):
        wrecv(ch, z, 1 - y)
        src = wslab(ch, z, 1 - y)
        pl.when(has_r)(lambda: wsend(ch, z, 1 - y, src, True).start())
        pl.when(has_l)(lambda: wsend(ch, z, 1 - y, src, False, True).start())

    def gather_hop(ch, k):
        for sub in range(2):
            gather_hop1(ch, k, sub)

    def gather_end(ch):
        for k in range(1, nz):
            for sub in range(2):
                pl.when(is_end)(lambda: wrecv(ch, plane_at(k), sub))

    def gather_hop1(ch, k, sub):
        def from_left():
            wrecv(ch, z - k, sub)
            pl.when(has_r)(lambda: wsend(ch, z - k, sub, wslab(ch, z - k, sub), True).start())

        def from_right():
            wrecv(ch, z + k, sub)
            pl.when(has_l)(lambda: wsend(ch, z + k, sub, wslab(ch, z + k, sub), False).start())

        pl.when(middle & (z - k >= 0))(from_left)
        pl.when(middle & (z + k < nz))(from_right)

    def gather_drain(ch):
        for k in range(nz):
            for sub in range(2):
                pl.when((z - k >= 0) & has_r)(
                    lambda: wsend(ch, z - k, sub, wslab(ch, z - k, sub), True).wait_send())
                pl.when((z + k < nz) & has_l)(
                    lambda: wsend(ch, z + k, sub, wslab(ch, z + k, sub), False, k == 0).wait_send())
        rc(wp.at[1 - y, :, pl.ds(ch * cols, cols)], wslab(ch, z, y), gy_s.at[ch], g_r.at[ch, z, y],
           y_n).wait_send()

    split = width // 256 * 128 + 128

    def osend(to_right, half):
        part_of = ow.at[:, pl.ds(0, split)] if half == 0 else ow.at[:, pl.ds(split, width - split)]
        return rc(part_of, part_of, o_s.at[0 if to_right else 1, half], o_r.at[half], right if to_right else left)

    def o_own(when):
        def outer():
            load_o.wait()
            for half in range(2):
                pl.when(has_r)(lambda: osend(True, half).start())
                pl.when(has_l)(lambda: osend(False, half).start())

        def inner():
            load_o.wait()
            for half in range(2):
                pl.when(z == 1)(lambda: osend(True, half).start())
                pl.when(z == 2)(lambda: osend(False, half).start())

        def last():
            for half in range(2):
                pl.when(z == 1)(lambda: osend(False, half).start())
                pl.when(z == 2)(lambda: osend(True, half).start())
        cond = is_end if when == 0 else middle
        pl.when((z == s) & cond)((outer, inner, last)[when])

    def o_pass(when, half):
        def go():
            osend(True, half).wait_recv()
            pl.when((z > s) & has_r)(lambda: osend(True, half).start())
            pl.when((z < s) & has_l)(lambda: osend(False, half).start())
        near = (s == 0) & (z == 1) | (s == 3) & (z == 2)
        cross = (s == 1) & (z == 2) | (s == 2) & (z == 1)
        far = (s == 0) & (z == 2) | (s == 3) & (z == 1)
        pl.when((near, cross, far)[when])(go)

    def o_wait():
        def go():
            osend(True, 0).wait_recv()
            osend(True, 1).wait_recv()
        pl.when((z != s) & is_end)(go)

    def o_drain():
        for half in range(2):
            pl.when((z >= s) & has_r)(lambda: osend(True, half).wait_send())
            pl.when((z <= s) & has_l)(lambda: osend(False, half).wait_send())

    def agather(inst, dst):
        ss, rr = (rs_s.at[1], rs_r.at[1]) if inst == 1 else (ag_s, ag_r)

        def blk(yy, sq, i):
            return dst.at[2 * yy + i, pl.ds(pl.multiple_of(sq * own_len, 16), own_len)]

        sx, sp = (s + 2) % 4, s + 1 - 2 * c
        spx = (sp + 2) % 4

        def msg(n, block, dev):
            return rc(block, block, ss.at[n], rr.at[n], dev)

        mine = [blk(y, s, i) for i in range(2)]
        xs = [blk(y, sx, i) for i in range(2)]
        ys = [blk(1 - y, s, i) for i in range(2)]
        dg = [blk(1 - y, sx, i) for i in range(2)]
        sends = [msg(0, mine[0], x_n), msg(1, mine[1], x_n), msg(2, ys[1], x_n),
                 msg(3, mine[0], y_n), msg(4, mine[1], y_n), msg(5, xs[0], y_n)]
        sends += [msg(6 + i, mine[i], core_n) for i in range(2)]
        sends += [msg(8 + i, xs[i], core_n) for i in range(2)]
        sends += [msg(10 + i, ys[i], core_n) for i in range(2)]
        sends += [msg(12 + i, dg[i], core_n) for i in range(2)]
        recvs = [msg(0, xs[0], x_n), msg(1, xs[1], x_n), msg(2, dg[1], x_n),
                 msg(3, ys[0], y_n), msg(4, ys[1], y_n), msg(5, dg[0], y_n)]
        recvs += [msg(6 + i, blk(y, sp, i), core_n) for i in range(2)]
        recvs += [msg(8 + i, blk(y, spx, i), core_n) for i in range(2)]
        recvs += [msg(10 + i, blk(1 - y, sp, i), core_n) for i in range(2)]
        recvs += [msg(12 + i, blk(1 - y, spx, i), core_n) for i in range(2)]

        def begin():
            for n in (0, 4, 1, 3, 6, 7):
                sends[n].start()

        def relay(parts=(0, 1, 2, 3)):
            if 0 in parts:
                recvs[0].wait_recv()
                sends[5].start()
                sends[8].start()
            if 1 in parts:
                recvs[4].wait_recv()
                sends[2].start()
                sends[11].start()
            if 2 in parts:
                recvs[1].wait_recv()
                sends[9].start()
            if 3 in parts:
                recvs[3].wait_recv()
                sends[10].start()

        def finish(parts=(0, 1)):
            if 0 in parts:
                recvs[2].wait_recv()
                sends[13].start()
                recvs[5].wait_recv()
                sends[12].start()
            if 1 in parts:
                for n in range(6, 14):
                    recvs[n].wait_recv()

        def drain():
            for m in sends:
                m.wait_send()

        return begin, relay, finish, drain

    def rscatter(inst, pt, ra, bufs, produce):
        bdx, bdy, brx, bry = bufs
        ss, rr = rs_s.at[inst % 2], rs_r.at[inst % 2]
        xo = 1 - x

        def image(it):
            return (2 * (1 - y) + it) % 4

        def rows(xx, cc):
            return pl.ds(pl.multiple_of((2 * xx + cc) * own_len, 16), own_len)

        def swap(it, xx):
            img = image(it)
            return rc(pt.at[img, rows(xx, 1 - c)], ra.at[img, xx], ss.at[2 * it + xx],
                      rr.at[2 * it + xx], core_n)

        def add(it, xx):
            swap(it, xx).wait_recv()
            img = image(it)
            ra[img, xx] = (ra[img, xx].astype(F32) + pt[img, rows(xx, c)].astype(F32)).astype(BF16)

        m = [
            rc(ra.at[image(0), xo], bdx, ss.at[8], rr.at[8], x_n),
            rc(ra.at[image(1), xo], bdy, ss.at[9], rr.at[9], y_n),
            rc(ra.at[image(1), x], bry.at[1], ss.at[10], rr.at[10], y_n),
            rc(ra.at[image(2), xo], brx.at[0], ss.at[11], rr.at[11], x_n),
            rc(ra.at[image(0), x], bry.at[0], ss.at[12], rr.at[12], y_n),
            rc(ra.at[image(3), xo], brx.at[1], ss.at[13], rr.at[13], x_n),
        ]

        def run_a():
            def step(it, carry):
                produce(image(it))
                swap(it, xo).start()
                swap(it, x).start()
                return carry
            lax.fori_loop(0, nimg, step, 0)

        def run_c():
            add(0, xo)
            m[0].start()
            add(1, xo)
            m[1].start()
            add(1, x)
            m[2].start()
            add(2, xo)
            m[3].start()
            add(0, x)
            add(3, xo)

        def run_b():
            m[0].wait_recv()
            ra[image(0), x] = (ra[image(0), x].astype(F32) + bdx[...].astype(F32)).astype(BF16)
            m[4].start()
            m[1].wait_recv()
            ra[image(3), xo] = (ra[image(3), xo].astype(F32) + bdy[...].astype(F32)).astype(BF16)
            m[5].start()
            add(2, x)
            add(3, x)

        def result(i):
            rc(brx.at[i], brx.at[i], ss.at[11 + 2 * i], rr.at[11 + 2 * i], x_n).wait_recv()
            rc(bry.at[i], bry.at[i], ss.at[12 - 2 * i], rr.at[12 - 2 * i], y_n).wait_recv()
            return (ra[image(2 + i), x].astype(F32) + brx[i].astype(F32)) + bry[i].astype(F32)

        def drain():
            for it in range(nimg):
                swap(it, 0).wait_send()
                swap(it, 1).wait_send()
            for n in range(8, 14):
                rc(bdx, bdx, ss.at[n], rr.at[n], x_n).wait_send()

        return run_a, run_b, result, drain, run_c

    zch = [(2 * cols, cols), (cols, cols), (cols // 2, cols // 2), (0, cols // 2)]
    order = (1 - y, y)

    def rb_at(ch, slot, sub):
        return (rb if ch < 2 else rbh).at[ch % 2, slot, sub]

    def gslab(ch, dest, sub):
        return g.at[wrows(dest, sub), pl.ds(*zch[ch])]

    def zsend(ch, where, sub, outer):
        k = (1, 2, 3, -1)[where]
        to, slot = (1, (z, nz + 1, nz)[where]) if outer else (k, z)
        return rc(gslab(ch, plane_at(k), sub), rb_at(ch, slot, sub), z_s.at[(0, 1, 0, 2)[ch], where, sub],
                  z_r.at[ch, slot, sub], away(to))

    def zadd(ch, dest, slot, sub):
        ref = rb_at(ch, slot, sub)
        rc(ref, ref, z_r.at[ch, slot, sub], z_r.at[ch, slot, sub], core_n).wait_recv()
        r, cs = wrows(dest, sub), slice(zch[ch][0], sum(zch[ch]))
        g[r, cs] = (g[r, cs].astype(F32) + ref[...].astype(F32)).astype(BF16)

    def z_first(ch, parts=(2, 1, 0, 3)):
        def outer():
            for where in (2, 1, 0):
                if where in parts:
                    for sub in order:
                        zsend(ch, where, sub, True).start()

        def inner():
            if 3 in parts:
                for sub in order:
                    zsend(ch, 3, sub, False).start()
        pl.when(is_end)(outer)
        pl.when(middle)(inner)

    def z_merge(ch, where):
        def inner():
            for sub in order:
                zadd(ch, plane_at(where + 1), nz + 1 - where, sub)
                zsend(ch, where, sub, False).start()
        pl.when(middle)(inner)

    def zreduce_own(ch):
        def outer(sub):
            zadd(ch, z, plane_at(1), sub)
            zadd(ch, z, plane_at(2), sub)

        def inner(sub):
            zadd(ch, z, plane_at(-1), sub)
            zadd(ch, z, plane_at(1), sub)
        for sub in order:
            pl.when(is_end)(functools.partial(outer, sub))
            pl.when(middle)(functools.partial(inner, sub))

    def zdrain(ch):
        for sub in range(2):
            zsend(ch, 0, sub, False).wait_send()
            zsend(ch, 1, sub, False).wait_send()
            pl.when(is_end)(lambda: zsend(ch, 2, sub, True).wait_send())
            pl.when(middle)(lambda: zsend(ch, 3, sub, False).wait_send())

    def f_swap(ch):
        src = g.at[wrows(z, 1 - y), pl.ds(*zch[ch])]
        return rc(src, fgrad.at[rank, :, pl.ds(*zch[ch])], f_s.at[ch % 2, 0], f_r.at[ch, 0], y_n)

    def f_msg(ch, n, slot, dev):
        piece = fgrad.at[slot, :, pl.ds(*zch[ch])]
        return rc(piece, piece, f_s.at[ch % 2, n], f_r.at[ch, n], dev)

    sx, sp = (s + 2) % 4, s + 1 - 2 * c
    spx = (sp + 2) % 4

    def f_begin(ch):
        f_swap(ch).start()
        cs = slice(zch[ch][0], sum(zch[ch]))
        fgrad[rank, :, cs] = g[wrows(z, y), cs]
        f_msg(ch, 1, rank, x_n).start()
        f_msg(ch, 3, rank, core_n).start()

    def f_spread(ch):
        other = 2 * s + 1 - y
        f_msg(ch, 0, other, y_n).wait_recv()
        f_msg(ch, 2, other, x_n).start()
        f_msg(ch, 4, other, core_n).start()

    def f_relay(ch):
        f_msg(ch, 1, 2 * sx + y, x_n).wait_recv()
        f_msg(ch, 5, 2 * sx + y, core_n).start()
        f_msg(ch, 2, 2 * sx + 1 - y, x_n).wait_recv()
        f_msg(ch, 6, 2 * sx + 1 - y, core_n).start()

    def f_end(ch):
        f_msg(ch, 3, 2 * sp + y, core_n).wait_recv()
        f_msg(ch, 4, 2 * sp + 1 - y, core_n).wait_recv()
        f_msg(ch, 5, 2 * spx + y, core_n).wait_recv()
        f_msg(ch, 6, 2 * spx + 1 - y, core_n).wait_recv()

    def f_drain(ch):
        f_swap(ch).wait_send()
        for n in range(1, 7):
            f_msg(ch, n, rank, core_n).wait_send()

    far_out = is_end & (plane_at(0) != s) & (plane_at(1) != s)
    adds = middle & ((plane_at(1) == s) | (plane_at(2) == s))

    def zo_send(far):
        if far:
            return rc(og, rbo.at[nz], zo_s.at[0], zo_r.at[nz], away(1))
        return rc(og, rbo.at[z], zo_s.at[0], zo_r.at[z], (2 * s + y, s))

    def zo_add(slot):
        rc(rbo.at[slot], rbo.at[slot], zo_s.at[0], zo_r.at[slot], core_n).wait_recv()
        og[...] = (og[...].astype(F32) + rbo[slot].astype(F32)).astype(BF16)

    def zo_first():
        pl.when(far_out)(lambda: zo_send(True).start())
        pl.when(jnp.logical_not(far_out | adds) & (z != s))(lambda: zo_send(False).start())

    def zo_merge():
        def go():
            zo_add(nz)
            zo_send(False).start()
        pl.when(adds)(go)

    def zo_last():
        def outer():
            zo_add(plane_at(1))
            zo_add(plane_at(2))

        def inner():
            zo_add(plane_at(-1))
            zo_add(plane_at(1))
        pl.when(is_end)(outer)
        pl.when(middle)(inner)

    def qb_send():
        return rc(qbs, qbx.at[z], qb_s.at[0], qb_r.at[z], (2 * s + y, s))

    def qb_begin():
        bsum = jnp.zeros((1, cols), F32)
        for img in range(nimg):
            bsum = bsum + jnp.sum(dqkv[img].astype(F32), axis=0, keepdims=True)
        qbs[...] = jnp.broadcast_to(bsum, (8, cols))
        pl.when(z != s)(lambda: qb_send().start())

    def o_here():
        zo_last()
        total = qbs[...]
        for k in range(1, nz):
            zz = (z + k) % nz
            rc(qbs, qbx.at[zz], qb_s.at[0], qb_r.at[zz], core_n).wait_recv()
            total = total + qbx[zz]
        ograd[0:qw] = og[...]
        ograd[qw:, 0:cols] = jnp.concatenate([total, total], axis=0).astype(BF16)
        ograd[qw:, cols:] = jnp.zeros((16, width - cols), BF16)
        rc(ograd, ograd, zo_s.at[2], zo_r.at[nz + 1], x_n).start()
        rc(ograd, ograd, zo_s.at[3], zo_r.at[nz + 2], core_n).start()

    def o_x():
        rc(ograd, ograd, zo_s.at[2], zo_r.at[nz + 1], x_n).wait_recv()
        rc(ograd, ograd, zo_s.at[3], zo_r.at[nz + 2], core_n).start()

    def o_end():
        pl.when((sp == z) | (spx == z))(
            lambda: rc(ograd, ograd, zo_s.at[3], zo_r.at[nz + 2], core_n).wait_recv())

    def o_out_done(n):
        rc(ograd, ograd, zo_s.at[n], zo_r.at[0], core_n).wait_send()

    def ib_send(k):
        return rc(isb, ibx.at[z], ib_s.at[k - 1], ib_r.at[z], ((d + 2 * k) % (2 * nz), s))

    def ib_begin():
        ib = jnp.zeros((1, win), F32)
        for img in range(nimg):
            ib = ib + jnp.sum(gp[img].astype(F32), axis=0, keepdims=True)
        isb[...] = jnp.broadcast_to(ib, (8, win))
        for k in range(1, nz):
            ib_send(k).start()

    def ib_msg(n, slot, dev):
        return rc(ibgrad.at[slot], ibgrad.at[slot], ib_s.at[n], ib_r.at[n], dev)

    def ib_pass():
        ibsum = isb[...]
        for k in range(1, nz):
            zz = (z + k) % nz
            rc(isb, ibx.at[zz], ib_s.at[0], ib_r.at[zz], core_n).wait_recv()
            ibsum = ibsum + ibx[zz]
        ibgrad[rank] = ibsum
        ib_msg(nz, rank, y_n).start()
        ib_msg(nz + 1, rank, x_n).start()
        ib_msg(nz + 3, rank, core_n).start()

    def ib_mid():
        other = 2 * s + 1 - y
        ib_msg(nz, other, y_n).wait_recv()
        ib_msg(nz + 2, other, x_n).start()
        ib_msg(nz + 4, other, core_n).start()
        ib_msg(nz + 1, 2 * sx + y, x_n).wait_recv()
        ib_msg(nz + 5, 2 * sx + y, core_n).start()

    def ib_last():
        ib_msg(nz + 2, 2 * sx + 1 - y, x_n).wait_recv()
        ib_msg(nz + 6, 2 * sx + 1 - y, core_n).start()

    def ib_end():
        ib_msg(nz + 3, 2 * sp + y, core_n).wait_recv()
        ib_msg(nz + 4, 2 * sp + 1 - y, core_n).wait_recv()
        ib_msg(nz + 5, 2 * spx + y, core_n).wait_recv()
        ib_msg(nz + 6, 2 * spx + 1 - y, core_n).wait_recv()

    def vec_send(k):
        return rc(vslab.at[y, z], vslab.at[y, z], v_s.at[k - 1], v_r.at[z], ((d + 2 * k) % (2 * nz), s))

    def vec_cross():
        return rc(vslab.at[y], vslab.at[y], v_s.at[nz - 1], v_r.at[nz], y_n)

    def vec_begin():
        for k in range(1, nz):
            vec_send(k).start()

    def vec_pass():
        for k in range(1, nz):
            zz = (z + k) % nz
            rc(vslab.at[y, zz], vslab.at[y, zz], v_s.at[0], v_r.at[zz], core_n).wait_recv()
        vec_cross().start()

    def vec_end():
        rc(vslab.at[1 - y], vslab.at[1 - y], v_s.at[0], v_r.at[nz], y_n).wait_recv()
        for zz in range(nz):
            for yy in range(2):
                at = (2 * zz + yy) * rows8
                vecs[:, at : at + rows8] = vslab[yy, zz].astype(F32)[0:VEC, 0:rows8]

    def vec_drain():
        for k in range(1, nz):
            vec_send(k).wait_send()
        vec_cross().wait_send()

    nrank = fgrad.shape[0]
    stores = [pltpu.make_async_copy(a, b, ag_s.at[n]) for n, (a, b) in enumerate(
        [(st_q, q_out), (st_k, k_out), (st_v, v_out), (st_in, in_out), (st_out, out_out), (ograd, o_out),
         (st_o, out_ref), (st_g, gtok_ref), (st_vec, vec_out), (st_ib, ib_out)])]

    def emit_out():
        for t in range(nrank):
            st_out[:, t * ffp : (t + 1) * ffp] = fgrad[t, :, out_at : out_at + ffp]
            st_in[:, t * ffp + cols - in_at : (t + 1) * ffp] = fgrad[t, :, cols : in_at + ffp]
        stores[4].start()

    def emit_ib():
        for t in range(nrank):
            st_ib[0:1, t * ffp : (t + 1) * ffp] = ibgrad[t, 0:1, off_in : off_in + ffp]
        stores[9].start()

    def emit_upper():
        h = cols // 2
        k_from = h - VEC - qw
        for t in range(nrank):
            st_k[:, t * qw + k_from : (t + 1) * qw] = fgrad[t, :, h : VEC + 2 * qw]
            st_v[:, t * qw : (t + 1) * qw] = fgrad[t, :, VEC + 2 * qw : VEC + 3 * qw]
            st_in[:, t * ffp : t * ffp + cols - in_at] = fgrad[t, :, in_at:cols]
        stores[2].start()
        stores[3].start()

    def emit_lower():
        h = cols // 2
        k_from = h - VEC - qw
        for t in range(nrank):
            st_q[:, t * qw : (t + 1) * qw] = fgrad[t, :, VEC : VEC + qw]
            st_k[:, t * qw : t * qw + k_from] = fgrad[t, :, VEC + qw : h]
        stores[0].start()
        stores[1].start()
        vcols = jnp.zeros((rows8, 128), F32)
        for t in range(nrank):
            vcols = vcols + fgrad[t, :, 0:128].astype(F32)
        st_vec[0:VEC] = jnp.transpose(vcols, (1, 0))[0:VEC]
        st_vec[6:7] = ograd[qw : qw + 8, VEC : VEC + qw].astype(F32)[0:1]
        st_vec[7:8] = ograd[qw : qw + 8, VEC + 2 * qw : VEC + 3 * qw].astype(F32)[0:1]
        stores[8].start()

    gather_swap(0)
    ag_x = agather(0, xall)
    ag_c = agather(1, call)
    ag_x[0]()
    vec_begin()
    gather_own(0)
    for cp in loads[VEC + 6 :]:
        cp.wait()
    build_rest()
    inrow[...] = inflat[...].astype(F32).reshape(inrow.shape)
    build_bias()
    gather_other(0)
    o_own(0)
    gather_hop1(0, 1, y)
    ag_x[1]((0, 1))
    gather_hop1(0, 1, 1 - y)
    o_own(1)
    gather_hop1(0, 2, y)
    vec_pass()
    o_pass(0, 0)
    ag_x[1]((2, 3))
    o_pass(0, 1)
    gather_swap(1)
    ag_c[0]()
    ag_x[2]((0,))
    gather_hop1(0, 2, 1 - y)
    o_own(2)
    ag_x[2]((1,))
    vec_end()
    g1, s1 = vecs[0:1], vecs[1:2]
    o_b, g2, s2, out_b = vecs[4:5], vecs[5:6], vecs[6:7], vecs[7:8]

    def ln1_step(b, carry):
        img, r = b // 4, pl.ds(pl.multiple_of((b % 4) * 64, 64), 64)
        values = xall[img, r].astype(F32)
        row_mean = jnp.mean(values, axis=-1, keepdims=True)
        centred = values - row_mean
        inverse = lax.rsqrt(jnp.mean(centred * centred, axis=-1, keepdims=True) + eps_norm)
        n1[img, r] = (centred * inverse * g1 + s1).astype(BF16)
        mean1[img, r] = jnp.broadcast_to(row_mean, (64, 128))
        inv1[img, r] = jnp.broadcast_to(inverse, (64, 128))
        return carry

    o_pass(1, 0)
    lax.fori_loop(0, 2 * nimg, ln1_step, 0)
    o_pass(2, 0)
    lax.fori_loop(2 * nimg, 4 * nimg, ln1_step, 0)
    o_pass(1, 1)
    o_pass(2, 1)
    gather_own(1)
    gather_other(1)
    gather_end(0)

    lane = lax.broadcasted_iota(jnp.int32, (1, cols), 1)
    qb = pltpu.roll(vecs[...], (VEC - rank * qw + width) % width, 1)[2:3, :cols]
    vb = pltpu.roll(vecs[...], (VEC + 2 * qw - rank * qw + width) % width, 1)[3:4, :cols]
    qkv_bias = jnp.where((lane >= VEC) & (lane < VEC + qw), qb, 0.0) + jnp.where(
        (lane >= VEC + 2 * qw) & (lane < VEC + 3 * qw), vb, 0.0)

    def att_step(img, carry):
        proj = dot(n1[img], w[:, 0:cols], 1, 0) + qkv_bias
        proj = proj.astype(BF16)
        qkv[img] = proj
        outs = []
        for h in range(2):
            at = VEC + h * HEAD_DIM
            q = proj[:, at : at + HEAD_DIM]
            k = proj[:, qw + at : qw + at + HEAD_DIM]
            v = proj[:, 2 * qw + at : 2 * qw + at + HEAD_DIM]
            sc = dot(q, k, 1, 1) * factor
            e = jnp.exp(sc - jnp.max(sc, axis=-1, keepdims=True))
            p = e / jnp.sum(e, axis=-1, keepdims=True)
            probs[img, h] = p
            outs.append(dot(p.astype(BF16), v, 1, 0).astype(BF16))
        mix[img] = jnp.concatenate(outs, axis=1)
        return carry

    lax.fori_loop(0, 2, att_step, 0)
    ag_c[1]()
    gather_swap(2)
    lax.fori_loop(2, nimg, att_step, 0)
    o_wait()

    def o_part(img):
        part[img] = dot(mix[img], ow[...], 1, 0).astype(BF16)

    rs_h = rscatter(0, part, r1, (dx, dy, rx, ry), o_part)
    rs_h[0]()
    rs_h[4]()
    gather_hop(1, 1)
    gather_drain(0)
    gather_own(2)
    gather_other(2)
    rs_h[1]()
    gather_hop(1, 2)
    ag_c[2]()
    rs_h[3]()
    ag_x[3]()
    ag_n = agather(2, n2)
    for i in range(2):
        hidden = xall[2 * y + i, own_rows].astype(F32) + rs_h[2](i) + o_b
        hid_s[i] = hidden
        hat, inv = normalize(hidden)
        hat2_s[i] = hat
        inv2_s[i] = jnp.broadcast_to(inv, (own_len, 128))
        n2[2 * y + i, own_rows] = (hat * g2 + s2).astype(BF16)
    ag_n[0]()
    gather_hop(2, 1)
    ag_n[1]()
    gather_end(1)
    gather_hop(2, 2)
    ag_n[2]()

    wlane = lax.broadcasted_iota(jnp.int32, (1, win), 1)
    valid = (wlane >= off_out) & (wlane < off_out + ffp)

    def in_step(img, carry):
        pre = dot(n2[img], w[:, in_win : in_win + win], 1, 0) + inb[0:1]
        a, sl = gelu_parts(pltpu.roll(pre, shift, 1))
        act[img] = jnp.where(valid, a, 0.0).astype(BF16)
        slope[img] = jnp.where(valid, sl, 0.0)
        return carry
    lax.fori_loop(0, nimg, in_step, 0)

    rtile = width // 3

    def gout_step(t, carry):
        t = 1 + sg * (1 - t)
        r = pl.ds(pl.multiple_of(t * rtile, rtile), rtile)
        acc = jnp.zeros((rtile, win), F32)
        for img in range(nimg):
            acc = acc + dot(call[img, :, r], act[img], 0, 0)
        gout_tail[r] = acc[:, 0 : 2 * cols - out_win].astype(BF16)
        g[r, 2 * cols : 3 * cols] = acc[:, 2 * cols - out_win :].astype(BF16)
        return carry
    lax.fori_loop(0, 1, gout_step, 0)
    z_first(0, (2,))
    lax.fori_loop(1, 2, gout_step, 0)
    z_first(0, (1,))
    lax.fori_loop(2, 3, gout_step, 0)
    z_first(0, (0, 3))
    gather_end(2)

    def gp_step(img, carry):
        ga = dot(call[img], w[:, out_win : out_win + win], 1, 0) * slope[img]
        gp[img] = pltpu.roll(ga, win - shift, 1).astype(BF16)
        return carry
    lax.fori_loop(0, nimg, gp_step, 0, unroll=2)
    ib_begin()

    def gn2_part(img):
        part[img] = dot(gp[img], w[:, in_win : in_win + win], 1, 1).astype(BF16)

    rs_g2 = rscatter(2, part, r1, (dx, dy, rx, ry), gn2_part)
    rs_g2[0]()
    rs_g2[4]()

    def gin_step(t, carry):
        r = pl.ds(pl.multiple_of(t * rtile, rtile), rtile)
        acc = jnp.zeros((rtile, win), F32)
        for img in range(nimg):
            acc = acc + dot(n2[img, :, r], gp[img], 0, 0)
        lo = cols - in_win
        gin_tail[r] = acc[:, 0:lo].astype(BF16)
        g[r, cols : 2 * cols - 128] = acc[:, lo : win - 128].astype(BF16)
        g[r, 2 * cols - 128 : 2 * cols] = (acc[:, win - 128 :] + gout_tail[r].astype(F32)).astype(BF16)
        return carry

    lax.fori_loop(0, 3, gin_step, 0)
    z_first(1)
    rs_g2[1]()
    z_merge(0, 1)

    sums = [jnp.zeros((1, width), F32) for _ in range(6)]
    ag_g = agather(3, gb)
    for i in range(2):
        gn2 = rs_g2[2](i)
        hat = hat2_s[i]
        sums[2] = sums[2] + jnp.sum(gn2 * hat, axis=0, keepdims=True)
        sums[3] = sums[3] + jnp.sum(gn2, axis=0, keepdims=True)
        up = call[2 * y + i, own_rows].astype(F32)
        gh = up + norm_back(gn2, g2, hat, inv2_s[i][:, 0:1])
        gh_s[i] = gh
        low = gh.astype(BF16)
        gb[2 * y + i, own_rows] = low
        sums[4] = sums[4] + jnp.sum(low.astype(F32), axis=0, keepdims=True)
        sums[5] = sums[5] + jnp.sum(up, axis=0, keepdims=True)
    rs_g2[3]()
    ag_c[3]()
    ag_n[3]()
    ag_g[0]()
    for n in range(2, 6):
        vsum[n : n + 1] = sums[n]
    vsum[6:8] = jnp.zeros((2, width), F32)
    vsum[0:2] = jnp.zeros((2, width), F32)
    z_merge(0, 0)

    def out_part(img):
        part2[img] = dot(act[img], w[:, out_win : out_win + win], 1, 1).astype(BF16)

    rs_o = rscatter(1, part2, r1b, (dxb, dyb, rxb, ryb), out_part)
    rs_o[0]()
    ag_g[1]()
    ag_g[2]()

    gacc = jnp.zeros((qw, width), F32)
    for img in range(nimg):
        gacc = gacc + dot(mix[img], gb[img], 0, 0)
    og[...] = gacc.astype(BF16)
    zo_first()
    rs_o[4]()

    def attb_step(img, carry):
        proj, gbi = qkv[img], gb[img]
        gmix = dot(gbi, ow[...], 1, 1).astype(BF16)
        zero = jnp.zeros((length, VEC), BF16)
        dq, dk, dv = [], [], []
        for h in range(2):
            at = VEC + h * HEAD_DIM
            q = proj[:, at : at + HEAD_DIM]
            k = proj[:, qw + at : qw + at + HEAD_DIM]
            v = proj[:, 2 * qw + at : 2 * qw + at + HEAD_DIM]
            gm = gmix[:, h * HEAD_DIM : (h + 1) * HEAD_DIM]
            p = probs[img, h]
            gpr = dot(gm, v, 1, 1)
            gs = (p * (gpr - jnp.sum(p * gpr, axis=-1, keepdims=True))).astype(BF16)
            dq.append((dot(gs, k, 1, 0) * factor).astype(BF16))
            dk.append((dot(gs, q, 0, 0) * factor).astype(BF16))
            dv.append(dot(p.astype(BF16), gm, 0, 0).astype(BF16))
        pad = jnp.zeros((length, cols - VEC - 3 * qw), BF16)
        dqkv[img] = jnp.concatenate([zero] + dq + dk + dv + [pad], axis=1)
        return carry

    def ln1_sum_step(img, carry):
        pr = part[img].astype(F32)
        hat = (xall[img].astype(F32) - mean1[img][:, 0:1]) * inv1[img][:, 0:1]
        vsum[0:1] = vsum[0:1] + jnp.sum(pr * hat, axis=0, keepdims=True)
        vsum[1:2] = vsum[1:2] + jnp.sum(pr, axis=0, keepdims=True)
        return carry

    def vcol_step(t, carry):
        r = pl.ds(pl.multiple_of(t * rtile, rtile), rtile)
        vcol = jnp.transpose(jnp.concatenate([vsum[:, r], jnp.zeros((120, rtile), F32)], axis=0), (1, 0))
        g[r, 0:128] = (g[r, 0:128].astype(F32) + vcol).astype(BF16)
        return carry

    def gn1_part(img):
        part[img] = dot(dqkv[img], w[:, 0:cols], 1, 1).astype(BF16)
    rs_g1 = rscatter(4, part, r1, (dx, dy, rx, ry), gn1_part)

    def gqkv_step(t, carry):
        t = 1 + sg * (1 - t)
        r = pl.ds(pl.multiple_of(t * rtile, rtile), rtile)
        acc = jnp.zeros((rtile, cols), F32)
        for img in range(nimg):
            acc = acc + dot(n1[img, :, r], dqkv[img], 0, 0)
        g[r, 0 : cols - 128] = acc[:, 0 : cols - 128].astype(BF16)
        g[r, cols - 128 : cols] = (acc[:, cols - 128 :] + gin_tail[r].astype(F32)).astype(BF16)
        return carry

    lax.fori_loop(0, 1, attb_step, 0)
    ib_pass()
    zreduce_own(0)
    f_begin(0)
    lax.fori_loop(1, 3, attb_step, 0)
    z_merge(1, 1)
    lax.fori_loop(3, nimg, attb_step, 0)
    zdrain(0)
    lax.fori_loop(0, 1, gqkv_step, 0)
    z_first(2, (2,))
    lax.fori_loop(1, 2, gqkv_step, 0)
    z_first(2, (1,))
    lax.fori_loop(2, 3, gqkv_step, 0)
    z_first(2, (0, 3))
    rs_o[1]()
    rs_g1[0]()
    rs_g1[4]()
    qb_begin()
    z_merge(1, 0)
    lax.fori_loop(0, nimg, ln1_sum_step, 0)
    lax.fori_loop(0, 3, vcol_step, 0)
    z_first(3)
    f_spread(0)
    ib_mid()
    zo_merge()
    z_merge(2, 1)
    zreduce_own(1)
    f_begin(1)
    rs_g1[1]()
    z_merge(2, 0)
    f_relay(0)
    ib_last()
    f_spread(1)
    z_merge(3, 1)

    z_merge(3, 0)
    pl.when(z == s)(o_here)
    f_relay(1)
    f_drain(0)
    zreduce_own(2)
    f_begin(2)
    f_spread(2)
    f_drain(1)
    zreduce_own(3)
    f_begin(3)
    f_end(0)
    f_end(1)
    emit_out()
    f_relay(2)
    f_spread(3)
    for i in range(2):
        gn1 = rs_g1[2](i)
        hat, inv = normalize(xall[2 * y + i, own_rows].astype(F32))
        st_g[i] = (gh_s[i] + norm_back(gn1, g1, hat, inv)).astype(BF16)
    ag_g[3]()
    stores[7].start()
    for i in range(2):
        st_o[i] = (hid_s[i] + rs_o[2](i) + out_b).astype(BF16)
    stores[6].start()
    pl.when((s + 2) % 4 == z)(o_x)
    ib_end()
    emit_ib()
    f_end(2)
    emit_upper()
    o_end()
    stores[5].start()
    f_relay(3)
    f_end(3)
    emit_lower()

    for ch in (1, 2):
        gather_drain(ch)
    for ch in (1, 2, 3):
        zdrain(ch)
    for ch in (2, 3):
        f_drain(ch)
    o_drain()
    vec_drain()
    rs_o[3]()
    rs_g1[3]()
    pl.when(z != s)(lambda: zo_send(False).wait_send())
    pl.when(z == s)(lambda: o_out_done(2))
    pl.when((z == s) | ((s + 2) % 4 == z))(lambda: o_out_done(3))
    pl.when(z != s)(lambda: qb_send().wait_send())
    for k in range(1, nz):
        ib_send(k).wait_send()
    for n in range(7):
        ib_msg(nz + n, rank, core_n).wait_send()
    for cp in stores:
        cp.wait()


def widen_kernel(n_mat, n_copy, n_row, *refs):
    n = n_mat + n_copy + n_row
    src, refs = refs[:n], refs[n:]
    big, refs = refs[: n_mat + n_copy], refs[n_mat + n_copy :]
    n_flat = (len(refs) - 2 - n - n_mat) // 2
    flat_out, refs = refs[:n_flat], refs[n_flat:]
    held, refs = refs[:n], refs[n:]
    wide, refs = refs[:n_mat], refs[n_mat:]
    flat, (in_s, out_s) = refs[:n_flat], refs[n_flat:]
    got = [pltpu.make_async_copy(src[i], held[i], in_s.at[i]) for i in range(n)]
    put = [pltpu.make_async_copy(wide[i] if i < n_mat else held[i], big[i], out_s.at[i])
           for i in range(n_mat + n_copy)]
    put_flat = [pltpu.make_async_copy(flat[i], flat_out[i], out_s.at[n_mat + n_copy + i]) for i in range(n_flat)]
    for cp in got:
        cp.start()
    for i in range(n_mat + n_copy):
        got[i].wait()
        if i < n_mat:
            rows = wide[i].shape[0]
            for r in range(0, rows, 48):
                wide[i][r : r + 48] = held[i][r : r + 48].astype(F32)
        put[i].start()
    at = 0
    for i in range(n_mat + n_copy, n):
        got[i].wait()
        for r in range(held[i].shape[0]):
            flat[at][...] = held[i][r : r + 1].reshape(held[i].shape[1])
            put_flat[at].start()
            at += 1
    for cp in put + put_flat:
        cp.wait()


def widen(mats, rows, others, tables):
    hbm = pl.BlockSpec(memory_space=pl.ANY)
    arrays = list(mats) + list(others) + list(tables)
    n = len(arrays)
    flat = [jax.ShapeDtypeStruct((t.shape[1],), F32) for t in tables for _ in range(t.shape[0])]
    shapes = [jax.ShapeDtypeStruct((rows, m.shape[1]), F32) for m in mats]
    shapes += [jax.ShapeDtypeStruct(o.shape, o.dtype) for o in others] + flat
    return pl.pallas_call(
        functools.partial(widen_kernel, len(mats), len(others), len(tables)),
        out_shape=tuple(shapes),
        in_specs=[hbm] * n,
        out_specs=[hbm] * len(shapes),
        scratch_shapes=[pltpu.VMEM(a.shape, a.dtype) for a in arrays]
        + [pltpu.VMEM((rows, m.shape[1]), F32) for m in mats]
        + [pltpu.VMEM(f.shape, F32) for f in flat]
        + [pltpu.SemaphoreType.DMA((n,)), pltpu.SemaphoreType.DMA((len(shapes),))],
    )(*arrays)


def layer_fast(
    tokens, cotangent, ln1_gain, ln1_shift, q_weight, q_bias, k_weight, v_weight, v_bias,
    o_weight, o_bias, ln2_gain, ln2_shift, in_weight, in_bias, out_weight, out_bias,
):
    ns, ndp = lax.axis_size("seq"), lax.axis_size("dp")
    nz, ranks = ndp // 2, 2 * ns
    images, own_len, width = tokens.shape
    ff = in_weight.shape[1]
    hid, ffp = width // ranks, ff // ranks
    rows = q_weight.shape[0]
    vec = [ln1_gain, ln1_shift, q_bias, v_bias, o_bias, ln2_gain, ln2_shift, out_bias]
    slab = (2 * VEC, (rows + 127) // 128 * 128)
    total = 3 * 512
    win = (ffp + 127) // 128 * 128
    nimg, length, cols = 2 * images, own_len * ns, 512
    tall = (nimg, length, width)
    half = (own_len, width)
    D = pltpu.SemaphoreType.DMA
    V = pltpu.VMEM
    scratch = dict(
        wp=V((2, rows, total), BF16), fgrad=V((ranks, rows, total), BF16), ograd=V((hid + 16, width), BF16),
        ibgrad=V((ranks, 8, win), F32), st_q=V((rows, width), BF16), st_k=V((rows, width), BF16),
        st_v=V((rows, width), BF16), st_in=V((rows, ff), BF16), st_out=V((rows, ff), BF16),
        vslab=V((2, nz) + slab, BF16), inb=V((8, win), F32), inflat=V((ff,), BF16), inrow=V((1, ff), F32),
        **{f"vflat{n}": V((rows,), BF16) for n in range(VEC)}, vrows=V(slab, F32),
        st_o=V((2,) + half, BF16), st_g=V((2,) + half, BF16), st_vec=V((VEC, rows), F32), st_ib=V((1, ff), F32),
        w=V((2 * nz * rows, total), BF16), ow=V((hid, width), BF16), xall=V(tall, BF16), call=V(tall, BF16),
        n1=V(tall, BF16), n2=V(tall, BF16), gb=V(tall, BF16), qkv=V((nimg, length, cols), BF16),
        probs=V((nimg, 2, length, length), F32), mix=V((nimg, length, hid), BF16),
        act=V((nimg, length, win), BF16), slope=V((nimg, length, win), F32), gp=V((nimg, length, win), BF16),
        part=V(tall, BF16), part2=V(tall, BF16), r1=V((nimg, 2) + half, BF16), r1b=V((nimg, 2) + half, BF16),
        dx=V(half, BF16), dy=V(half, BF16), rx=V((2,) + half, BF16), ry=V((2,) + half, BF16),
        dxb=V(half, BF16), dyb=V(half, BF16), rxb=V((2,) + half, BF16), ryb=V((2,) + half, BF16),
        hid_s=V((2,) + half, F32), hat2_s=V((2,) + half, F32), inv2_s=V((2, own_len, 128), F32),
        gh_s=V((2,) + half, F32), vecs=V((VEC, width), F32),
        g=V((2 * nz * rows, total), BF16), rb=V((2, nz + 2, 2, rows, cols), BF16),
        rbh=V((2, nz + 2, 2, rows, cols // 2), BF16),
        rbo=V((nz + 1, hid, width), BF16), gin_tail=V((width, 128), BF16), gout_tail=V((width, 128), BF16),
        dqkv=V((nimg, length, cols), BF16), vsum=V((8, width), F32),
        mean1=V((nimg, length, 128), F32), inv1=V((nimg, length, 128), F32), ibx=V((nz, 8, win), F32),
        isb=V((8, win), F32), og=V((hid, width), BF16),
        qbs=V((8, cols), F32), qbx=V((nz, 8, cols), F32),
        gy_s=D((3,)), gz_s=D((2, nz, 2)), gzl_s=D((2, 2)), g_r=D((3, nz, 2)), o_s=D((2, 2)), o_r=D((2,)),
        ag_s=D((14,)), ag_r=D((14,)), rs_s=D((2, 14)), rs_r=D((2, 14)), z_s=D((3, 4, 2)),
        z_r=D((4, nz + 2, 2)), zo_s=D((4,)), zo_r=D((nz + 3,)), f_s=D((2, 7)), f_r=D((4, 7)), ib_s=D((nz + 7,)),
        ib_r=D((nz + 7,)), qb_s=D((1,)), qb_r=D((nz,)), v_s=D((nz,)),
        v_r=D((nz + 1,)),
    )
    hbm = pl.BlockSpec(memory_space=pl.ANY)
    out, gtok, gq, gk, gv, gin, gout, go, gvec, gib = pl.pallas_call(
        functools.partial(layer_kernel, nz, hid, ffp),
        out_shape=(
            jax.ShapeDtypeStruct(tokens.shape, BF16), jax.ShapeDtypeStruct(tokens.shape, BF16),
            jax.ShapeDtypeStruct((rows, width), BF16), jax.ShapeDtypeStruct((rows, width), BF16),
            jax.ShapeDtypeStruct((rows, width), BF16), jax.ShapeDtypeStruct((rows, ff), BF16),
            jax.ShapeDtypeStruct((rows, ff), BF16), jax.ShapeDtypeStruct((hid + 16, width), BF16),
            jax.ShapeDtypeStruct((VEC, rows), F32), jax.ShapeDtypeStruct((1, ff), F32),
        ),
        in_specs=[hbm] * (9 + VEC),
        out_specs=[hbm] * 10,
        scratch_shapes=list(scratch.values()),
        compiler_params=pltpu.CompilerParams(
            collective_id=0, has_side_effects=True, vmem_limit_bytes=65000 * 1024),
    )(tokens, cotangent, q_weight, k_weight, v_weight, in_weight, out_weight.T, o_weight, in_bias, *vec)
    (gin, gout, gq, gk, gv, go, out, gtok, d_g1, d_s1, d_g2, d_s2, d_ob, d_outb, d_qb, d_vb, gib) = widen(
        [gin, gout, gq, gk, gv, go], rows, [out, gtok], [gvec, gib])
    return (out, gtok, d_g1, d_s1, gq, d_qb, gk, gv, d_vb, go, d_ob, d_g2, d_s2, gin, gib, gout.T, d_outb)


def mm(a, b, ca, cb):
    return lax.dot_general(a, b, (((ca,), (cb,)), ((), ())), preferred_element_type=F32)


def on_device(
    tokens, cotangent, ln1_gain, ln1_shift, q_weight, q_bias, k_weight, v_weight, v_bias,
    o_weight, o_bias, ln2_gain, ln2_shift, in_weight, in_bias, out_weight, out_bias,
):
    part = lax.axis_index("seq")
    parts = lax.axis_size("seq")
    groups = lax.axis_size("dp")
    images, own_len, width = tokens.shape
    ff = in_weight.shape[1]
    hid = width // parts
    ffp = ff // parts
    heads = HEADS // parts
    length = own_len * parts
    rows = images * length

    def cols(w, n):
        return lax.dynamic_slice_in_dim(w, part * n, n, axis=1)

    vecs = jnp.stack(
        [ln1_gain, ln1_shift, q_bias, v_bias, o_bias, ln2_gain, ln2_shift, out_bias]
    )
    vecs = lax.all_gather(vecs, "dp", axis=1, tiled=True).astype(F32)
    g1, s1, qb, vb, ob, g2, s2, outb = [vecs[i] for i in range(8)]
    x = lax.all_gather(tokens, "seq", axis=1, tiled=True).reshape(rows, width)
    cot = lax.all_gather(cotangent, "seq", axis=1, tiled=True).reshape(rows, width)
    qkv = jnp.concatenate([cols(q_weight, hid), cols(k_weight, hid), cols(v_weight, hid)], axis=1)
    qkv = lax.all_gather(qkv, "dp", axis=0, tiled=True)
    o_w = lax.all_gather(o_weight, "dp", axis=0, tiled=True)
    o_w = lax.dynamic_slice_in_dim(o_w, part * hid, hid, axis=0)
    in_w = lax.all_gather(cols(in_weight, ffp), "dp", axis=0, tiled=True)
    out_w = lax.dynamic_slice_in_dim(out_weight, part * ffp, ffp, axis=0)
    out_w = lax.all_gather(out_w.T, "dp", axis=0, tiled=True)
    qb_own = lax.dynamic_slice_in_dim(qb, part * hid, hid)
    vb_own = lax.dynamic_slice_in_dim(vb, part * hid, hid)
    inb_own = lax.dynamic_slice_in_dim(in_bias, part * ffp, ffp).astype(F32)

    def scatter_tokens(partial):
        return lax.psum_scatter(
            partial.astype(BF16).reshape(images, length, width),
            "seq", scatter_dimension=1, tiled=True,
        ).astype(F32)

    hat1, _ = normalize(x.astype(F32))
    normed1 = (hat1 * g1 + s1).astype(BF16)
    proj = mm(normed1, qkv, 1, 0)
    queries = (proj[:, :hid] + qb_own).astype(BF16).reshape(images, length, heads, HEAD_DIM)
    keys = proj[:, hid : 2 * hid].astype(BF16).reshape(images, length, heads, HEAD_DIM)
    values = (proj[:, 2 * hid :] + vb_own).astype(BF16).reshape(images, length, heads, HEAD_DIM)
    factor = 1.0 / math.sqrt(HEAD_DIM)
    ein = lambda s, a, b: jnp.einsum(s, a, b, preferred_element_type=F32)
    scores = ein("iqhd,ikhd->ihqk", queries, keys) * factor
    top = jnp.max(scores, axis=-1, keepdims=True)
    expo = jnp.exp(scores - top)
    probs = expo / jnp.sum(expo, axis=-1, keepdims=True)
    probs_low = probs.astype(BF16)
    mixed = ein("ihqk,ikhd->iqhd", probs_low, values).astype(BF16).reshape(rows, hid)
    start = tokens.astype(F32)
    hidden = start + scatter_tokens(mm(mixed, o_w, 1, 0)) + ob
    hat2, r2 = normalize(hidden)
    normed2 = (hat2 * g2 + s2).astype(BF16)
    normed2 = lax.all_gather(normed2, "seq", axis=1, tiled=True).reshape(rows, width)
    pre = mm(normed2, in_w, 1, 0) + inb_own
    act, slope = gelu_parts(pre)
    act = act.astype(BF16)
    out = hidden + scatter_tokens(mm(act, out_w, 1, 1)) + outb
    d_out_w = mm(cot, act, 0, 0)
    cot_own = cotangent.astype(F32)
    grad_pre = (mm(cot, out_w, 1, 0) * slope).astype(BF16)
    d_in_w = mm(normed2, grad_pre, 0, 0)
    d_in_b = jnp.sum(grad_pre.astype(F32), axis=0)
    grad_n2 = scatter_tokens(mm(grad_pre, in_w, 1, 1))
    grad_hidden = cot_own + norm_back(grad_n2, g2, hat2, r2)
    branch_own = grad_hidden.astype(BF16)
    branch = lax.all_gather(branch_own, "seq", axis=1, tiled=True).reshape(rows, width)
    d_o_w = mm(mixed, branch, 0, 0)
    grad_mixed = mm(branch, o_w, 1, 1).astype(BF16).reshape(images, length, heads, HEAD_DIM)
    grad_probs = ein("iqhd,ikhd->ihqk", grad_mixed, values)
    row_dot = jnp.sum(probs * grad_probs, axis=-1, keepdims=True)
    grad_scores = (probs * (grad_probs - row_dot)).astype(BF16)
    grad_q = (ein("ihqk,ikhd->iqhd", grad_scores, keys) * factor).astype(BF16).reshape(rows, hid)
    grad_k = (ein("ihqk,iqhd->ikhd", grad_scores, queries) * factor).astype(BF16).reshape(rows, hid)
    grad_v = ein("ihqk,iqhd->ikhd", probs_low, grad_mixed).astype(BF16).reshape(rows, hid)
    grad_qkv = jnp.concatenate([grad_q, grad_k, grad_v], axis=1)
    d_qkv = mm(normed1, grad_qkv, 0, 0)
    d_qb = jnp.sum(grad_q.astype(F32), axis=0)
    d_vb = jnp.sum(grad_v.astype(F32), axis=0)
    grad_n1 = scatter_tokens(mm(grad_qkv, qkv, 1, 1))
    hat1o, r1o = normalize(start)
    grad_tokens = grad_hidden + norm_back(grad_n1, g1, hat1o, r1o)
    wide = jnp.concatenate([d_qkv, d_in_w, d_out_w], axis=1).astype(BF16)
    wide = lax.psum_scatter(wide, "dp", scatter_dimension=0, tiled=True)
    wide = lax.all_gather(wide, "seq", axis=0, tiled=False).astype(F32)

    def spread(lo, n):
        return wide[:, :, lo : lo + n].transpose(1, 0, 2).reshape(width // groups, n * parts)

    gq, gk, gv = [spread(i * hid, hid) for i in range(3)]
    gin = spread(3 * hid, ffp)
    gout = wide[:, :, 3 * hid + ffp :].transpose(0, 2, 1).reshape(ff, width // groups)
    o_full = lax.all_gather(
        lax.psum_scatter(d_o_w.astype(BF16), "dp", scatter_dimension=1, tiled=True),
        "seq", axis=0, tiled=True,
    )
    go = lax.all_to_all(o_full, "dp", split_axis=0, concat_axis=1, tiled=True).astype(F32)
    own_sums = jnp.stack([
        jnp.sum(grad_n1 * hat1o, axis=(0, 1)), jnp.sum(grad_n1, axis=(0, 1)),
        jnp.sum(grad_n2 * hat2, axis=(0, 1)), jnp.sum(grad_n2, axis=(0, 1)),
        jnp.sum(branch_own.astype(F32), axis=(0, 1)), jnp.sum(cot_own, axis=(0, 1)),
        lax.dynamic_update_slice_in_dim(jnp.zeros(width, F32), d_qb, part * hid, 0),
        lax.dynamic_update_slice_in_dim(jnp.zeros(width, F32), d_vb, part * hid, 0),
    ])
    bias_in = lax.dynamic_update_slice_in_dim(jnp.zeros(ff, F32), d_in_b, part * ffp, 0)
    total = lax.psum(jnp.concatenate([own_sums.reshape(-1), bias_in]), ("dp", "seq"))
    vec_part = total[: 8 * width].reshape(8, groups, width // groups)
    vec_part = lax.dynamic_index_in_dim(vec_part, lax.axis_index("dp"), axis=1, keepdims=False)
    bias_total = total[8 * width :]
    return (
        out.astype(BF16), grad_tokens.astype(BF16), vec_part[0], vec_part[1], gq, vec_part[6],
        gk, gv, vec_part[7], go, vec_part[4], vec_part[2], vec_part[3], gin, bias_total, gout,
        vec_part[5],
    )


def solution(mesh):
    fast = mesh.shape["dp"] == 2 * mesh.shape["seq"]
    rows, vec = P("dp", None), P("dp")
    tok = P("dp", "seq", None)
    return jax.shard_map(
        layer_fast if fast else on_device,
        mesh=mesh,
        in_specs=(tok, tok, vec, vec, rows, vec, rows, rows, vec, rows, vec, vec, vec, rows,
                  P(), P(None, "dp"), vec),
        out_specs=(tok, tok, vec, vec, rows, vec, rows, rows, vec, rows, vec, vec, vec, rows,
                   P(), P(None, "dp"), vec),
        check_vma=False,
    )
```

```python
import functools
import math

import jax
import jax.numpy as jnp
from jax import lax
from jax.experimental import pallas as pl
from jax.experimental.pallas import tpu as pltpu
from jax.sharding import PartitionSpec as P

BF16, F32 = jnp.bfloat16, jnp.float32
HEADS, HEAD_DIM = 16, 72
eps_norm = 1e-06
gelu_coef = 0.7978845608028654
gelu_cube = 0.044715
MESH = pl.DeviceIdType.MESH
VEC = 8


def normalize(values):
    row_mean = jnp.mean(values, axis=-1, keepdims=True)
    centred = values - row_mean
    inverse = lax.rsqrt(jnp.mean(centred * centred, axis=-1, keepdims=True) + eps_norm)
    return centred * inverse, inverse


def norm_back(grad_normed, gain_vec, scaled, inverse):
    grad_scaled = grad_normed * gain_vec
    centred_grad = grad_scaled - jnp.mean(grad_scaled, axis=-1, keepdims=True)
    return inverse * (
        centred_grad - scaled * jnp.mean(grad_scaled * scaled, axis=-1, keepdims=True)
    )


def gelu_parts(pre_act):
    square = pre_act * pre_act
    tanh_val = jnp.tanh(pre_act * (gelu_coef + gelu_coef * gelu_cube * square))
    gate = 0.5 + 0.5 * tanh_val
    value_part = pre_act * gate
    slope_part = gate + value_part * (1.0 - gate) * (2.0 * gelu_coef + 6.0 * gelu_coef * gelu_cube * square)
    return (value_part, slope_part)


def dot(a, b, ca, cb):
    return lax.dot_general(a, b, (((ca,), (cb,)), ((), ())), preferred_element_type=F32)


def layer_kernel(
    nz, hid, ffp,
    tok, cot_in, q_in, k_in, v_in, in_in, out_in, ow_in, inb_in, vin0, vin1, vin2, vin3, vin4, vin5, vin6, vin7,
    out_ref, gtok_ref, q_out, k_out, v_out, in_out, out_out, o_out, vec_out, ib_out,
    wp, fgrad, ograd, ibgrad, st_q, st_k, st_v, st_in, st_out, vslab, inb, inflat, inrow, vflat0, vflat1, vflat2, vflat3, vflat4, vflat5, vflat6, vflat7, vrows, st_o, st_g, st_vec, st_ib,
    w, ow, xall, call, n1, n2, gb, qkv, probs, mix, act, slope, gp, part, part2, r1, r1b,
    dx, dy, rx, ry, dxb, dyb, rxb, ryb, hid_s, hat2_s, inv2_s, gh_s, vecs, g, rb, rbh, rbo, gin_tail,
    gout_tail, dqkv, vsum, mean1, inv1, ibx, isb, og, qbs, qbx,
    gy_s, gz_s, gzl_s, g_r, o_s, o_r, ag_s, ag_r, rs_s, rs_r, z_s, z_r, zo_s, zo_r, f_s, f_r,
    ib_s, ib_r, qb_s, qb_r, v_s, v_r,
):
    d, s = lax.axis_index("dp"), lax.axis_index("seq")
    z, y = d // 2, d % 2
    x, c = s // 2, s % 2
    rank = 2 * s + y
    nimg, length, width = xall.shape
    own_len = dx.shape[0]
    rows8 = wp.shape[1]
    plane = 2 * rows8
    cols = 512
    qw = hid
    in_at = VEC + 3 * qw
    in_win = in_at // 128 * 128
    out_at = in_at + ffp
    out_win = out_at // 128 * 128
    win = (ffp + 127) // 128 * 128
    off_in, off_out = in_at - in_win, out_at - out_win
    shift = off_out - off_in
    core_n, x_n, y_n = (d, s + 1 - 2 * c), (d, (s + 2) % 4), (d + 1 - 2 * y, s)
    right, left = (d + 2, s), (d - 2, s)
    has_r, has_l = z < nz - 1, z > 0
    sg = 1 - 2 * (z // 2)
    is_end = (z == 0) | (z == nz - 1)
    middle = (z > 0) & (z < nz - 1)
    factor = 1.0 / math.sqrt(HEAD_DIM)

    def plane_at(k):
        return z + sg * k

    def away(k):
        return (d + 2 * sg * k, s)

    def rc(src, dst, ss, rs, dev):
        return pltpu.make_async_remote_copy(
            src_ref=src, dst_ref=dst, send_sem=ss, recv_sem=rs, device_id=dev, device_id_type=MESH
        )

    barrier = pltpu.get_barrier_semaphore()
    column = [((d + 2 * k) % (2 * nz), s) for k in range(1, nz)]
    for dev in [core_n, x_n, y_n] + column:
        pl.semaphore_signal(barrier, inc=1, device_id=dev, device_id_type=MESH)

    own_rows = pl.ds(pl.multiple_of(s * own_len, 16), own_len)
    vflat = (vflat0, vflat1, vflat2, vflat3, vflat4, vflat5, vflat6, vflat7)
    vec_loads = list(zip((vin0, vin1, vin2, vin3, vin4, vin5, vin6, vin7), vflat))
    loads = [pltpu.make_async_copy(a, b, rs_s.at[n // 14, n % 14]) for n, (a, b) in enumerate(
        [(q_in, st_q), (k_in, st_k), (v_in, st_v), (in_in, st_in),
         (tok.at[0], xall.at[2 * y, own_rows]), (tok.at[1], xall.at[2 * y + 1, own_rows])] + vec_loads + [(out_in, st_out),
         (cot_in.at[0], call.at[2 * y, own_rows]), (cot_in.at[1], call.at[2 * y + 1, own_rows]),
         (inb_in, inflat)])]
    for cp in loads:
        cp.start()
    load_o = pltpu.make_async_copy(ow_in, ow, rs_s.at[1, 13])
    pl.when(z == s)(lambda: load_o.start())

    def build_first():
        def go(k):
            for j in range(2):
                t = 2 * k + j
                wp[j, :, 0:128] = jnp.zeros((rows8, 128), BF16)
                for n, st in enumerate((st_q, st_k, st_v)):
                    wp[j, :, VEC + n * qw : VEC + (n + 1) * qw] = st[:, t * qw : (t + 1) * qw]
                wp[j, :, in_at:cols] = st_in[:, t * ffp : t * ffp + cols - in_at]
        for k in range(4):
            pl.when(s == k)(functools.partial(go, k))

    def build_rest():
        def go(k):
            for j in range(2):
                t = 2 * k + j
                wp[j, :, 3 * cols - 128 :] = jnp.zeros((rows8, 128), BF16)
                wp[j, :, cols : in_at + ffp] = st_in[:, t * ffp + cols - in_at : (t + 1) * ffp]
                wp[j, :, out_at : out_at + ffp] = st_out[:, t * ffp : (t + 1) * ffp]
        for k in range(4):
            pl.when(s == k)(functools.partial(go, k))

    def build_bias():
        def go(t):
            inb[...] = jnp.zeros_like(inb)
            inb[0:1, off_in : off_in + ffp] = inrow[0:1, t * ffp : (t + 1) * ffp]
        for t in range(8):
            pl.when(rank == t)(functools.partial(go, t))

    for cp in loads[:6]:
        cp.wait()
    build_first()
    pl.semaphore_wait(barrier, 3 + len(column))

    def wrows(origin, sub):
        return pl.ds(pl.multiple_of(origin * plane + sub * rows8, 16), rows8)

    def wslab(ch, origin, sub):
        return w.at[wrows(origin, sub), pl.ds(ch * cols, cols)]

    def wsend(ch, origin, sub, src, to_right, own=False):
        sems = gz_s.at[ch % 2, origin, sub] if to_right or not own else gzl_s.at[ch % 2, sub]
        return rc(src, wslab(ch, origin, sub), sems, g_r.at[ch, origin, sub],
                  right if to_right else left)

    def wrecv(ch, origin, sub):
        slab = wslab(ch, origin, sub)
        rc(slab, slab, g_r.at[ch, origin, sub], g_r.at[ch, origin, sub], core_n).wait_recv()

    def gather_own(ch):
        src = wp.at[y, :, pl.ds(ch * cols, cols)]
        pl.when(has_r)(lambda: wsend(ch, z, y, src, True).start())
        pl.when(has_l)(lambda: wsend(ch, z, y, src, False, True).start())
        w[wrows(z, y), ch * cols : (ch + 1) * cols] = wp[y, :, ch * cols : (ch + 1) * cols]

    def gather_swap(ch):
        rc(wp.at[1 - y, :, pl.ds(ch * cols, cols)], wslab(ch, z, y), gy_s.at[ch], g_r.at[ch, z, y],
           y_n).start()

    def gather_other(ch):
        wrecv(ch, z, 1 - y)
        src = wslab(ch, z, 1 - y)
        pl.when(has_r)(lambda: wsend(ch, z, 1 - y, src, True).start())
        pl.when(has_l)(lambda: wsend(ch, z, 1 - y, src, False, True).start())

    def gather_hop(ch, k):
        for sub in range(2):
            gather_hop1(ch, k, sub)

    def gather_end(ch):
        for k in range(1, nz):
            for sub in range(2):
                pl.when(is_end)(lambda: wrecv(ch, plane_at(k), sub))

    def gather_hop1(ch, k, sub):
        def from_left():
            wrecv(ch, z - k, sub)
            pl.when(has_r)(lambda: wsend(ch, z - k, sub, wslab(ch, z - k, sub), True).start())

        def from_right():
            wrecv(ch, z + k, sub)
            pl.when(has_l)(lambda: wsend(ch, z + k, sub, wslab(ch, z + k, sub), False).start())

        pl.when(middle & (z - k >= 0))(from_left)
        pl.when(middle & (z + k < nz))(from_right)

    def gather_drain(ch):
        for k in range(nz):
            for sub in range(2):
                pl.when((z - k >= 0) & has_r)(
                    lambda: wsend(ch, z - k, sub, wslab(ch, z - k, sub), True).wait_send())
                pl.when((z + k < nz) & has_l)(
                    lambda: wsend(ch, z + k, sub, wslab(ch, z + k, sub), False, k == 0).wait_send())
        rc(wp.at[1 - y, :, pl.ds(ch * cols, cols)], wslab(ch, z, y), gy_s.at[ch], g_r.at[ch, z, y],
           y_n).wait_send()

    split = width // 256 * 128 + 128

    def osend(to_right, half):
        part_of = ow.at[:, pl.ds(0, split)] if half == 0 else ow.at[:, pl.ds(split, width - split)]
        return rc(part_of, part_of, o_s.at[0 if to_right else 1, half], o_r.at[half], right if to_right else left)

    def o_own(when):
        def outer():
            load_o.wait()
            for half in range(2):
                pl.when(has_r)(lambda: osend(True, half).start())
                pl.when(has_l)(lambda: osend(False, half).start())

        def inner():
            load_o.wait()
            for half in range(2):
                pl.when(z == 1)(lambda: osend(True, half).start())
                pl.when(z == 2)(lambda: osend(False, half).start())

        def last():
            for half in range(2):
                pl.when(z == 1)(lambda: osend(False, half).start())
                pl.when(z == 2)(lambda: osend(True, half).start())
        cond = is_end if when == 0 else middle
        pl.when((z == s) & cond)((outer, inner, last)[when])

    def o_pass(when, half):
        def go():
            osend(True, half).wait_recv()
            pl.when((z > s) & has_r)(lambda: osend(True, half).start())
            pl.when((z < s) & has_l)(lambda: osend(False, half).start())
        near = (s == 0) & (z == 1) | (s == 3) & (z == 2)
        cross = (s == 1) & (z == 2) | (s == 2) & (z == 1)
        far = (s == 0) & (z == 2) | (s == 3) & (z == 1)
        pl.when((near, cross, far)[when])(go)

    def o_wait():
        def go():
            osend(True, 0).wait_recv()
            osend(True, 1).wait_recv()
        pl.when((z != s) & is_end)(go)

    def o_drain():
        for half in range(2):
            pl.when((z >= s) & has_r)(lambda: osend(True, half).wait_send())
            pl.when((z <= s) & has_l)(lambda: osend(False, half).wait_send())

    def agather(inst, dst):
        ss, rr = (rs_s.at[1], rs_r.at[1]) if inst == 1 else (ag_s, ag_r)

        def blk(yy, sq, i):
            return dst.at[2 * yy + i, pl.ds(pl.multiple_of(sq * own_len, 16), own_len)]

        sx, sp = (s + 2) % 4, s + 1 - 2 * c
        spx = (sp + 2) % 4

        def msg(n, block, dev):
            return rc(block, block, ss.at[n], rr.at[n], dev)

        mine = [blk(y, s, i) for i in range(2)]
        xs = [blk(y, sx, i) for i in range(2)]
        ys = [blk(1 - y, s, i) for i in range(2)]
        dg = [blk(1 - y, sx, i) for i in range(2)]
        sends = [msg(0, mine[0], x_n), msg(1, mine[1], x_n), msg(2, ys[1], x_n),
                 msg(3, mine[0], y_n), msg(4, mine[1], y_n), msg(5, xs[0], y_n)]
        sends += [msg(6 + i, mine[i], core_n) for i in range(2)]
        sends += [msg(8 + i, xs[i], core_n) for i in range(2)]
        sends += [msg(10 + i, ys[i], core_n) for i in range(2)]
        sends += [msg(12 + i, dg[i], core_n) for i in range(2)]
        recvs = [msg(0, xs[0], x_n), msg(1, xs[1], x_n), msg(2, dg[1], x_n),
                 msg(3, ys[0], y_n), msg(4, ys[1], y_n), msg(5, dg[0], y_n)]
        recvs += [msg(6 + i, blk(y, sp, i), core_n) for i in range(2)]
        recvs += [msg(8 + i, blk(y, spx, i), core_n) for i in range(2)]
        recvs += [msg(10 + i, blk(1 - y, sp, i), core_n) for i in range(2)]
        recvs += [msg(12 + i, blk(1 - y, spx, i), core_n) for i in range(2)]

        def begin():
            for n in (0, 4, 1, 3, 6, 7):
                sends[n].start()

        def relay(parts=(0, 1, 2, 3)):
            if 0 in parts:
                recvs[0].wait_recv()
                sends[5].start()
                sends[8].start()
            if 1 in parts:
                recvs[4].wait_recv()
                sends[2].start()
                sends[11].start()
            if 2 in parts:
                recvs[1].wait_recv()
                sends[9].start()
            if 3 in parts:
                recvs[3].wait_recv()
                sends[10].start()

        def finish(parts=(0, 1)):
            if 0 in parts:
                recvs[2].wait_recv()
                sends[13].start()
                recvs[5].wait_recv()
                sends[12].start()
            if 1 in parts:
                for n in range(6, 14):
                    recvs[n].wait_recv()

        def drain():
            for m in sends:
                m.wait_send()

        return begin, relay, finish, drain

    def rscatter(inst, pt, ra, bufs, produce):
        bdx, bdy, brx, bry = bufs
        ss, rr = rs_s.at[inst % 2], rs_r.at[inst % 2]
        xo = 1 - x

        def image(it):
            return (2 * (1 - y) + it) % 4

        def rows(xx, cc):
            return pl.ds(pl.multiple_of((2 * xx + cc) * own_len, 16), own_len)

        def swap(it, xx):
            img = image(it)
            return rc(pt.at[img, rows(xx, 1 - c)], ra.at[img, xx], ss.at[2 * it + xx],
                      rr.at[2 * it + xx], core_n)

        def add(it, xx):
            swap(it, xx).wait_recv()
            img = image(it)
            ra[img, xx] = (ra[img, xx].astype(F32) + pt[img, rows(xx, c)].astype(F32)).astype(BF16)

        m = [
            rc(ra.at[image(0), xo], bdx, ss.at[8], rr.at[8], x_n),
            rc(ra.at[image(1), xo], bdy, ss.at[9], rr.at[9], y_n),
            rc(ra.at[image(1), x], bry.at[1], ss.at[10], rr.at[10], y_n),
            rc(ra.at[image(2), xo], brx.at[0], ss.at[11], rr.at[11], x_n),
            rc(ra.at[image(0), x], bry.at[0], ss.at[12], rr.at[12], y_n),
            rc(ra.at[image(3), xo], brx.at[1], ss.at[13], rr.at[13], x_n),
        ]

        def run_a():
            def step(it, carry):
                produce(image(it))
                swap(it, xo).start()
                swap(it, x).start()
                return carry
            lax.fori_loop(0, nimg, step, 0)

        def run_c():
            add(0, xo)
            m[0].start()
            add(1, xo)
            m[1].start()
            add(1, x)
            m[2].start()
            add(2, xo)
            m[3].start()
            add(0, x)
            add(3, xo)

        def run_b():
            m[0].wait_recv()
            ra[image(0), x] = (ra[image(0), x].astype(F32) + bdx[...].astype(F32)).astype(BF16)
            m[4].start()
            m[1].wait_recv()
            ra[image(3), xo] = (ra[image(3), xo].astype(F32) + bdy[...].astype(F32)).astype(BF16)
            m[5].start()
            add(2, x)
            add(3, x)

        def result(i):
            rc(brx.at[i], brx.at[i], ss.at[11 + 2 * i], rr.at[11 + 2 * i], x_n).wait_recv()
            rc(bry.at[i], bry.at[i], ss.at[12 - 2 * i], rr.at[12 - 2 * i], y_n).wait_recv()
            return (ra[image(2 + i), x].astype(F32) + brx[i].astype(F32)) + bry[i].astype(F32)

        def drain():
            for it in range(nimg):
                swap(it, 0).wait_send()
                swap(it, 1).wait_send()
            for n in range(8, 14):
                rc(bdx, bdx, ss.at[n], rr.at[n], x_n).wait_send()

        return run_a, run_b, result, drain, run_c

    zch = [(2 * cols, cols), (cols, cols), (cols // 2, cols // 2), (0, cols // 2)]
    order = (1 - y, y)

    def rb_at(ch, slot, sub):
        return (rb if ch < 2 else rbh).at[ch % 2, slot, sub]

    def gslab(ch, dest, sub):
        return g.at[wrows(dest, sub), pl.ds(*zch[ch])]

    def zsend(ch, where, sub, outer):
        k = (1, 2, 3, -1)[where]
        to, slot = (1, (z, nz + 1, nz)[where]) if outer else (k, z)
        return rc(gslab(ch, plane_at(k), sub), rb_at(ch, slot, sub), z_s.at[(0, 1, 0, 2)[ch], where, sub],
                  z_r.at[ch, slot, sub], away(to))

    def zadd(ch, dest, slot, sub):
        ref = rb_at(ch, slot, sub)
        rc(ref, ref, z_r.at[ch, slot, sub], z_r.at[ch, slot, sub], core_n).wait_recv()
        r, cs = wrows(dest, sub), slice(zch[ch][0], sum(zch[ch]))
        g[r, cs] = (g[r, cs].astype(F32) + ref[...].astype(F32)).astype(BF16)

    def z_first(ch, parts=(2, 1, 0, 3)):
        def outer():
            for where in (2, 1, 0):
                if where in parts:
                    for sub in order:
                        zsend(ch, where, sub, True).start()

        def inner():
            if 3 in parts:
                for sub in order:
                    zsend(ch, 3, sub, False).start()
        pl.when(is_end)(outer)
        pl.when(middle)(inner)

    def z_merge(ch, where):
        def inner():
            for sub in order:
                zadd(ch, plane_at(where + 1), nz + 1 - where, sub)
                zsend(ch, where, sub, False).start()
        pl.when(middle)(inner)

    def zreduce_own(ch):
        def outer(sub):
            zadd(ch, z, plane_at(1), sub)
            zadd(ch, z, plane_at(2), sub)

        def inner(sub):
            zadd(ch, z, plane_at(-1), sub)
            zadd(ch, z, plane_at(1), sub)
        for sub in order:
            pl.when(is_end)(functools.partial(outer, sub))
            pl.when(middle)(functools.partial(inner, sub))

    def zdrain(ch):
        for sub in range(2):
            zsend(ch, 0, sub, False).wait_send()
            zsend(ch, 1, sub, False).wait_send()
            pl.when(is_end)(lambda: zsend(ch, 2, sub, True).wait_send())
            pl.when(middle)(lambda: zsend(ch, 3, sub, False).wait_send())

    def f_swap(ch):
        src = g.at[wrows(z, 1 - y), pl.ds(*zch[ch])]
        return rc(src, fgrad.at[rank, :, pl.ds(*zch[ch])], f_s.at[ch % 2, 0], f_r.at[ch, 0], y_n)

    def f_msg(ch, n, slot, dev):
        piece = fgrad.at[slot, :, pl.ds(*zch[ch])]
        return rc(piece, piece, f_s.at[ch % 2, n], f_r.at[ch, n], dev)

    sx, sp = (s + 2) % 4, s + 1 - 2 * c
    spx = (sp + 2) % 4

    def f_begin(ch):
        f_swap(ch).start()
        cs = slice(zch[ch][0], sum(zch[ch]))
        fgrad[rank, :, cs] = g[wrows(z, y), cs]
        f_msg(ch, 1, rank, x_n).start()
        f_msg(ch, 3, rank, core_n).start()

    def f_spread(ch):
        other = 2 * s + 1 - y
        f_msg(ch, 0, other, y_n).wait_recv()
        f_msg(ch, 2, other, x_n).start()
        f_msg(ch, 4, other, core_n).start()

    def f_relay(ch):
        f_msg(ch, 1, 2 * sx + y, x_n).wait_recv()
        f_msg(ch, 5, 2 * sx + y, core_n).start()
        f_msg(ch, 2, 2 * sx + 1 - y, x_n).wait_recv()
        f_msg(ch, 6, 2 * sx + 1 - y, core_n).start()

    def f_end(ch):
        f_msg(ch, 3, 2 * sp + y, core_n).wait_recv()
        f_msg(ch, 4, 2 * sp + 1 - y, core_n).wait_recv()
        f_msg(ch, 5, 2 * spx + y, core_n).wait_recv()
        f_msg(ch, 6, 2 * spx + 1 - y, core_n).wait_recv()

    def f_drain(ch):
        f_swap(ch).wait_send()
        for n in range(1, 7):
            f_msg(ch, n, rank, core_n).wait_send()

    far_out = is_end & (plane_at(0) != s) & (plane_at(1) != s)
    adds = middle & ((plane_at(1) == s) | (plane_at(2) == s))

    def zo_send(far):
        if far:
            return rc(og, rbo.at[nz], zo_s.at[0], zo_r.at[nz], away(1))
        return rc(og, rbo.at[z], zo_s.at[0], zo_r.at[z], (2 * s + y, s))

    def zo_add(slot):
        rc(rbo.at[slot], rbo.at[slot], zo_s.at[0], zo_r.at[slot], core_n).wait_recv()
        og[...] = (og[...].astype(F32) + rbo[slot].astype(F32)).astype(BF16)

    def zo_first():
        pl.when(far_out)(lambda: zo_send(True).start())
        pl.when(jnp.logical_not(far_out | adds) & (z != s))(lambda: zo_send(False).start())

    def zo_merge():
        def go():
            zo_add(nz)
            zo_send(False).start()
        pl.when(adds)(go)

    def zo_last():
        def outer():
            zo_add(plane_at(1))
            zo_add(plane_at(2))

        def inner():
            zo_add(plane_at(-1))
            zo_add(plane_at(1))
        pl.when(is_end)(outer)
        pl.when(middle)(inner)

    def qb_send():
        return rc(qbs, qbx.at[z], qb_s.at[0], qb_r.at[z], (2 * s + y, s))

    def qb_begin():
        bsum = jnp.zeros((1, cols), F32)
        for img in range(nimg):
            bsum = bsum + jnp.sum(dqkv[img].astype(F32), axis=0, keepdims=True)
        qbs[...] = jnp.broadcast_to(bsum, (8, cols))
        pl.when(z != s)(lambda: qb_send().start())

    def o_here():
        zo_last()
        total = qbs[...]
        for k in range(1, nz):
            zz = (z + k) % nz
            rc(qbs, qbx.at[zz], qb_s.at[0], qb_r.at[zz], core_n).wait_recv()
            total = total + qbx[zz]
        ograd[0:qw] = og[...]
        ograd[qw:, 0:cols] = jnp.concatenate([total, total], axis=0).astype(BF16)
        ograd[qw:, cols:] = jnp.zeros((16, width - cols), BF16)
        rc(ograd, ograd, zo_s.at[2], zo_r.at[nz + 1], x_n).start()
        rc(ograd, ograd, zo_s.at[3], zo_r.at[nz + 2], core_n).start()

    def o_x():
        rc(ograd, ograd, zo_s.at[2], zo_r.at[nz + 1], x_n).wait_recv()
        rc(ograd, ograd, zo_s.at[3], zo_r.at[nz + 2], core_n).start()

    def o_end():
        pl.when((sp == z) | (spx == z))(
            lambda: rc(ograd, ograd, zo_s.at[3], zo_r.at[nz + 2], core_n).wait_recv())

    def o_out_done(n):
        rc(ograd, ograd, zo_s.at[n], zo_r.at[0], core_n).wait_send()

    def ib_send(k):
        return rc(isb, ibx.at[z], ib_s.at[k - 1], ib_r.at[z], ((d + 2 * k) % (2 * nz), s))

    def ib_begin():
        ib = jnp.zeros((1, win), F32)
        for img in range(nimg):
            ib = ib + jnp.sum(gp[img].astype(F32), axis=0, keepdims=True)
        isb[...] = jnp.broadcast_to(ib, (8, win))
        for k in range(1, nz):
            ib_send(k).start()

    def ib_msg(n, slot, dev):
        return rc(ibgrad.at[slot], ibgrad.at[slot], ib_s.at[n], ib_r.at[n], dev)

    def ib_pass():
        ibsum = isb[...]
        for k in range(1, nz):
            zz = (z + k) % nz
            rc(isb, ibx.at[zz], ib_s.at[0], ib_r.at[zz], core_n).wait_recv()
            ibsum = ibsum + ibx[zz]
        ibgrad[rank] = ibsum
        ib_msg(nz, rank, y_n).start()
        ib_msg(nz + 1, rank, x_n).start()
        ib_msg(nz + 3, rank, core_n).start()

    def ib_mid():
        other = 2 * s + 1 - y
        ib_msg(nz, other, y_n).wait_recv()
        ib_msg(nz + 2, other, x_n).start()
        ib_msg(nz + 4, other, core_n).start()
        ib_msg(nz + 1, 2 * sx + y, x_n).wait_recv()
        ib_msg(nz + 5, 2 * sx + y, core_n).start()

    def ib_last():
        ib_msg(nz + 2, 2 * sx + 1 - y, x_n).wait_recv()
        ib_msg(nz + 6, 2 * sx + 1 - y, core_n).start()

    def ib_end():
        ib_msg(nz + 3, 2 * sp + y, core_n).wait_recv()
        ib_msg(nz + 4, 2 * sp + 1 - y, core_n).wait_recv()
        ib_msg(nz + 5, 2 * spx + y, core_n).wait_recv()
        ib_msg(nz + 6, 2 * spx + 1 - y, core_n).wait_recv()

    def vec_send(k):
        return rc(vslab.at[y, z], vslab.at[y, z], v_s.at[k - 1], v_r.at[z], ((d + 2 * k) % (2 * nz), s))

    def vec_cross():
        return rc(vslab.at[y], vslab.at[y], v_s.at[nz - 1], v_r.at[nz], y_n)

    def vec_begin():
        for k in range(1, nz):
            vec_send(k).start()

    def vec_pass():
        for k in range(1, nz):
            zz = (z + k) % nz
            rc(vslab.at[y, zz], vslab.at[y, zz], v_s.at[0], v_r.at[zz], core_n).wait_recv()
        vec_cross().start()

    def vec_end():
        rc(vslab.at[1 - y], vslab.at[1 - y], v_s.at[0], v_r.at[nz], y_n).wait_recv()
        for zz in range(nz):
            for yy in range(2):
                at = (2 * zz + yy) * rows8
                vecs[:, at : at + rows8] = vslab[yy, zz].astype(F32)[0:VEC, 0:rows8]

    def vec_drain():
        for k in range(1, nz):
            vec_send(k).wait_send()
        vec_cross().wait_send()

    nrank = fgrad.shape[0]
    stores = [pltpu.make_async_copy(a, b, ag_s.at[n]) for n, (a, b) in enumerate(
        [(st_q, q_out), (st_k, k_out), (st_v, v_out), (st_in, in_out), (st_out, out_out), (ograd, o_out),
         (st_o, out_ref), (st_g, gtok_ref), (st_vec, vec_out), (st_ib, ib_out)])]

    def emit_out():
        for t in range(nrank):
            st_out[:, t * ffp : (t + 1) * ffp] = fgrad[t, :, out_at : out_at + ffp]
            st_in[:, t * ffp + cols - in_at : (t + 1) * ffp] = fgrad[t, :, cols : in_at + ffp]
        stores[4].start()

    def emit_ib():
        for t in range(nrank):
            st_ib[0:1, t * ffp : (t + 1) * ffp] = ibgrad[t, 0:1, off_in : off_in + ffp]
        stores[9].start()

    def emit_upper():
        h = cols // 2
        k_from = h - VEC - qw
        for t in range(nrank):
            st_k[:, t * qw + k_from : (t + 1) * qw] = fgrad[t, :, h : VEC + 2 * qw]
            st_v[:, t * qw : (t + 1) * qw] = fgrad[t, :, VEC + 2 * qw : VEC + 3 * qw]
            st_in[:, t * ffp : t * ffp + cols - in_at] = fgrad[t, :, in_at:cols]
        stores[2].start()
        stores[3].start()

    def emit_lower():
        h = cols // 2
        k_from = h - VEC - qw
        for t in range(nrank):
            st_q[:, t * qw : (t + 1) * qw] = fgrad[t, :, VEC : VEC + qw]
            st_k[:, t * qw : t * qw + k_from] = fgrad[t, :, VEC + qw : h]
        stores[0].start()
        stores[1].start()
        vcols = jnp.zeros((rows8, 128), F32)
        for t in range(nrank):
            vcols = vcols + fgrad[t, :, 0:128].astype(F32)
        st_vec[0:VEC] = jnp.transpose(vcols, (1, 0))[0:VEC]
        st_vec[6:7] = ograd[qw : qw + 8, VEC : VEC + qw].astype(F32)[0:1]
        st_vec[7:8] = ograd[qw : qw + 8, VEC + 2 * qw : VEC + 3 * qw].astype(F32)[0:1]
        stores[8].start()

    gather_swap(0)
    ag_x = agather(0, xall)
    ag_c = agather(1, call)
    ag_x[0]()
    gather_own(0)
    for cp in loads[6 : VEC + 6]:
        cp.wait()
    vrows[...] = jnp.zeros_like(vrows)
    for n in range(VEC):
        vrows[n : n + 1, 0:rows8] = vflat[n][...].astype(F32).reshape(1, rows8)
    vslab[y, z] = vrows[...].astype(BF16)
    vec_begin()
    for cp in loads[VEC + 6 :]:
        cp.wait()
    build_rest()
    inrow[...] = inflat[...].astype(F32).reshape(inrow.shape)
    build_bias()
    gather_other(0)
    o_own(0)
    gather_hop1(0, 1, y)
    ag_x[1]((0, 1))
    gather_hop1(0, 1, 1 - y)
    o_own(1)
    gather_hop1(0, 2, y)
    vec_pass()
    o_pass(0, 0)
    ag_x[1]((2, 3))
    o_pass(0, 1)
    gather_swap(1)
    ag_c[0]()
    ag_x[2]((0,))
    gather_hop1(0, 2, 1 - y)
    o_own(2)
    ag_x[2]((1,))
    vec_end()
    g1, s1 = vecs[0:1], vecs[1:2]
    o_b, g2, s2, out_b = vecs[4:5], vecs[5:6], vecs[6:7], vecs[7:8]

    def ln1_step(b, carry):
        img, r = b // 4, pl.ds(pl.multiple_of((b % 4) * 64, 64), 64)
        values = xall[img, r].astype(F32)
        row_mean = jnp.mean(values, axis=-1, keepdims=True)
        centred = values - row_mean
        inverse = lax.rsqrt(jnp.mean(centred * centred, axis=-1, keepdims=True) + eps_norm)
        n1[img, r] = (centred * inverse * g1 + s1).astype(BF16)
        mean1[img, r] = jnp.broadcast_to(row_mean, (64, 128))
        inv1[img, r] = jnp.broadcast_to(inverse, (64, 128))
        return carry

    o_pass(1, 0)
    lax.fori_loop(0, 2 * nimg, ln1_step, 0)
    o_pass(2, 0)
    lax.fori_loop(2 * nimg, 4 * nimg, ln1_step, 0)
    o_pass(1, 1)
    o_pass(2, 1)
    gather_own(1)
    gather_other(1)
    gather_end(0)

    lane = lax.broadcasted_iota(jnp.int32, (1, cols), 1)
    qb = pltpu.roll(vecs[...], (VEC - rank * qw + width) % width, 1)[2:3, :cols]
    vb = pltpu.roll(vecs[...], (VEC + 2 * qw - rank * qw + width) % width, 1)[3:4, :cols]
    qkv_bias = jnp.where((lane >= VEC) & (lane < VEC + qw), qb, 0.0) + jnp.where(
        (lane >= VEC + 2 * qw) & (lane < VEC + 3 * qw), vb, 0.0)

    def att_step(img, carry):
        proj = dot(n1[img], w[:, 0:cols], 1, 0) + qkv_bias
        proj = proj.astype(BF16)
        qkv[img] = proj
        outs = []
        for h in range(2):
            at = VEC + h * HEAD_DIM
            q = proj[:, at : at + HEAD_DIM]
            k = proj[:, qw + at : qw + at + HEAD_DIM]
            v = proj[:, 2 * qw + at : 2 * qw + at + HEAD_DIM]
            sc = dot(q, k, 1, 1) * factor
            e = jnp.exp(sc - jnp.max(sc, axis=-1, keepdims=True))
            p = e / jnp.sum(e, axis=-1, keepdims=True)
            probs[img, h] = p
            outs.append(dot(p.astype(BF16), v, 1, 0).astype(BF16))
        mix[img] = jnp.concatenate(outs, axis=1)
        return carry

    lax.fori_loop(0, 2, att_step, 0)
    ag_c[1]()
    gather_swap(2)
    lax.fori_loop(2, nimg, att_step, 0)
    o_wait()

    def o_part(img):
        part[img] = dot(mix[img], ow[...], 1, 0).astype(BF16)

    rs_h = rscatter(0, part, r1, (dx, dy, rx, ry), o_part)
    rs_h[0]()
    rs_h[4]()
    gather_hop(1, 1)
    gather_drain(0)
    gather_own(2)
    gather_other(2)
    rs_h[1]()
    gather_hop(1, 2)
    ag_c[2]()
    rs_h[3]()
    ag_x[3]()
    ag_n = agather(2, n2)
    for i in range(2):
        hidden = xall[2 * y + i, own_rows].astype(F32) + rs_h[2](i) + o_b
        hid_s[i] = hidden
        hat, inv = normalize(hidden)
        hat2_s[i] = hat
        inv2_s[i] = jnp.broadcast_to(inv, (own_len, 128))
        n2[2 * y + i, own_rows] = (hat * g2 + s2).astype(BF16)
    ag_n[0]()
    gather_hop(2, 1)
    ag_n[1]()
    gather_end(1)
    gather_hop(2, 2)
    ag_n[2]()

    wlane = lax.broadcasted_iota(jnp.int32, (1, win), 1)
    valid = (wlane >= off_out) & (wlane < off_out + ffp)

    def in_step(img, carry):
        pre = dot(n2[img], w[:, in_win : in_win + win], 1, 0) + inb[0:1]
        a, sl = gelu_parts(pltpu.roll(pre, shift, 1))
        act[img] = jnp.where(valid, a, 0.0).astype(BF16)
        slope[img] = jnp.where(valid, sl, 0.0)
        return carry
    lax.fori_loop(0, nimg, in_step, 0)

    rtile = width // 3

    def gout_step(t, carry):
        t = 1 + sg * (1 - t)
        r = pl.ds(pl.multiple_of(t * rtile, rtile), rtile)
        acc = jnp.zeros((rtile, win), F32)
        for img in range(nimg):
            acc = acc + dot(call[img, :, r], act[img], 0, 0)
        gout_tail[r] = acc[:, 0 : 2 * cols - out_win].astype(BF16)
        g[r, 2 * cols : 3 * cols] = acc[:, 2 * cols - out_win :].astype(BF16)
        return carry
    lax.fori_loop(0, 1, gout_step, 0)
    z_first(0, (2,))
    lax.fori_loop(1, 2, gout_step, 0)
    z_first(0, (1,))
    lax.fori_loop(2, 3, gout_step, 0)
    z_first(0, (0, 3))
    gather_end(2)

    def gp_step(img, carry):
        ga = dot(call[img], w[:, out_win : out_win + win], 1, 0) * slope[img]
        gp[img] = pltpu.roll(ga, win - shift, 1).astype(BF16)
        return carry
    lax.fori_loop(0, nimg, gp_step, 0, unroll=2)
    ib_begin()

    def gn2_part(img):
        part[img] = dot(gp[img], w[:, in_win : in_win + win], 1, 1).astype(BF16)

    rs_g2 = rscatter(2, part, r1, (dx, dy, rx, ry), gn2_part)
    rs_g2[0]()
    rs_g2[4]()

    def gin_step(t, carry):
        r = pl.ds(pl.multiple_of(t * rtile, rtile), rtile)
        acc = jnp.zeros((rtile, win), F32)
        for img in range(nimg):
            acc = acc + dot(n2[img, :, r], gp[img], 0, 0)
        lo = cols - in_win
        gin_tail[r] = acc[:, 0:lo].astype(BF16)
        g[r, cols : 2 * cols - 128] = acc[:, lo : win - 128].astype(BF16)
        g[r, 2 * cols - 128 : 2 * cols] = (acc[:, win - 128 :] + gout_tail[r].astype(F32)).astype(BF16)
        return carry

    lax.fori_loop(0, 3, gin_step, 0)
    z_first(1)
    rs_g2[1]()
    z_merge(0, 1)

    sums = [jnp.zeros((1, width), F32) for _ in range(6)]
    ag_g = agather(3, gb)
    for i in range(2):
        gn2 = rs_g2[2](i)
        hat = hat2_s[i]
        sums[2] = sums[2] + jnp.sum(gn2 * hat, axis=0, keepdims=True)
        sums[3] = sums[3] + jnp.sum(gn2, axis=0, keepdims=True)
        up = call[2 * y + i, own_rows].astype(F32)
        gh = up + norm_back(gn2, g2, hat, inv2_s[i][:, 0:1])
        gh_s[i] = gh
        low = gh.astype(BF16)
        gb[2 * y + i, own_rows] = low
        sums[4] = sums[4] + jnp.sum(low.astype(F32), axis=0, keepdims=True)
        sums[5] = sums[5] + jnp.sum(up, axis=0, keepdims=True)
    rs_g2[3]()
    ag_c[3]()
    ag_n[3]()
    ag_g[0]()
    for n in range(2, 6):
        vsum[n : n + 1] = sums[n]
    vsum[6:8] = jnp.zeros((2, width), F32)
    vsum[0:2] = jnp.zeros((2, width), F32)
    z_merge(0, 0)

    def out_part(img):
        part2[img] = dot(act[img], w[:, out_win : out_win + win], 1, 1).astype(BF16)

    rs_o = rscatter(1, part2, r1b, (dxb, dyb, rxb, ryb), out_part)
    rs_o[0]()
    ag_g[1]()
    ag_g[2]()

    gacc = jnp.zeros((qw, width), F32)
    for img in range(nimg):
        gacc = gacc + dot(mix[img], gb[img], 0, 0)
    og[...] = gacc.astype(BF16)
    zo_first()
    rs_o[4]()

    def attb_step(img, carry):
        proj, gbi = qkv[img], gb[img]
        gmix = dot(gbi, ow[...], 1, 1).astype(BF16)
        zero = jnp.zeros((length, VEC), BF16)
        dq, dk, dv = [], [], []
        for h in range(2):
            at = VEC + h * HEAD_DIM
            q = proj[:, at : at + HEAD_DIM]
            k = proj[:, qw + at : qw + at + HEAD_DIM]
            v = proj[:, 2 * qw + at : 2 * qw + at + HEAD_DIM]
            gm = gmix[:, h * HEAD_DIM : (h + 1) * HEAD_DIM]
            p = probs[img, h]
            gpr = dot(gm, v, 1, 1)
            gs = (p * (gpr - jnp.sum(p * gpr, axis=-1, keepdims=True))).astype(BF16)
            dq.append((dot(gs, k, 1, 0) * factor).astype(BF16))
            dk.append((dot(gs, q, 0, 0) * factor).astype(BF16))
            dv.append(dot(p.astype(BF16), gm, 0, 0).astype(BF16))
        pad = jnp.zeros((length, cols - VEC - 3 * qw), BF16)
        dqkv[img] = jnp.concatenate([zero] + dq + dk + dv + [pad], axis=1)
        return carry

    def ln1_sum_step(img, carry):
        pr = part[img].astype(F32)
        hat = (xall[img].astype(F32) - mean1[img][:, 0:1]) * inv1[img][:, 0:1]
        vsum[0:1] = vsum[0:1] + jnp.sum(pr * hat, axis=0, keepdims=True)
        vsum[1:2] = vsum[1:2] + jnp.sum(pr, axis=0, keepdims=True)
        return carry

    def vcol_step(t, carry):
        r = pl.ds(pl.multiple_of(t * rtile, rtile), rtile)
        vcol = jnp.transpose(jnp.concatenate([vsum[:, r], jnp.zeros((120, rtile), F32)], axis=0), (1, 0))
        g[r, 0:128] = (g[r, 0:128].astype(F32) + vcol).astype(BF16)
        return carry

    def gn1_part(img):
        part[img] = dot(dqkv[img], w[:, 0:cols], 1, 1).astype(BF16)
    rs_g1 = rscatter(4, part, r1, (dx, dy, rx, ry), gn1_part)

    def gqkv_step(t, carry):
        t = 1 + sg * (1 - t)
        r = pl.ds(pl.multiple_of(t * rtile, rtile), rtile)
        acc = jnp.zeros((rtile, cols), F32)
        for img in range(nimg):
            acc = acc + dot(n1[img, :, r], dqkv[img], 0, 0)
        g[r, 0 : cols - 128] = acc[:, 0 : cols - 128].astype(BF16)
        g[r, cols - 128 : cols] = (acc[:, cols - 128 :] + gin_tail[r].astype(F32)).astype(BF16)
        return carry

    lax.fori_loop(0, 1, attb_step, 0)
    ib_pass()
    zreduce_own(0)
    f_begin(0)
    lax.fori_loop(1, 3, attb_step, 0)
    z_merge(1, 1)
    lax.fori_loop(3, nimg, attb_step, 0)
    zdrain(0)
    lax.fori_loop(0, 1, gqkv_step, 0)
    z_first(2, (2,))
    lax.fori_loop(1, 2, gqkv_step, 0)
    z_first(2, (1,))
    lax.fori_loop(2, 3, gqkv_step, 0)
    z_first(2, (0, 3))
    rs_o[1]()
    rs_g1[0]()
    rs_g1[4]()
    qb_begin()
    z_merge(1, 0)
    lax.fori_loop(0, nimg, ln1_sum_step, 0)
    lax.fori_loop(0, 3, vcol_step, 0)
    z_first(3)
    f_spread(0)
    ib_mid()
    zo_merge()
    z_merge(2, 1)
    zreduce_own(1)
    f_begin(1)
    rs_g1[1]()
    z_merge(2, 0)
    f_relay(0)
    ib_last()
    f_spread(1)
    z_merge(3, 1)

    z_merge(3, 0)
    pl.when(z == s)(o_here)
    f_relay(1)
    f_drain(0)
    zreduce_own(2)
    f_begin(2)
    f_spread(2)
    f_drain(1)
    zreduce_own(3)
    f_begin(3)
    f_end(0)
    f_end(1)
    emit_out()
    f_relay(2)
    f_spread(3)
    for i in range(2):
        gn1 = rs_g1[2](i)
        hat, inv = normalize(xall[2 * y + i, own_rows].astype(F32))
        st_g[i] = (gh_s[i] + norm_back(gn1, g1, hat, inv)).astype(BF16)
    ag_g[3]()
    stores[7].start()
    for i in range(2):
        st_o[i] = (hid_s[i] + rs_o[2](i) + out_b).astype(BF16)
    stores[6].start()
    pl.when((s + 2) % 4 == z)(o_x)
    ib_end()
    emit_ib()
    f_end(2)
    emit_upper()
    o_end()
    stores[5].start()
    f_relay(3)
    f_end(3)
    emit_lower()

    for ch in (1, 2):
        gather_drain(ch)
    for ch in (1, 2, 3):
        zdrain(ch)
    for ch in (2, 3):
        f_drain(ch)
    o_drain()
    vec_drain()
    rs_o[3]()
    rs_g1[3]()
    pl.when(z != s)(lambda: zo_send(False).wait_send())
    pl.when(z == s)(lambda: o_out_done(2))
    pl.when((z == s) | ((s + 2) % 4 == z))(lambda: o_out_done(3))
    pl.when(z != s)(lambda: qb_send().wait_send())
    for k in range(1, nz):
        ib_send(k).wait_send()
    for n in range(7):
        ib_msg(nz + n, rank, core_n).wait_send()
    for cp in stores:
        cp.wait()


def widen_kernel(n_mat, n_copy, n_row, *refs):
    n = n_mat + n_copy + n_row
    src, refs = refs[:n], refs[n:]
    big, refs = refs[: n_mat + n_copy], refs[n_mat + n_copy :]
    n_flat = (len(refs) - 2 - n - n_mat) // 2
    flat_out, refs = refs[:n_flat], refs[n_flat:]
    held, refs = refs[:n], refs[n:]
    wide, refs = refs[:n_mat], refs[n_mat:]
    flat, (in_s, out_s) = refs[:n_flat], refs[n_flat:]
    got = [pltpu.make_async_copy(src[i], held[i], in_s.at[i]) for i in range(n)]
    put = [pltpu.make_async_copy(wide[i] if i < n_mat else held[i], big[i], out_s.at[i])
           for i in range(n_mat + n_copy)]
    put_flat = [pltpu.make_async_copy(flat[i], flat_out[i], out_s.at[n_mat + n_copy + i]) for i in range(n_flat)]
    for cp in got:
        cp.start()
    for i in range(n_mat + n_copy):
        got[i].wait()
        if i < n_mat:
            rows = wide[i].shape[0]
            for r in range(0, rows, 48):
                wide[i][r : r + 48] = held[i][r : r + 48].astype(F32)
        put[i].start()
    at = 0
    for i in range(n_mat + n_copy, n):
        got[i].wait()
        for r in range(held[i].shape[0]):
            flat[at][...] = held[i][r : r + 1].reshape(held[i].shape[1])
            put_flat[at].start()
            at += 1
    for cp in put + put_flat:
        cp.wait()


def widen(mats, rows, others, tables):
    hbm = pl.BlockSpec(memory_space=pl.ANY)
    arrays = list(mats) + list(others) + list(tables)
    n = len(arrays)
    flat = [jax.ShapeDtypeStruct((t.shape[1],), F32) for t in tables for _ in range(t.shape[0])]
    shapes = [jax.ShapeDtypeStruct((rows, m.shape[1]), F32) for m in mats]
    shapes += [jax.ShapeDtypeStruct(o.shape, o.dtype) for o in others] + flat
    return pl.pallas_call(
        functools.partial(widen_kernel, len(mats), len(others), len(tables)),
        out_shape=tuple(shapes),
        in_specs=[hbm] * n,
        out_specs=[hbm] * len(shapes),
        scratch_shapes=[pltpu.VMEM(a.shape, a.dtype) for a in arrays]
        + [pltpu.VMEM((rows, m.shape[1]), F32) for m in mats]
        + [pltpu.VMEM(f.shape, F32) for f in flat]
        + [pltpu.SemaphoreType.DMA((n,)), pltpu.SemaphoreType.DMA((len(shapes),))],
    )(*arrays)


def layer_fast(
    tokens, cotangent, ln1_gain, ln1_shift, q_weight, q_bias, k_weight, v_weight, v_bias,
    o_weight, o_bias, ln2_gain, ln2_shift, in_weight, in_bias, out_weight, out_bias,
):
    ns, ndp = lax.axis_size("seq"), lax.axis_size("dp")
    nz, ranks = ndp // 2, 2 * ns
    images, own_len, width = tokens.shape
    ff = in_weight.shape[1]
    hid, ffp = width // ranks, ff // ranks
    rows = q_weight.shape[0]
    vec = [ln1_gain, ln1_shift, q_bias, v_bias, o_bias, ln2_gain, ln2_shift, out_bias]
    slab = (2 * VEC, (rows + 127) // 128 * 128)
    total = 3 * 512
    win = (ffp + 127) // 128 * 128
    nimg, length, cols = 2 * images, own_len * ns, 512
    tall = (nimg, length, width)
    half = (own_len, width)
    D = pltpu.SemaphoreType.DMA
    V = pltpu.VMEM
    scratch = dict(
        wp=V((2, rows, total), BF16), fgrad=V((ranks, rows, total), BF16), ograd=V((hid + 16, width), BF16),
        ibgrad=V((ranks, 8, win), F32), st_q=V((rows, width), BF16), st_k=V((rows, width), BF16),
        st_v=V((rows, width), BF16), st_in=V((rows, ff), BF16), st_out=V((rows, ff), BF16),
        vslab=V((2, nz) + slab, BF16), inb=V((8, win), F32), inflat=V((ff,), BF16), inrow=V((1, ff), F32),
        **{f"vflat{n}": V((rows,), BF16) for n in range(VEC)}, vrows=V(slab, F32),
        st_o=V((2,) + half, BF16), st_g=V((2,) + half, BF16), st_vec=V((VEC, rows), F32), st_ib=V((1, ff), F32),
        w=V((2 * nz * rows, total), BF16), ow=V((hid, width), BF16), xall=V(tall, BF16), call=V(tall, BF16),
        n1=V(tall, BF16), n2=V(tall, BF16), gb=V(tall, BF16), qkv=V((nimg, length, cols), BF16),
        probs=V((nimg, 2, length, length), F32), mix=V((nimg, length, hid), BF16),
        act=V((nimg, length, win), BF16), slope=V((nimg, length, win), F32), gp=V((nimg, length, win), BF16),
        part=V(tall, BF16), part2=V(tall, BF16), r1=V((nimg, 2) + half, BF16), r1b=V((nimg, 2) + half, BF16),
        dx=V(half, BF16), dy=V(half, BF16), rx=V((2,) + half, BF16), ry=V((2,) + half, BF16),
        dxb=V(half, BF16), dyb=V(half, BF16), rxb=V((2,) + half, BF16), ryb=V((2,) + half, BF16),
        hid_s=V((2,) + half, F32), hat2_s=V((2,) + half, F32), inv2_s=V((2, own_len, 128), F32),
        gh_s=V((2,) + half, F32), vecs=V((VEC, width), F32),
        g=V((2 * nz * rows, total), BF16), rb=V((2, nz + 2, 2, rows, cols), BF16),
        rbh=V((2, nz + 2, 2, rows, cols // 2), BF16),
        rbo=V((nz + 1, hid, width), BF16), gin_tail=V((width, 128), BF16), gout_tail=V((width, 128), BF16),
        dqkv=V((nimg, length, cols), BF16), vsum=V((8, width), F32),
        mean1=V((nimg, length, 128), F32), inv1=V((nimg, length, 128), F32), ibx=V((nz, 8, win), F32),
        isb=V((8, win), F32), og=V((hid, width), BF16),
        qbs=V((8, cols), F32), qbx=V((nz, 8, cols), F32),
        gy_s=D((3,)), gz_s=D((2, nz, 2)), gzl_s=D((2, 2)), g_r=D((3, nz, 2)), o_s=D((2, 2)), o_r=D((2,)),
        ag_s=D((14,)), ag_r=D((14,)), rs_s=D((2, 14)), rs_r=D((2, 14)), z_s=D((3, 4, 2)),
        z_r=D((4, nz + 2, 2)), zo_s=D((4,)), zo_r=D((nz + 3,)), f_s=D((2, 7)), f_r=D((4, 7)), ib_s=D((nz + 7,)),
        ib_r=D((nz + 7,)), qb_s=D((1,)), qb_r=D((nz,)), v_s=D((nz,)),
        v_r=D((nz + 1,)),
    )
    hbm = pl.BlockSpec(memory_space=pl.ANY)
    out, gtok, gq, gk, gv, gin, gout, go, gvec, gib = pl.pallas_call(
        functools.partial(layer_kernel, nz, hid, ffp),
        out_shape=(
            jax.ShapeDtypeStruct(tokens.shape, BF16), jax.ShapeDtypeStruct(tokens.shape, BF16),
            jax.ShapeDtypeStruct((rows, width), BF16), jax.ShapeDtypeStruct((rows, width), BF16),
            jax.ShapeDtypeStruct((rows, width), BF16), jax.ShapeDtypeStruct((rows, ff), BF16),
            jax.ShapeDtypeStruct((rows, ff), BF16), jax.ShapeDtypeStruct((hid + 16, width), BF16),
            jax.ShapeDtypeStruct((VEC, rows), F32), jax.ShapeDtypeStruct((1, ff), F32),
        ),
        in_specs=[hbm] * (9 + VEC),
        out_specs=[hbm] * 10,
        scratch_shapes=list(scratch.values()),
        compiler_params=pltpu.CompilerParams(
            collective_id=0, has_side_effects=True, vmem_limit_bytes=65000 * 1024),
    )(tokens, cotangent, q_weight, k_weight, v_weight, in_weight, out_weight.T, o_weight, in_bias, *vec)
    (gin, gout, gq, gk, gv, go, out, gtok, d_g1, d_s1, d_g2, d_s2, d_ob, d_outb, d_qb, d_vb, gib) = widen(
        [gin, gout, gq, gk, gv, go], rows, [out, gtok], [gvec, gib])
    return (out, gtok, d_g1, d_s1, gq, d_qb, gk, gv, d_vb, go, d_ob, d_g2, d_s2, gin, gib, gout.T, d_outb)


def mm(a, b, ca, cb):
    return lax.dot_general(a, b, (((ca,), (cb,)), ((), ())), preferred_element_type=F32)


def on_device(
    tokens, cotangent, ln1_gain, ln1_shift, q_weight, q_bias, k_weight, v_weight, v_bias,
    o_weight, o_bias, ln2_gain, ln2_shift, in_weight, in_bias, out_weight, out_bias,
):
    part = lax.axis_index("seq")
    parts = lax.axis_size("seq")
    groups = lax.axis_size("dp")
    images, own_len, width = tokens.shape
    ff = in_weight.shape[1]
    hid = width // parts
    ffp = ff // parts
    heads = HEADS // parts
    length = own_len * parts
    rows = images * length

    def cols(w, n):
        return lax.dynamic_slice_in_dim(w, part * n, n, axis=1)

    vecs = jnp.stack(
        [ln1_gain, ln1_shift, q_bias, v_bias, o_bias, ln2_gain, ln2_shift, out_bias]
    )
    vecs = lax.all_gather(vecs, "dp", axis=1, tiled=True).astype(F32)
    g1, s1, qb, vb, ob, g2, s2, outb = [vecs[i] for i in range(8)]
    x = lax.all_gather(tokens, "seq", axis=1, tiled=True).reshape(rows, width)
    cot = lax.all_gather(cotangent, "seq", axis=1, tiled=True).reshape(rows, width)
    qkv = jnp.concatenate([cols(q_weight, hid), cols(k_weight, hid), cols(v_weight, hid)], axis=1)
    qkv = lax.all_gather(qkv, "dp", axis=0, tiled=True)
    o_w = lax.all_gather(o_weight, "dp", axis=0, tiled=True)
    o_w = lax.dynamic_slice_in_dim(o_w, part * hid, hid, axis=0)
    in_w = lax.all_gather(cols(in_weight, ffp), "dp", axis=0, tiled=True)
    out_w = lax.dynamic_slice_in_dim(out_weight, part * ffp, ffp, axis=0)
    out_w = lax.all_gather(out_w.T, "dp", axis=0, tiled=True)
    qb_own = lax.dynamic_slice_in_dim(qb, part * hid, hid)
    vb_own = lax.dynamic_slice_in_dim(vb, part * hid, hid)
    inb_own = lax.dynamic_slice_in_dim(in_bias, part * ffp, ffp).astype(F32)

    def scatter_tokens(partial):
        return lax.psum_scatter(
            partial.astype(BF16).reshape(images, length, width),
            "seq", scatter_dimension=1, tiled=True,
        ).astype(F32)

    hat1, _ = normalize(x.astype(F32))
    normed1 = (hat1 * g1 + s1).astype(BF16)
    proj = mm(normed1, qkv, 1, 0)
    queries = (proj[:, :hid] + qb_own).astype(BF16).reshape(images, length, heads, HEAD_DIM)
    keys = proj[:, hid : 2 * hid].astype(BF16).reshape(images, length, heads, HEAD_DIM)
    values = (proj[:, 2 * hid :] + vb_own).astype(BF16).reshape(images, length, heads, HEAD_DIM)
    factor = 1.0 / math.sqrt(HEAD_DIM)
    ein = lambda s, a, b: jnp.einsum(s, a, b, preferred_element_type=F32)
    scores = ein("iqhd,ikhd->ihqk", queries, keys) * factor
    top = jnp.max(scores, axis=-1, keepdims=True)
    expo = jnp.exp(scores - top)
    probs = expo / jnp.sum(expo, axis=-1, keepdims=True)
    probs_low = probs.astype(BF16)
    mixed = ein("ihqk,ikhd->iqhd", probs_low, values).astype(BF16).reshape(rows, hid)
    start = tokens.astype(F32)
    hidden = start + scatter_tokens(mm(mixed, o_w, 1, 0)) + ob
    hat2, r2 = normalize(hidden)
    normed2 = (hat2 * g2 + s2).astype(BF16)
    normed2 = lax.all_gather(normed2, "seq", axis=1, tiled=True).reshape(rows, width)
    pre = mm(normed2, in_w, 1, 0) + inb_own
    act, slope = gelu_parts(pre)
    act = act.astype(BF16)
    out = hidden + scatter_tokens(mm(act, out_w, 1, 1)) + outb
    d_out_w = mm(cot, act, 0, 0)
    cot_own = cotangent.astype(F32)
    grad_pre = (mm(cot, out_w, 1, 0) * slope).astype(BF16)
    d_in_w = mm(normed2, grad_pre, 0, 0)
    d_in_b = jnp.sum(grad_pre.astype(F32), axis=0)
    grad_n2 = scatter_tokens(mm(grad_pre, in_w, 1, 1))
    grad_hidden = cot_own + norm_back(grad_n2, g2, hat2, r2)
    branch_own = grad_hidden.astype(BF16)
    branch = lax.all_gather(branch_own, "seq", axis=1, tiled=True).reshape(rows, width)
    d_o_w = mm(mixed, branch, 0, 0)
    grad_mixed = mm(branch, o_w, 1, 1).astype(BF16).reshape(images, length, heads, HEAD_DIM)
    grad_probs = ein("iqhd,ikhd->ihqk", grad_mixed, values)
    row_dot = jnp.sum(probs * grad_probs, axis=-1, keepdims=True)
    grad_scores = (probs * (grad_probs - row_dot)).astype(BF16)
    grad_q = (ein("ihqk,ikhd->iqhd", grad_scores, keys) * factor).astype(BF16).reshape(rows, hid)
    grad_k = (ein("ihqk,iqhd->ikhd", grad_scores, queries) * factor).astype(BF16).reshape(rows, hid)
    grad_v = ein("ihqk,iqhd->ikhd", probs_low, grad_mixed).astype(BF16).reshape(rows, hid)
    grad_qkv = jnp.concatenate([grad_q, grad_k, grad_v], axis=1)
    d_qkv = mm(normed1, grad_qkv, 0, 0)
    d_qb = jnp.sum(grad_q.astype(F32), axis=0)
    d_vb = jnp.sum(grad_v.astype(F32), axis=0)
    grad_n1 = scatter_tokens(mm(grad_qkv, qkv, 1, 1))
    hat1o, r1o = normalize(start)
    grad_tokens = grad_hidden + norm_back(grad_n1, g1, hat1o, r1o)
    wide = jnp.concatenate([d_qkv, d_in_w, d_out_w], axis=1).astype(BF16)
    wide = lax.psum_scatter(wide, "dp", scatter_dimension=0, tiled=True)
    wide = lax.all_gather(wide, "seq", axis=0, tiled=False).astype(F32)

    def spread(lo, n):
        return wide[:, :, lo : lo + n].transpose(1, 0, 2).reshape(width // groups, n * parts)

    gq, gk, gv = [spread(i * hid, hid) for i in range(3)]
    gin = spread(3 * hid, ffp)
    gout = wide[:, :, 3 * hid + ffp :].transpose(0, 2, 1).reshape(ff, width // groups)
    o_full = lax.all_gather(
        lax.psum_scatter(d_o_w.astype(BF16), "dp", scatter_dimension=1, tiled=True),
        "seq", axis=0, tiled=True,
    )
    go = lax.all_to_all(o_full, "dp", split_axis=0, concat_axis=1, tiled=True).astype(F32)
    own_sums = jnp.stack([
        jnp.sum(grad_n1 * hat1o, axis=(0, 1)), jnp.sum(grad_n1, axis=(0, 1)),
        jnp.sum(grad_n2 * hat2, axis=(0, 1)), jnp.sum(grad_n2, axis=(0, 1)),
        jnp.sum(branch_own.astype(F32), axis=(0, 1)), jnp.sum(cot_own, axis=(0, 1)),
        lax.dynamic_update_slice_in_dim(jnp.zeros(width, F32), d_qb, part * hid, 0),
        lax.dynamic_update_slice_in_dim(jnp.zeros(width, F32), d_vb, part * hid, 0),
    ])
    bias_in = lax.dynamic_update_slice_in_dim(jnp.zeros(ff, F32), d_in_b, part * ffp, 0)
    total = lax.psum(jnp.concatenate([own_sums.reshape(-1), bias_in]), ("dp", "seq"))
    vec_part = total[: 8 * width].reshape(8, groups, width // groups)
    vec_part = lax.dynamic_index_in_dim(vec_part, lax.axis_index("dp"), axis=1, keepdims=False)
    bias_total = total[8 * width :]
    return (
        out.astype(BF16), grad_tokens.astype(BF16), vec_part[0], vec_part[1], gq, vec_part[6],
        gk, gv, vec_part[7], go, vec_part[4], vec_part[2], vec_part[3], gin, bias_total, gout,
        vec_part[5],
    )


def solution(mesh):
    fast = mesh.shape["dp"] == 2 * mesh.shape["seq"]
    rows, vec = P("dp", None), P("dp")
    tok = P("dp", "seq", None)
    return jax.shard_map(
        layer_fast if fast else on_device,
        mesh=mesh,
        in_specs=(tok, tok, vec, vec, rows, vec, rows, rows, vec, rows, vec, vec, vec, rows,
                  P(), P(None, "dp"), vec),
        out_specs=(tok, tok, vec, vec, rows, vec, rows, rows, vec, rows, vec, vec, vec, rows,
                   P(), P(None, "dp"), vec),
        check_vma=False,
    )
```
